32 devices in a mesh: dp: 2 (over x), tp: 16 (over y, z, core).
Axes of the slice: x: 2, y: 2, z: 4, core: 2. Of those that a mesh axis runs over, the one named last changes fastest.
Arguments:
- x: bfloat16 [4096, 2048], P('dp'), parts along dimension 0
- w_gate: bfloat16 [2048, 16384], P(None, 'tp')
- w_up: bfloat16 [2048, 16384], P(None, 'tp')
- w_down: bfloat16 [16384, 2048], P('tp')
Outputs:
- output: bfloat16 [4096, 2048], P('dp'), parts along dimension 0
There are 2 independent parts. The reference program is written for one: setup_inputs(seed, part) draws one part's arguments, and reference() takes and returns one part's arrays. A program takes and returns all parts, laid end to end along the dimension named above; an argument that names none is the same for every part.
All inputs are finite; a program needn't handle non-finite values.
Results may differ from the reference program's by a relative error of at most 0.016.
Values are sent between devices in bfloat16 or wider.
A program may use at most 2 GiB of HBM per device.

```python
import jax
import jax.numpy as jnp

ROWS = 2048
D = 2048
FF = 16384


def setup_inputs(seed: int = 0, part: int = 0) -> dict:
    kx, kg, ku, kd = jax.random.split(jax.random.key(seed), 4)
    drawn = {
        "x": jax.random.normal(jax.random.fold_in(kx, part), (ROWS, D), jnp.float32),
        "w_gate": jax.random.normal(kg, (D, FF), jnp.float32) * D**-0.5,
        "w_up": jax.random.normal(ku, (D, FF), jnp.float32) * D**-0.5,
        "w_down": jax.random.normal(kd, (FF, D), jnp.float32) * FF**-0.5,
    }
    return {k: v.astype(jnp.bfloat16) for k, v in drawn.items()}


def reference(x, w_gate, w_up, w_down):
    gate = jnp.dot(x, w_gate, preferred_element_type=jnp.float32)
    up = jnp.dot(x, w_up, preferred_element_type=jnp.float32)
    hidden = (jax.nn.gelu(gate) * up).astype(jnp.bfloat16)
    return jnp.dot(hidden, w_down, preferred_element_type=jnp.float32).astype(jnp.bfloat16)
```

```python
import functools

import jax
import jax.numpy as jnp
from jax import lax
from jax.experimental import pallas as pl
from jax.experimental.pallas import tpu as pltpu
from jax.sharding import PartitionSpec as P

F32, BF16 = jnp.float32, jnp.bfloat16

R = 256
R1, R2 = 160, 96
ROOT1 = (0, 3)
ROOT2 = (0, 1, 2, 3)
NZ = 4


def _lag(z, k):
    return jnp.where(z < k, z, jnp.where(z > k, NZ - 1 - z, max(k, NZ - 1 - k)))


def kernel(
    x_hbm, wg_hbm, wu_hbm, wd_hbm, y,
    x, wg, wu, wd, hid, part,
    sy1, ry1, sz1, rl1, rr1, sz2, rl2, rr2, sy2, ry2,
    in_sem, wd_s, wd_r, hid_s, hid_r,
    y1_s, y1_r, z1_s, l1_r, r1_r, bl1_s, br1_s, b1_r, a1_s, a1_r,
    z2_s, l2_r, r2_r, y2_s, y2_r, a2_s, a2_r, bl2_s, br2_s, b2_r,
    df_s, df_r,
):
    rows, width = y.shape
    n_super = rows // R
    n = 2 * n_super
    half = width // 2
    cw = half // 2
    units = wg_hbm.shape[1]
    uh = units // 2
    n1, n2 = len(ROOT1), len(ROOT2)
    w1 = cw // 2 // n1
    w2 = cw // n2
    rh = R2 // 2

    me = lax.axis_index("tp")
    core = lax.rem(me, 2)
    z = lax.rem(lax.div(me, 2), NZ)
    yy = lax.div(me, 2 * NZ)
    peer = {"tp": me + 1 - 2 * core}
    ypeer = {"tp": lax.rem(me + 2 * NZ, 4 * NZ)}
    left = {"tp": me - 2}
    right = {"tp": me + 2}

    def load(i, src, dst):
        return pltpu.make_async_copy(src, dst, in_sem.at[i])

    def al(v, m):
        return pl.multiple_of(v, m)

    def x_copy(s):
        return load(s, x_hbm.at[pl.ds(al(s * R, R), R)], x.at[s])

    def g_copy(j):
        return load(n_super + j, wg_hbm.at[:, pl.ds(j * uh, uh)], wg.at[j])

    def u_copy(j):
        return load(n_super + 2 + j, wu_hbm.at[:, pl.ds(j * uh, uh)], wu.at[j])

    def d_copy(j):
        return load(
            n_super + 4 + j,
            wd_hbm.at[:, pl.ds(al(core * half + j * cw, cw), cw)],
            wd.at[j, pl.ds(al(core * units, units), units)],
        )

    def remote(src, dst, ssem, rsem, dev):
        return pltpu.make_async_remote_copy(
            src_ref=src, dst_ref=dst, send_sem=ssem, recv_sem=rsem,
            device_id=dev, device_id_type=pl.DeviceIdType.MESH,
        )

    x_copy(0).start()
    g_copy(0).start()
    u_copy(0).start()
    g_copy(1).start()
    u_copy(1).start()
    if n_super > 1:
        x_copy(1).start()
    d_copy(0).start()
    d_copy(1).start()

    barrier = pltpu.get_barrier_semaphore()

    def hello(dev):
        pl.semaphore_signal(barrier, inc=1, device_id=dev, device_id_type=pl.DeviceIdType.MESH)

    hello(peer)
    hello(ypeer)
    pl.when(z > 0)(lambda: hello(left))
    pl.when(z < NZ - 1)(lambda: hello(right))
    pl.semaphore_wait(barrier, 2 + jnp.minimum(z, 1) + jnp.minimum(NZ - 1 - z, 1))

    def wd_msg(j):
        return remote(
            wd_hbm.at[:, pl.ds(al((1 - core) * half + j * cw, cw), cw)],
            wd.at[j, pl.ds(al(core * units, units), units)],
            wd_s.at[j], wd_r.at[j], peer,
        )

    wd_msg(0).start()
    wd_msg(1).start()
    for s in range(2, n_super):
        x_copy(s).start()

    def hid_msg(c):
        s, j = lax.div(c, 2), lax.rem(c, 2)
        place = hid.at[s, :, pl.ds(al(core * units + j * uh, uh), uh)]
        return remote(place, place, hid_s.at[c], hid_r.at[c], peer)

    def row0(c):
        return al(lax.div(c, 2) * R, R)

    def col0(c, who):
        return al(who * half + lax.rem(c, 2) * cw, cw)

    def y1_place(c, h, p):
        return y.at[pl.ds(row0(c), R1), pl.ds(al(col0(c, core) + h * (cw // 2) + p * w1, w1), w1)]

    def y2_place(c, q):
        return y.at[pl.ds(al(row0(c) + R1, 16), R2), pl.ds(al(col0(c, core) + q * w2, w2), w2)]

    def y2_rows(c, q, h):
        return y.at[pl.ds(al(row0(c) + R1 + h * rh, 16), rh), pl.ds(al(col0(c, core) + q * w2, w2), w2)]

    def part1(c, h, p):
        return part.at[c, pl.ds(0, R1), pl.ds(al(h * (cw // 2) + p * w1, w1), w1)]

    def part2(c, q):
        return part.at[c, pl.ds(R1, R2), pl.ds(q * w2, w2)]

    def part2_rows(c, q, h):
        return part.at[c, pl.ds(al(R1 + h * rh, 16), rh), pl.ds(q * w2, w2)]

    def m_y1(c, p):
        return remote(sy1.at[c, p], ry1.at[c, p], y1_s.at[c, p], y1_r.at[c, p], ypeer)

    def m_z1(c, p, to_right):
        dst, sem = (rl1, l1_r) if to_right else (rr1, r1_r)
        return remote(sz1.at[c, p], dst.at[c, p], z1_s.at[c, p], sem.at[c, p], right if to_right else left)

    def m_b1(c, p, to_right):
        place = y1_place(c, yy, p)
        return remote(place, place, (br1_s if to_right else bl1_s).at[c, p], b1_r.at[c, p], right if to_right else left)

    def m_a1(c, p, h):
        place = y1_place(c, h, p)
        return remote(place, place, a1_s.at[c, p], a1_r.at[c, p], ypeer)

    def m_z2(c, q, to_right):
        dst, sem = (rl2, l2_r) if to_right else (rr2, r2_r)
        return remote(sz2.at[c, q], dst.at[c, q], z2_s.at[c, q], sem.at[c, q], right if to_right else left)

    def m_y2(c, q):
        return remote(sy2.at[c], ry2.at[c], y2_s.at[c, q], y2_r.at[c, q], ypeer)

    def m_a2(c, q, h):
        place = y2_rows(c, q, h)
        return remote(place, place, a2_s.at[c, q], a2_r.at[c, q], ypeer)

    def m_b2(c, q, to_right):
        place = y2_place(c, q)
        return remote(place, place, (br2_s if to_right else bl2_s).at[c, q], b2_r.at[c, q], right if to_right else left)

    def m_df(c, who):
        place = y.at[pl.ds(row0(c), R), pl.ds(col0(c, who), cw)]
        return remote(place, place, df_s.at[c], df_r.at[c], peer)

    def gate_up(it):
        s, j = lax.div(it, 2), lax.rem(it, 2)

        @pl.when(j == 0)
        def _():
            x_copy(s).wait()

        @pl.when(it == 0)
        def _():
            g_copy(0).wait()
            u_copy(0).wait()

        @pl.when(it == 1)
        def _():
            g_copy(1).wait()
            u_copy(1).wait()

        nb = min(256, uh)
        for b in range(uh // nb):
            cols = pl.ds(b * nb, nb)
            gate = jnp.dot(x[s], wg[j, :, cols], preferred_element_type=F32)
            up = jnp.dot(x[s], wu[j, :, cols], preferred_element_type=F32)
            hid[s, :, pl.ds(al(core * units + j * uh + b * nb, nb), nb)] = (jax.nn.gelu(gate) * up).astype(BF16)
        hid_msg(it).start()

    def down(c):
        s, j = lax.div(c, 2), lax.rem(c, 2)

        @pl.when(c == 0)
        def _():
            d_copy(0).wait()
            wd_msg(0).wait_recv()

        @pl.when(c == 1)
        def _():
            d_copy(1).wait()
            wd_msg(1).wait_recv()

        @pl.when(j == 0)
        def _():
            hid_msg(c).wait_recv()
            hid_msg(c + 1).wait_recv()

        nb = 256
        for b in range(cw // nb):
            cols = pl.ds(b * nb, nb)
            part[c, :, cols] = jnp.dot(hid[s], wd[j, :, cols], preferred_element_type=F32)
        for p in range(n1):
            sy1[c, p] = part1(c, 1 - yy, p)[...].astype(BF16)
            m_y1(c, p).start()

    def guarded(c, f):
        pl.when((c >= 0) & (c < n))(lambda: f(c))

    def chain(c, k, acc, lbuf, rbuf, sbuf, msg, root):
        @pl.when((z >= 1) & (z <= k))
        def _():
            msg(True).wait_recv()
            acc[...] += lbuf[...].astype(F32)

        @pl.when((z <= NZ - 2) & (z >= k))
        def _():
            msg(False).wait_recv()
            acc[...] += rbuf[...].astype(F32)

        @pl.when(z != k)
        def _():
            sbuf[...] = acc[...].astype(BF16)
            pl.when(z < k)(lambda: msg(True).start())
            pl.when(z > k)(lambda: msg(False).start())

        pl.when(z == k)(root)

    def spread(k, msg):
        if k < NZ - 1:
            pl.when((z >= k) & (z < NZ - 1))(lambda: msg(True).start())
        if k > 0:
            pl.when((z <= k) & (z > 0))(lambda: msg(False).start())

    def reduce1(c, p):
        k = ROOT1[p]
        acc = part1(c, yy, p)
        m_y1(c, p).wait_recv()
        acc[...] += ry1[c, p].astype(F32)

        def root():
            y1_place(c, yy, p)[...] = acc[...].astype(BF16)
            spread(k, lambda to_right: m_b1(c, p, to_right))
            m_a1(c, p, yy).start()

        chain(c, k, acc, rl1.at[c, p], rr1.at[c, p], sz1.at[c, p], lambda to_right: m_z1(c, p, to_right), root)

    def bcast1(c, p):
        k = ROOT1[p]

        @pl.when(z != k)
        def _():
            m_b1(c, p, True).wait_recv()
            spread(k, lambda to_right: m_b1(c, p, to_right))
            m_a1(c, p, yy).start()

    def reduce2(c, q):
        k = ROOT2[q]
        acc = part2(c, q)

        def root():
            sy2[c] = part2_rows(c, q, 1 - yy)[...].astype(BF16)
            m_y2(c, q).start()

        chain(c, k, acc, rl2.at[c, q], rr2.at[c, q], sz2.at[c, q], lambda to_right: m_z2(c, q, to_right), root)

    def cross2(c, q):
        @pl.when(z == ROOT2[q])
        def _():
            m_y2(c, q).wait_recv()
            y2_rows(c, q, yy)[...] = (part2_rows(c, q, yy)[...] + ry2[c].astype(F32)).astype(BF16)
            m_a2(c, q, yy).start()

    def bcast2(c, q):
        k = ROOT2[q]
        pl.when(z == k)(lambda: m_a2(c, q, 1 - yy).wait_recv())
        pl.when(z != k)(lambda: m_b2(c, q, True).wait_recv())
        spread(k, lambda to_right: m_b2(c, q, to_right))

    def finish(c):
        for p in range(n1):
            m_a1(c, p, 1 - yy).wait_recv()
        m_df(c, core).start()

    def dist(k):
        return jnp.where(z < k, k - z, z - k)

    last = max(
        [3 + max(k, NZ - 1 - k) * 2 + 1 for k in ROOT1] + [4 + max(k, NZ - 1 - k) * 2 for k in ROOT2]
    )

    def step(it, carry):
        pl.when(it < n)(lambda: gate_up(it))
        guarded(it - 2, down)
        for p in range(n1):
            guarded(it - 3 - _lag(z, ROOT1[p]), functools.partial(reduce1, p=p))
        for q in range(n2):
            guarded(it - 2 - _lag(z, ROOT2[q]), functools.partial(reduce2, q=q))
        for q, k in enumerate(ROOT2):
            guarded(it - 3 - max(k, NZ - 1 - k), functools.partial(cross2, q=q))
        for p, k in enumerate(ROOT1):
            guarded(it - 3 - max(k, NZ - 1 - k) - dist(k), functools.partial(bcast1, p=p))
        for q, k in enumerate(ROOT2):
            guarded(it - 4 - max(k, NZ - 1 - k) - dist(k), functools.partial(bcast2, q=q))
        guarded(it - last, finish)
        return carry

    lax.fori_loop(0, n + last, step, 0)

    wd_msg(0).wait_send()
    wd_msg(1).wait_send()

    def drain(c, carry):
        hid_msg(c).wait_send()
        for p, k in enumerate(ROOT1):
            m_y1(c, p).wait_send()
            pl.when(z != k)(lambda: m_z1(c, p, True).wait_send())
            if k < NZ - 1:
                pl.when((z >= k) & (z < NZ - 1))(lambda: m_b1(c, p, True).wait_send())
            if k > 0:
                pl.when((z <= k) & (z > 0))(lambda: m_b1(c, p, False).wait_send())
            m_a1(c, p, yy).wait_send()
        for q, k in enumerate(ROOT2):
            pl.when(z != k)(lambda: m_z2(c, q, True).wait_send())

            @pl.when(z == k)
            def _():
                m_y2(c, q).wait_send()
                m_a2(c, q, yy).wait_send()

            if k < NZ - 1:
                pl.when((z >= k) & (z < NZ - 1))(lambda: m_b2(c, q, True).wait_send())
            if k > 0:
                pl.when((z <= k) & (z > 0))(lambda: m_b2(c, q, False).wait_send())
        m_df(c, core).wait_send()
        m_df(c, 1 - core).wait_recv()
        return carry

    lax.fori_loop(0, n, drain, 0)


def block(x, w_gate, w_up, w_down):
    rows, width = x.shape
    units = w_gate.shape[1]
    n_super = rows // R
    n = 2 * n_super
    cw = width // 4
    n1, n2 = len(ROOT1), len(ROOT2)
    w1, w2 = cw // 2 // n1, cw // n2
    dma = pltpu.SemaphoreType.DMA
    one = pltpu.VMEM((n, n1, R1, w1), BF16)
    two = pltpu.VMEM((n, n2, R2, w2), BF16)
    cross = pltpu.VMEM((n, R2 // 2, w2), BF16)
    return pl.pallas_call(
        kernel,
        out_shape=pltpu.VMEM((rows, width), BF16),
        in_specs=[pl.BlockSpec(memory_space=pl.ANY)] * 4,
        out_specs=pl.BlockSpec(memory_space=pltpu.VMEM),
        scratch_shapes=[
            pltpu.VMEM((n_super, R, width), BF16),
            pltpu.VMEM((2, width, units // 2), BF16),
            pltpu.VMEM((2, width, units // 2), BF16),
            pltpu.VMEM((2, 2 * units, cw), BF16),
            pltpu.VMEM((n_super, R, 2 * units), BF16),
            pltpu.VMEM((n, R, cw), F32),
            one, one, one, one, one, two, two, two, cross, cross,
            dma((n_super + 6,)), dma((2,)), dma((2,)), dma((n,)), dma((n,)),
            *[dma((n, n1))] * 10,
            *[dma((n, n2))] * 10,
            dma((n,)), dma((n,)),
        ],
        compiler_params=pltpu.CompilerParams(
            collective_id=0, has_side_effects=True, vmem_limit_bytes=52 * 1024 * 1024
        ),
    )(x, w_gate, w_up, w_down)


def solution(mesh):
    return jax.shard_map(
        block,
        mesh=mesh,
        in_specs=(P("dp", None), P(None, "tp"), P(None, "tp"), P("tp", None)),
        out_specs=P("dp", None),
        check_vma=False,
    )
```

```python
import functools

import jax
import jax.numpy as jnp
from jax import lax
from jax.experimental import pallas as pl
from jax.experimental.pallas import tpu as pltpu
from jax.sharding import PartitionSpec as P

F32, BF16 = jnp.float32, jnp.bfloat16

R = 256
R1, R2 = 192, 64
NJ = 2
ROOT1 = (0, 3)
ROOT2 = (0, 3, 1, 2)
M1, M2 = 1, 1
NZ = 4
HY, HZ, HX, HB, EB, HF = 2, 2, 2, 2, 1, 0


def _far(k):
    return max(k, NZ - 1 - k)


def _hops(z, k):
    return jnp.where(z < k, z, jnp.where(z > k, NZ - 1 - z, _far(k)))


def kernel(
    x_hbm, wg_hbm, wu_hbm, wd_hbm, y,
    x, wg, wu, wd, hid, part,
    sy1, ry1, sz1, rl1, rr1, sz2, rl2, rr2, sy2, ry2,
    in_sem, wd_s, wd_r, hid_s, hid_r,
    y1_s, y1_r, z1_s, l1_r, r1_r, bl1_s, br1_s, b1_r, a1_s, a1_r,
    z2_s, l2_r, r2_r, y2_s, y2_r, a2_s, a2_r, bl2_s, br2_s, b2_r,
    df_s, df_r,
):
    rows, width = y.shape
    n_super = rows // R
    n = NJ * n_super
    half = width // 2
    cw = half // NJ
    units = wg_hbm.shape[1]
    uh = units // NJ
    nb = min(256, uh)
    blocks = units // nb
    w1 = cw // 2 * M1 // len(ROOT1)
    w2 = cw * M2 // len(ROOT2)

    me = lax.axis_index("tp")
    core = lax.rem(me, 2)
    z = lax.rem(lax.div(me, 2), NZ)
    yy = lax.div(me, 2 * NZ)
    peer = {"tp": me + 1 - 2 * core}
    ypeer = {"tp": lax.rem(me + 2 * NZ, 4 * NZ)}
    left = {"tp": me - 2}
    right = {"tp": me + 2}

    def load(i, src, dst):
        return pltpu.make_async_copy(src, dst, in_sem.at[i])

    def al(v, m):
        return pl.multiple_of(v, m)

    def x_copy(s):
        return load(s, x_hbm.at[pl.ds(al(s * R, R), R)], x.at[s])

    def g_copy(b):
        return load(n_super + b, wg_hbm.at[:, pl.ds(b * nb, nb)], wg.at[b])

    def u_copy(b):
        return load(n_super + blocks + b, wu_hbm.at[:, pl.ds(b * nb, nb)], wu.at[b])

    def d_copy(j):
        return load(
            n_super + 2 * blocks + j,
            wd_hbm.at[:, pl.ds(al(core * half + j * cw, cw), cw)],
            wd.at[j, pl.ds(al(core * units, units), units)],
        )

    def remote(src, dst, ssem, rsem, dev):
        return pltpu.make_async_remote_copy(
            src_ref=src, dst_ref=dst, send_sem=ssem, recv_sem=rsem,
            device_id=dev, device_id_type=pl.DeviceIdType.MESH,
        )

    x_copy(0).start()
    for b in range(blocks):
        g_copy(b).start()
        u_copy(b).start()
    for j in range(NJ):
        d_copy(j).start()
    x_copy(1).start()

    barrier = pltpu.get_barrier_semaphore()

    def hello(dev):
        pl.semaphore_signal(barrier, inc=1, device_id=dev, device_id_type=pl.DeviceIdType.MESH)

    hello(peer)
    hello(ypeer)
    pl.when(z > 0)(lambda: hello(left))
    pl.when(z < NZ - 1)(lambda: hello(right))
    pl.semaphore_wait(barrier, 2 + jnp.minimum(z, 1) + jnp.minimum(NZ - 1 - z, 1))

    def wd_msg(j):
        return remote(
            wd_hbm.at[:, pl.ds(al((1 - core) * half + j * cw, cw), cw)],
            wd.at[j, pl.ds(al(core * units, units), units)],
            wd_s.at[j], wd_r.at[j], peer,
        )

    for j in range(NJ):
        wd_msg(j).start()
    for s in range(2, n_super):
        x_copy(s).start()

    def hid_msg(c):
        s, j = lax.div(c, NJ), lax.rem(c, NJ)
        place = hid.at[s, :, pl.ds(al(core * units + j * uh, uh), uh)]
        return remote(place, place, hid_s.at[c], hid_r.at[c], peer)

    def row0(c):
        return al(lax.div(c, NJ) * R, R)

    def col0(c, who):
        return al(who * half + lax.rem(c, NJ) * cw, cw)

    def y1_place(c, h, p):
        return y.at[pl.ds(row0(c), R1), pl.ds(al(col0(c, core) + h * (cw // 2) + p // M1 * w1, w1), w1)]

    def y2_place(c, q):
        return y.at[pl.ds(al(row0(c) + R1, 16), R2), pl.ds(al(col0(c, core) + q // M2 * w2, w2), w2)]

    def part1(c, h, p):
        return part.at[c, pl.ds(0, R1), pl.ds(al(h * (cw // 2) + p // M1 * w1, w1), w1)]

    def part2(c, q):
        return part.at[c, pl.ds(R1, R2), pl.ds(q // M2 * w2, w2)]

    def m_y1(c, p):
        i = p // M1
        return remote(sy1.at[c, i], ry1.at[c, i], y1_s.at[c, i], y1_r.at[c, i], ypeer)

    def m_z1(c, p, to_right):
        i = p // M1
        dst, sem = (rl1, l1_r) if to_right else (rr1, r1_r)
        return remote(sz1.at[c, i], dst.at[c, i], z1_s.at[c, i], sem.at[c, i], right if to_right else left)

    def m_b1(c, p, to_right):
        i = p // M1
        place = y1_place(c, yy, p)
        return remote(place, place, (br1_s if to_right else bl1_s).at[c, i], b1_r.at[c, i], right if to_right else left)

    def m_a1(c, p, h):
        i = p // M1
        place = y1_place(c, h, p)
        return remote(place, place, a1_s.at[c, i], a1_r.at[c, i], ypeer)

    def m_z2(c, q, to_right):
        i = q // M2
        dst, sem = (rl2, l2_r) if to_right else (rr2, r2_r)
        return remote(sz2.at[c, i], dst.at[c, i], z2_s.at[c, i], sem.at[c, i], right if to_right else left)

    def m_y2(c, q):
        return remote(sy2.at[c], ry2.at[c], y2_s.at[c], y2_r.at[c], ypeer)

    def m_a2(c, q):
        place = y2_place(c, q)
        return remote(place, place, a2_s.at[c], a2_r.at[c], ypeer)

    def m_b2(c, q, to_right):
        i = q // M2
        place = y2_place(c, q)
        return remote(place, place, (br2_s if to_right else bl2_s).at[c, i], b2_r.at[c, i], right if to_right else left)

    def y_root(c, q):
        return lax.rem(lax.div(c, M2) + q // 2, 2) == yy

    def m_df(c, who):
        place = y.at[pl.ds(row0(c), R), pl.ds(col0(c, who), cw)]
        return remote(place, place, df_s.at[c], df_r.at[c], peer)

    def gate_up_wait(it):
        @pl.when(lax.rem(it, NJ) == 0)
        def _():
            x_copy(lax.div(it, NJ)).wait()

    def gate_up(it, first=None):
        s, j = lax.div(it, NJ), lax.rem(it, NJ)
        for b in range(uh // nb):
            block = j * (uh // nb) + b
            if first is not None:
                g_copy(first * (uh // nb) + b).wait()
                u_copy(first * (uh // nb) + b).wait()
            gate = jnp.dot(x[s], wg[block], preferred_element_type=F32)
            up = jnp.dot(x[s], wu[block], preferred_element_type=F32)
            hid[s, :, pl.ds(al(core * units + j * uh + b * nb, nb), nb)] = (jax.nn.gelu(gate) * up).astype(BF16)

    def down_wait(c):
        for j in range(NJ):

            @pl.when(c == j)
            def _():
                d_copy(j).wait()
                wd_msg(j).wait_recv()

        @pl.when(lax.rem(c, NJ) == 0)
        def _():
            for j in range(NJ):
                hid_msg(c + j).wait_recv()

    def down(c):
        s, j = lax.div(c, NJ), lax.rem(c, NJ)
        db = min(256, cw)
        for b in range(cw // db):
            cols = pl.ds(b * db, db)
            part[c, :, cols] = jnp.dot(hid[s], wd[j, :, cols], preferred_element_type=F32)

    def down_send(c):
        for p in range(len(ROOT1)):

            @pl.when(active(c, p, M1))
            def _():
                sy1[c, p // M1] = part1(c, 1 - yy, p)[...].astype(BF16)
                m_y1(c, p).start()

    def compute(it):
        for j in range(NJ):

            @pl.when(it == j)
            def _():
                gate_up_wait(it)
                gate_up(it, first=j)
                hid_msg(it).start()

        @pl.when((it >= NJ) & (it < n))
        def _():
            gate_up_wait(it)
            down_wait(it - NJ)
            gate_up(it)
            down(it - NJ)
            hid_msg(it).start()
            down_send(it - NJ)

        @pl.when((it >= n) & (it < n + NJ))
        def _():
            down_wait(it - NJ)
            down(it - NJ)
            down_send(it - NJ)

    def active(c, p, m):
        return True if m == 1 else lax.rem(c, m) == p % m

    def guarded(c, f, p=0, m=1):
        pl.when((c >= 0) & (c < n) & active(c, p, m))(lambda: f(c))

    def chain(c, k, acc, lbuf, rbuf, sbuf, msg, root):
        @pl.when((z >= 1) & (z <= k))
        def _():
            msg(True).wait_recv()
            acc[...] += lbuf[...].astype(F32)

        @pl.when((z <= NZ - 2) & (z >= k))
        def _():
            msg(False).wait_recv()
            acc[...] += rbuf[...].astype(F32)

        @pl.when(z != k)
        def _():
            sbuf[...] = acc[...].astype(BF16)
            pl.when(z < k)(lambda: msg(True).start())
            pl.when(z > k)(lambda: msg(False).start())

        pl.when(z == k)(root)

    def spread(k, msg):
        if k < NZ - 1:
            pl.when((z >= k) & (z < NZ - 1))(lambda: msg(True).start())
        if k > 0:
            pl.when((z <= k) & (z > 0))(lambda: msg(False).start())

    def reduce1(c, p):
        k = ROOT1[p]
        i = p // M1
        acc = part1(c, yy, p)
        m_y1(c, p).wait_recv()
        acc[...] += ry1[c, i].astype(F32)

        def root():
            y1_place(c, yy, p)[...] = acc[...].astype(BF16)
            spread(k, lambda to_right: m_b1(c, p, to_right))
            m_a1(c, p, yy).start()

        chain(c, k, acc, rl1.at[c, i], rr1.at[c, i], sz1.at[c, i], lambda to_right: m_z1(c, p, to_right), root)

    def bcast1(c, p):
        k = ROOT1[p]

        @pl.when(z != k)
        def _():
            m_b1(c, p, True).wait_recv()
            spread(k, lambda to_right: m_b1(c, p, to_right))
            m_a1(c, p, yy).start()

    def reduce2(c, q):
        k = ROOT2[q]
        i = q // M2
        acc = part2(c, q)

        def root():
            @pl.when(jnp.logical_not(y_root(c, q)))
            def _():
                sy2[c] = acc[...].astype(BF16)
                m_y2(c, q).start()

        chain(c, k, acc, rl2.at[c, i], rr2.at[c, i], sz2.at[c, i], lambda to_right: m_z2(c, q, to_right), root)

    def cross2(c, q):
        @pl.when((z == ROOT2[q]) & y_root(c, q))
        def _():
            m_y2(c, q).wait_recv()
            y2_place(c, q)[...] = (part2(c, q)[...] + ry2[c].astype(F32)).astype(BF16)
            m_a2(c, q).start()

    def bcast2(c, q):
        k = ROOT2[q]
        pl.when((z == k) & jnp.logical_not(y_root(c, q)))(lambda: m_a2(c, q).wait_recv())
        pl.when(z != k)(lambda: m_b2(c, q, True).wait_recv())
        spread(k, lambda to_right: m_b2(c, q, to_right))

    def finish(c):
        for p in range(len(ROOT1)):
            pl.when(active(c, p, M1))(lambda: m_a1(c, p, 1 - yy).wait_recv())
        m_df(c, core).start()

    def dist(k):
        return jnp.where(z < k, k - z, z - k)

    last = max(
        [NJ + HY + EB + HF + (HZ + HB) * _far(k) for k in ROOT1]
        + [NJ + 2 * HX + EB + (HZ + HB) * _far(k) for k in ROOT2]
    )

    def step(it, carry):
        compute(it)
        for p, k in enumerate(ROOT1):
            guarded(it - (NJ + HY) - HZ * _hops(z, k), functools.partial(reduce1, p=p), p, M1)
        for q, k in enumerate(ROOT2):
            guarded(it - NJ - HZ * _hops(z, k), functools.partial(reduce2, q=q), q, M2)
        for q, k in enumerate(ROOT2):
            guarded(it - (NJ + HX) - HZ * _far(k), functools.partial(cross2, q=q), q, M2)
        for p, k in enumerate(ROOT1):
            guarded(it - (NJ + HY + EB) - HZ * _far(k) - HB * dist(k), functools.partial(bcast1, p=p), p, M1)
        for q, k in enumerate(ROOT2):
            guarded(it - (NJ + 2 * HX + EB) - HZ * _far(k) - HB * dist(k), functools.partial(bcast2, q=q), q, M2)
        guarded(it - last, finish)
        return carry

    lax.fori_loop(0, n + last, step, 0)

    for j in range(NJ):
        wd_msg(j).wait_send()

    def drain(c, carry):
        hid_msg(c).wait_send()
        for p, k in enumerate(ROOT1):

            @pl.when(active(c, p, M1))
            def _():
                m_y1(c, p).wait_send()
                pl.when(z != k)(lambda: m_z1(c, p, True).wait_send())
                if k < NZ - 1:
                    pl.when((z >= k) & (z < NZ - 1))(lambda: m_b1(c, p, True).wait_send())
                if k > 0:
                    pl.when((z <= k) & (z > 0))(lambda: m_b1(c, p, False).wait_send())
                m_a1(c, p, yy).wait_send()

        for q, k in enumerate(ROOT2):

            @pl.when(active(c, q, M2))
            def _():
                pl.when(z != k)(lambda: m_z2(c, q, True).wait_send())
                pl.when((z == k) & jnp.logical_not(y_root(c, q)))(lambda: m_y2(c, q).wait_send())
                pl.when((z == k) & y_root(c, q))(lambda: m_a2(c, q).wait_send())
                if k < NZ - 1:
                    pl.when((z >= k) & (z < NZ - 1))(lambda: m_b2(c, q, True).wait_send())
                if k > 0:
                    pl.when((z <= k) & (z > 0))(lambda: m_b2(c, q, False).wait_send())

        m_df(c, core).wait_send()
        m_df(c, 1 - core).wait_recv()
        return carry

    lax.fori_loop(0, n, drain, 0)


def block(x, w_gate, w_up, w_down):
    rows, width = x.shape
    units = w_gate.shape[1]
    n_super = rows // R
    n = NJ * n_super
    cw = width // 2 // NJ
    n1, n2 = len(ROOT1) // M1, len(ROOT2) // M2
    w1, w2 = cw // 2 // n1, cw // n2
    nb = min(256, units // NJ)
    blocks = units // nb
    dma = pltpu.SemaphoreType.DMA
    one = pltpu.VMEM((n, n1, R1, w1), BF16)
    two = pltpu.VMEM((n, n2, R2, w2), BF16)
    cross = pltpu.VMEM((n, R2, w2), BF16)
    return pl.pallas_call(
        kernel,
        out_shape=pltpu.VMEM((rows, width), BF16),
        in_specs=[pl.BlockSpec(memory_space=pl.ANY)] * 4,
        out_specs=pl.BlockSpec(memory_space=pltpu.VMEM),
        scratch_shapes=[
            pltpu.VMEM((n_super, R, width), BF16),
            pltpu.VMEM((blocks, width, nb), BF16),
            pltpu.VMEM((blocks, width, nb), BF16),
            pltpu.VMEM((NJ, 2 * units, cw), BF16),
            pltpu.VMEM((n_super, R, 2 * units), BF16),
            pltpu.VMEM((n, R, cw), F32),
            one, one, one, one, one, two, two, two, cross, cross,
            dma((n_super + 2 * blocks + NJ,)), dma((NJ,)), dma((NJ,)), dma((n,)), dma((n,)),
            *[dma((n, n1))] * 10,
            *[dma((n, n2))] * 3, *[dma((n,))] * 4, *[dma((n, n2))] * 3,
            dma((n,)), dma((n,)),
        ],
        compiler_params=pltpu.CompilerParams(
            collective_id=0, has_side_effects=True, vmem_limit_bytes=52 * 1024 * 1024
        ),
    )(x, w_gate, w_up, w_down)


def solution(mesh):
    return jax.shard_map(
        block,
        mesh=mesh,
        in_specs=(P("dp", None), P(None, "tp"), P(None, "tp"), P("tp", None)),
        out_specs=P("dp", None),
        check_vma=False,
    )
```

```python
import functools

import jax
import jax.numpy as jnp
from jax import lax
from jax.experimental import pallas as pl
from jax.experimental.pallas import tpu as pltpu
from jax.sharding import PartitionSpec as P

F32, BF16 = jnp.float32, jnp.bfloat16

R = 256
R1, R2 = 160, 96
NJ = 2
ROOT1 = (0, 3)
ROOT2 = (0, 3, 1, 2)
M1, M2 = 1, 1
NZ = 4
HY, HZ, HX, HB, EB, HF = 2, 2, 2, 2, 1, 0


def _far(k):
    return max(k, NZ - 1 - k)


def _hops(z, k):
    return jnp.where(z < k, z, jnp.where(z > k, NZ - 1 - z, _far(k)))


def kernel(
    x_hbm, wg_hbm, wu_hbm, wd_hbm, y,
    x, wg, wu, wd, hid, part,
    sy1, ry1, sz1, rl1, rr1, sz2, rl2, rr2, sy2, ry2,
    in_sem, wd_s, wd_r, hid_s, hid_r,
    y1_s, y1_r, z1_s, l1_r, r1_r, bl1_s, br1_s, b1_r, a1_s, a1_r,
    z2_s, l2_r, r2_r, y2_s, y2_r, a2_s, a2_r, bl2_s, br2_s, b2_r,
    df_s, df_r,
):
    rows, width = y.shape
    n_super = rows // R
    n = NJ * n_super
    half = width // 2
    cw = half // NJ
    units = wg_hbm.shape[1]
    uh = units // NJ
    nb = min(256, uh)
    blocks = units // nb
    w1 = cw // 2 * M1 // len(ROOT1)
    w2 = cw * M2 // len(ROOT2)

    me = lax.axis_index("tp")
    core = lax.rem(me, 2)
    z = lax.rem(lax.div(me, 2), NZ)
    yy = lax.div(me, 2 * NZ)
    peer = {"tp": me + 1 - 2 * core}
    ypeer = {"tp": lax.rem(me + 2 * NZ, 4 * NZ)}
    left = {"tp": me - 2}
    right = {"tp": me + 2}

    def load(i, src, dst):
        return pltpu.make_async_copy(src, dst, in_sem.at[i])

    def al(v, m):
        return pl.multiple_of(v, m)

    def x_copy(s):
        return load(s, x_hbm.at[pl.ds(al(s * R, R), R)], x.at[s])

    def g_copy(b):
        return load(n_super + b, wg_hbm.at[:, pl.ds(b * nb, nb)], wg.at[b])

    def u_copy(b):
        return load(n_super + blocks + b, wu_hbm.at[:, pl.ds(b * nb, nb)], wu.at[b])

    def d_copy(j):
        return load(
            n_super + 2 * blocks + j,
            wd_hbm.at[:, pl.ds(al(core * half + j * cw, cw), cw)],
            wd.at[j, pl.ds(al(core * units, units), units)],
        )

    def remote(src, dst, ssem, rsem, dev):
        return pltpu.make_async_remote_copy(
            src_ref=src, dst_ref=dst, send_sem=ssem, recv_sem=rsem,
            device_id=dev, device_id_type=pl.DeviceIdType.MESH,
        )

    x_copy(0).start()
    for b in range(blocks):
        g_copy(b).start()
        u_copy(b).start()
    for j in range(NJ):
        d_copy(j).start()
    x_copy(1).start()

    barrier = pltpu.get_barrier_semaphore()

    def hello(dev):
        pl.semaphore_signal(barrier, inc=1, device_id=dev, device_id_type=pl.DeviceIdType.MESH)

    hello(peer)
    hello(ypeer)
    pl.when(z > 0)(lambda: hello(left))
    pl.when(z < NZ - 1)(lambda: hello(right))
    pl.semaphore_wait(barrier, 2 + jnp.minimum(z, 1) + jnp.minimum(NZ - 1 - z, 1))

    def wd_msg(j):
        return remote(
            wd_hbm.at[:, pl.ds(al((1 - core) * half + j * cw, cw), cw)],
            wd.at[j, pl.ds(al(core * units, units), units)],
            wd_s.at[j], wd_r.at[j], peer,
        )

    for j in range(NJ):
        wd_msg(j).start()
    for s in range(2, n_super):
        x_copy(s).start()

    def hid_msg(c):
        s, j = lax.div(c, NJ), lax.rem(c, NJ)
        place = hid.at[s, :, pl.ds(al(core * units + j * uh, uh), uh)]
        return remote(place, place, hid_s.at[c], hid_r.at[c], peer)

    def row0(c):
        return al(lax.div(c, NJ) * R, R)

    def col0(c, who):
        return al(who * half + lax.rem(c, NJ) * cw, cw)

    def y1_place(c, h, p):
        return y.at[pl.ds(row0(c), R1), pl.ds(al(col0(c, core) + h * (cw // 2) + p // M1 * w1, w1), w1)]

    def y2_place(c, q):
        return y.at[pl.ds(al(row0(c) + R1, 16), R2), pl.ds(al(col0(c, core) + q // M2 * w2, w2), w2)]

    def part1(c, h, p):
        return part.at[c, pl.ds(0, R1), pl.ds(al(h * (cw // 2) + p // M1 * w1, w1), w1)]

    def part2(c, q):
        return part.at[c, pl.ds(R1, R2), pl.ds(q // M2 * w2, w2)]

    def m_y1(c, p):
        i = p // M1
        return remote(sy1.at[c, i], ry1.at[c, i], y1_s.at[c, i], y1_r.at[c, i], ypeer)

    def m_z1(c, p, to_right):
        i = p // M1
        dst, sem = (rl1, l1_r) if to_right else (rr1, r1_r)
        return remote(sz1.at[c, i], dst.at[c, i], z1_s.at[c, i], sem.at[c, i], right if to_right else left)

    def m_b1(c, p, to_right):
        i = p // M1
        place = y1_place(c, yy, p)
        return remote(place, place, (br1_s if to_right else bl1_s).at[c, i], b1_r.at[c, i], right if to_right else left)

    def m_a1(c, p, h):
        i = p // M1
        place = y1_place(c, h, p)
        return remote(place, place, a1_s.at[c, i], a1_r.at[c, i], ypeer)

    def m_z2(c, q, to_right):
        i = q // M2
        dst, sem = (rl2, l2_r) if to_right else (rr2, r2_r)
        return remote(sz2.at[c, i], dst.at[c, i], z2_s.at[c, i], sem.at[c, i], right if to_right else left)

    def m_y2(c, q):
        return remote(sy2.at[c], ry2.at[c], y2_s.at[c], y2_r.at[c], ypeer)

    def m_a2(c, q):
        place = y2_place(c, q)
        return remote(place, place, a2_s.at[c], a2_r.at[c], ypeer)

    def m_b2(c, q, to_right):
        i = q // M2
        place = y2_place(c, q)
        return remote(place, place, (br2_s if to_right else bl2_s).at[c, i], b2_r.at[c, i], right if to_right else left)

    def y_root(c, q):
        return lax.rem(lax.div(c, M2) + q // 2, 2) == yy

    def m_df(c, who):
        place = y.at[pl.ds(row0(c), R), pl.ds(col0(c, who), cw)]
        return remote(place, place, df_s.at[c], df_r.at[c], peer)

    def gate_up_wait(it):
        @pl.when(lax.rem(it, NJ) == 0)
        def _():
            x_copy(lax.div(it, NJ)).wait()

    def gate_up(it, first=None):
        s, j = lax.div(it, NJ), lax.rem(it, NJ)
        for b in range(uh // nb):
            block = j * (uh // nb) + b
            if first is not None:
                g_copy(first * (uh // nb) + b).wait()
                u_copy(first * (uh // nb) + b).wait()
            gate = jnp.dot(x[s], wg[block], preferred_element_type=F32)
            up = jnp.dot(x[s], wu[block], preferred_element_type=F32)
            hid[s, :, pl.ds(al(core * units + j * uh + b * nb, nb), nb)] = (jax.nn.gelu(gate) * up).astype(BF16)

    def down_wait(c):
        for j in range(NJ):

            @pl.when(c == j)
            def _():
                d_copy(j).wait()
                wd_msg(j).wait_recv()

        @pl.when(lax.rem(c, NJ) == 0)
        def _():
            for j in range(NJ):
                hid_msg(c + j).wait_recv()

    def down(c):
        s, j = lax.div(c, NJ), lax.rem(c, NJ)
        db = min(256, cw)
        for b in range(cw // db):
            cols = pl.ds(b * db, db)
            part[c, :, cols] = jnp.dot(hid[s], wd[j, :, cols], preferred_element_type=F32)

    def down_send(c):
        for p in range(len(ROOT1)):

            @pl.when(active(c, p, M1))
            def _():
                sy1[c, p // M1] = part1(c, 1 - yy, p)[...].astype(BF16)
                m_y1(c, p).start()

    def compute(it):
        for j in range(NJ):

            @pl.when(it == j)
            def _():
                gate_up_wait(it)
                gate_up(it, first=j)
                hid_msg(it).start()

        @pl.when((it >= NJ) & (it < n))
        def _():
            gate_up_wait(it)
            down_wait(it - NJ)
            gate_up(it)
            down(it - NJ)
            hid_msg(it).start()
            down_send(it - NJ)

        @pl.when((it >= n) & (it < n + NJ))
        def _():
            down_wait(it - NJ)
            down(it - NJ)
            down_send(it - NJ)

    def active(c, p, m):
        return True if m == 1 else lax.rem(c, m) == p % m

    def guarded(c, f, p=0, m=1):
        pl.when((c >= 0) & (c < n) & active(c, p, m))(lambda: f(c))

    def chain(c, k, acc, lbuf, rbuf, sbuf, msg, root):
        @pl.when((z >= 1) & (z <= k))
        def _():
            msg(True).wait_recv()
            acc[...] += lbuf[...].astype(F32)

        @pl.when((z <= NZ - 2) & (z >= k))
        def _():
            msg(False).wait_recv()
            acc[...] += rbuf[...].astype(F32)

        @pl.when(z != k)
        def _():
            sbuf[...] = acc[...].astype(BF16)
            pl.when(z < k)(lambda: msg(True).start())
            pl.when(z > k)(lambda: msg(False).start())

        pl.when(z == k)(root)

    def spread(k, msg):
        if k < NZ - 1:
            pl.when((z >= k) & (z < NZ - 1))(lambda: msg(True).start())
        if k > 0:
            pl.when((z <= k) & (z > 0))(lambda: msg(False).start())

    def reduce1(c, p):
        k = ROOT1[p]
        i = p // M1
        acc = part1(c, yy, p)
        m_y1(c, p).wait_recv()
        acc[...] += ry1[c, i].astype(F32)

        def root():
            y1_place(c, yy, p)[...] = acc[...].astype(BF16)
            spread(k, lambda to_right: m_b1(c, p, to_right))
            m_a1(c, p, yy).start()

        chain(c, k, acc, rl1.at[c, i], rr1.at[c, i], sz1.at[c, i], lambda to_right: m_z1(c, p, to_right), root)

    def bcast1(c, p):
        k = ROOT1[p]

        @pl.when(z != k)
        def _():
            m_b1(c, p, True).wait_recv()
            spread(k, lambda to_right: m_b1(c, p, to_right))
            m_a1(c, p, yy).start()

    def reduce2(c, q):
        k = ROOT2[q]
        i = q // M2
        acc = part2(c, q)

        def root():
            @pl.when(jnp.logical_not(y_root(c, q)))
            def _():
                sy2[c] = acc[...].astype(BF16)
                m_y2(c, q).start()

        chain(c, k, acc, rl2.at[c, i], rr2.at[c, i], sz2.at[c, i], lambda to_right: m_z2(c, q, to_right), root)

    def cross2(c, q):
        @pl.when((z == ROOT2[q]) & y_root(c, q))
        def _():
            m_y2(c, q).wait_recv()
            y2_place(c, q)[...] = (part2(c, q)[...] + ry2[c].astype(F32)).astype(BF16)
            m_a2(c, q).start()

    def bcast2(c, q):
        k = ROOT2[q]
        pl.when((z == k) & jnp.logical_not(y_root(c, q)))(lambda: m_a2(c, q).wait_recv())
        pl.when(z != k)(lambda: m_b2(c, q, True).wait_recv())
        spread(k, lambda to_right: m_b2(c, q, to_right))

    def finish(c):
        for p in range(len(ROOT1)):
            pl.when(active(c, p, M1))(lambda: m_a1(c, p, 1 - yy).wait_recv())
        m_df(c, core).start()

    def dist(k):
        return jnp.where(z < k, k - z, z - k)

    last = max(
        [NJ + HY + EB + HF + (HZ + HB) * _far(k) for k in ROOT1]
        + [NJ + 2 * HX + EB + (HZ + HB) * _far(k) for k in ROOT2]
    )

    def step(it, carry):
        compute(it)
        for p, k in enumerate(ROOT1):
            guarded(it - (NJ + HY) - HZ * _hops(z, k), functools.partial(reduce1, p=p), p, M1)
        for q, k in enumerate(ROOT2):
            guarded(it - NJ - HZ * _hops(z, k), functools.partial(reduce2, q=q), q, M2)
        for q, k in enumerate(ROOT2):
            guarded(it - (NJ + HX) - HZ * _far(k), functools.partial(cross2, q=q), q, M2)
        for p, k in enumerate(ROOT1):
            guarded(it - (NJ + HY + EB) - HZ * _far(k) - HB * dist(k), functools.partial(bcast1, p=p), p, M1)
        for q, k in enumerate(ROOT2):
            guarded(it - (NJ + 2 * HX + EB) - HZ * _far(k) - HB * dist(k), functools.partial(bcast2, q=q), q, M2)
        guarded(it - last, finish)
        return carry

    lax.fori_loop(0, n + last, step, 0)

    for j in range(NJ):
        wd_msg(j).wait_send()

    def drain(c, carry):
        hid_msg(c).wait_send()
        for p, k in enumerate(ROOT1):

            @pl.when(active(c, p, M1))
            def _():
                m_y1(c, p).wait_send()
                pl.when(z != k)(lambda: m_z1(c, p, True).wait_send())
                if k < NZ - 1:
                    pl.when((z >= k) & (z < NZ - 1))(lambda: m_b1(c, p, True).wait_send())
                if k > 0:
                    pl.when((z <= k) & (z > 0))(lambda: m_b1(c, p, False).wait_send())
                m_a1(c, p, yy).wait_send()

        for q, k in enumerate(ROOT2):

            @pl.when(active(c, q, M2))
            def _():
                pl.when(z != k)(lambda: m_z2(c, q, True).wait_send())
                pl.when((z == k) & jnp.logical_not(y_root(c, q)))(lambda: m_y2(c, q).wait_send())
                pl.when((z == k) & y_root(c, q))(lambda: m_a2(c, q).wait_send())
                if k < NZ - 1:
                    pl.when((z >= k) & (z < NZ - 1))(lambda: m_b2(c, q, True).wait_send())
                if k > 0:
                    pl.when((z <= k) & (z > 0))(lambda: m_b2(c, q, False).wait_send())

        m_df(c, core).wait_send()
        m_df(c, 1 - core).wait_recv()
        return carry

    lax.fori_loop(0, n, drain, 0)


def block(x, w_gate, w_up, w_down):
    rows, width = x.shape
    units = w_gate.shape[1]
    n_super = rows // R
    n = NJ * n_super
    cw = width // 2 // NJ
    n1, n2 = len(ROOT1) // M1, len(ROOT2) // M2
    w1, w2 = cw // 2 // n1, cw // n2
    nb = min(256, units // NJ)
    blocks = units // nb
    dma = pltpu.SemaphoreType.DMA
    one = pltpu.VMEM((n, n1, R1, w1), BF16)
    two = pltpu.VMEM((n, n2, R2, w2), BF16)
    cross = pltpu.VMEM((n, R2, w2), BF16)
    return pl.pallas_call(
        kernel,
        out_shape=pltpu.VMEM((rows, width), BF16),
        in_specs=[pl.BlockSpec(memory_space=pl.ANY)] * 4,
        out_specs=pl.BlockSpec(memory_space=pltpu.VMEM),
        scratch_shapes=[
            pltpu.VMEM((n_super, R, width), BF16),
            pltpu.VMEM((blocks, width, nb), BF16),
            pltpu.VMEM((blocks, width, nb), BF16),
            pltpu.VMEM((NJ, 2 * units, cw), BF16),
            pltpu.VMEM((n_super, R, 2 * units), BF16),
            pltpu.VMEM((n, R, cw), F32),
            one, one, one, one, one, two, two, two, cross, cross,
            dma((n_super + 2 * blocks + NJ,)), dma((NJ,)), dma((NJ,)), dma((n,)), dma((n,)),
            *[dma((n, n1))] * 10,
            *[dma((n, n2))] * 3, *[dma((n,))] * 4, *[dma((n, n2))] * 3,
            dma((n,)), dma((n,)),
        ],
        compiler_params=pltpu.CompilerParams(
            collective_id=0, has_side_effects=True, vmem_limit_bytes=52 * 1024 * 1024
        ),
    )(x, w_gate, w_up, w_down)


def solution(mesh):
    return jax.shard_map(
        block,
        mesh=mesh,
        in_specs=(P("dp", None), P(None, "tp"), P(None, "tp"), P("tp", None)),
        out_specs=P("dp", None),
        check_vma=False,
    )
```

```python
import functools

import jax
import jax.numpy as jnp
from jax import lax
from jax.experimental import pallas as pl
from jax.experimental.pallas import tpu as pltpu
from jax.sharding import PartitionSpec as P

F32, BF16 = jnp.float32, jnp.bfloat16

R = 256
R1, R2 = 192, 64
NJ = 2
ROOT1 = (0, 3)
ROOT2 = (0, 3, 1, 2)
M1, M2 = 2, 4
NZ = 4
HY, HZ, HX, HB, EB, HF = 2, 2, 2, 2, 1, 0


def _far(k):
    return max(k, NZ - 1 - k)


def _hops(z, k):
    return jnp.where(z < k, z, jnp.where(z > k, NZ - 1 - z, _far(k)))


def kernel(
    x_hbm, wg_hbm, wu_hbm, wd_hbm, y,
    x, wg, wu, wd, hid, part,
    sy1, ry1, sz1, rl1, rr1, sz2, rl2, rr2, sy2, ry2,
    in_sem, wd_s, wd_r, hid_s, hid_r,
    y1_s, y1_r, z1_s, l1_r, r1_r, bl1_s, br1_s, b1_r, a1_s, a1_r,
    z2_s, l2_r, r2_r, y2_s, y2_r, a2_s, a2_r, bl2_s, br2_s, b2_r,
    df_s, df_r,
):
    rows, width = y.shape
    n_super = rows // R
    n = NJ * n_super
    half = width // 2
    cw = half // NJ
    units = wg_hbm.shape[1]
    uh = units // NJ
    nb = min(256, uh)
    blocks = units // nb
    w1 = cw // 2 * M1 // len(ROOT1)
    w2 = cw * M2 // len(ROOT2)

    me = lax.axis_index("tp")
    core = lax.rem(me, 2)
    z = lax.rem(lax.div(me, 2), NZ)
    yy = lax.div(me, 2 * NZ)
    peer = {"tp": me + 1 - 2 * core}
    ypeer = {"tp": lax.rem(me + 2 * NZ, 4 * NZ)}
    left = {"tp": me - 2}
    right = {"tp": me + 2}

    def load(i, src, dst):
        return pltpu.make_async_copy(src, dst, in_sem.at[i])

    def al(v, m):
        return pl.multiple_of(v, m)

    def x_copy(s):
        return load(s, x_hbm.at[pl.ds(al(s * R, R), R)], x.at[s])

    def g_copy(b):
        return load(n_super + b, wg_hbm.at[:, pl.ds(b * nb, nb)], wg.at[b])

    def u_copy(b):
        return load(n_super + blocks + b, wu_hbm.at[:, pl.ds(b * nb, nb)], wu.at[b])

    def d_copy(j):
        return load(
            n_super + 2 * blocks + j,
            wd_hbm.at[:, pl.ds(al(core * half + j * cw, cw), cw)],
            wd.at[j, pl.ds(al(core * units, units), units)],
        )

    def remote(src, dst, ssem, rsem, dev):
        return pltpu.make_async_remote_copy(
            src_ref=src, dst_ref=dst, send_sem=ssem, recv_sem=rsem,
            device_id=dev, device_id_type=pl.DeviceIdType.MESH,
        )

    x_copy(0).start()
    for b in range(blocks):
        g_copy(b).start()
        u_copy(b).start()
    for j in range(NJ):
        d_copy(j).start()
    x_copy(1).start()

    barrier = pltpu.get_barrier_semaphore()

    def hello(dev):
        pl.semaphore_signal(barrier, inc=1, device_id=dev, device_id_type=pl.DeviceIdType.MESH)

    hello(peer)
    hello(ypeer)
    pl.when(z > 0)(lambda: hello(left))
    pl.when(z < NZ - 1)(lambda: hello(right))
    pl.semaphore_wait(barrier, 2 + jnp.minimum(z, 1) + jnp.minimum(NZ - 1 - z, 1))

    def wd_msg(j):
        return remote(
            wd_hbm.at[:, pl.ds(al((1 - core) * half + j * cw, cw), cw)],
            wd.at[j, pl.ds(al(core * units, units), units)],
            wd_s.at[j], wd_r.at[j], peer,
        )

    for j in range(NJ):
        wd_msg(j).start()
    for s in range(2, n_super):
        x_copy(s).start()

    def hid_msg(c):
        s, j = lax.div(c, NJ), lax.rem(c, NJ)
        place = hid.at[s, :, pl.ds(al(core * units + j * uh, uh), uh)]
        return remote(place, place, hid_s.at[c], hid_r.at[c], peer)

    def row0(c):
        return al(lax.div(c, NJ) * R, R)

    def col0(c, who):
        return al(who * half + lax.rem(c, NJ) * cw, cw)

    def y1_place(c, h, p):
        return y.at[pl.ds(row0(c), R1), pl.ds(al(col0(c, core) + h * (cw // 2) + p // M1 * w1, w1), w1)]

    def y2_place(c, q):
        return y.at[pl.ds(al(row0(c) + R1, 16), R2), pl.ds(al(col0(c, core) + q // M2 * w2, w2), w2)]

    def part1(c, h, p):
        return part.at[c, pl.ds(0, R1), pl.ds(al(h * (cw // 2) + p // M1 * w1, w1), w1)]

    def part2(c, q):
        return part.at[c, pl.ds(R1, R2), pl.ds(q // M2 * w2, w2)]

    def m_y1(c, p):
        i = p // M1
        return remote(sy1.at[c, i], ry1.at[c, i], y1_s.at[c, i], y1_r.at[c, i], ypeer)

    def m_z1(c, p, to_right):
        i = p // M1
        dst, sem = (rl1, l1_r) if to_right else (rr1, r1_r)
        return remote(sz1.at[c, i], dst.at[c, i], z1_s.at[c, i], sem.at[c, i], right if to_right else left)

    def m_b1(c, p, to_right):
        i = p // M1
        place = y1_place(c, yy, p)
        return remote(place, place, (br1_s if to_right else bl1_s).at[c, i], b1_r.at[c, i], right if to_right else left)

    def m_a1(c, p, h):
        i = p // M1
        place = y1_place(c, h, p)
        return remote(place, place, a1_s.at[c, i], a1_r.at[c, i], ypeer)

    def m_z2(c, q, to_right):
        i = q // M2
        dst, sem = (rl2, l2_r) if to_right else (rr2, r2_r)
        return remote(sz2.at[c, i], dst.at[c, i], z2_s.at[c, i], sem.at[c, i], right if to_right else left)

    def m_y2(c, q):
        return remote(sy2.at[c], ry2.at[c], y2_s.at[c], y2_r.at[c], ypeer)

    def m_a2(c, q):
        place = y2_place(c, q)
        return remote(place, place, a2_s.at[c], a2_r.at[c], ypeer)

    def m_b2(c, q, to_right):
        i = q // M2
        place = y2_place(c, q)
        return remote(place, place, (br2_s if to_right else bl2_s).at[c, i], b2_r.at[c, i], right if to_right else left)

    def y_root(c, q):
        return lax.rem(lax.div(c, M2) + q // 2, 2) == yy

    def m_df(c, who):
        place = y.at[pl.ds(row0(c), R), pl.ds(col0(c, who), cw)]
        return remote(place, place, df_s.at[c], df_r.at[c], peer)

    def gate_up_wait(it):
        @pl.when(lax.rem(it, NJ) == 0)
        def _():
            x_copy(lax.div(it, NJ)).wait()

    def gate_up(it, first=None):
        s, j = lax.div(it, NJ), lax.rem(it, NJ)
        for b in range(uh // nb):
            block = j * (uh // nb) + b
            if first is not None:
                g_copy(first * (uh // nb) + b).wait()
                u_copy(first * (uh // nb) + b).wait()
            gate = jnp.dot(x[s], wg[block], preferred_element_type=F32)
            up = jnp.dot(x[s], wu[block], preferred_element_type=F32)
            hid[s, :, pl.ds(al(core * units + j * uh + b * nb, nb), nb)] = (jax.nn.gelu(gate) * up).astype(BF16)

    def down_wait(c):
        for j in range(NJ):

            @pl.when(c == j)
            def _():
                d_copy(j).wait()
                wd_msg(j).wait_recv()

        @pl.when(lax.rem(c, NJ) == 0)
        def _():
            for j in range(NJ):
                hid_msg(c + j).wait_recv()

    def down(c):
        s, j = lax.div(c, NJ), lax.rem(c, NJ)
        db = min(256, cw)
        for b in range(cw // db):
            cols = pl.ds(b * db, db)
            part[c, :, cols] = jnp.dot(hid[s], wd[j, :, cols], preferred_element_type=F32)

    def down_send(c):
        for p in range(len(ROOT1)):

            @pl.when(active(c, p, M1))
            def _():
                sy1[c, p // M1] = part1(c, 1 - yy, p)[...].astype(BF16)
                m_y1(c, p).start()

    def compute(it):
        for j in range(NJ):

            @pl.when(it == j)
            def _():
                gate_up_wait(it)
                gate_up(it, first=j)
                hid_msg(it).start()

        @pl.when((it >= NJ) & (it < n))
        def _():
            gate_up_wait(it)
            down_wait(it - NJ)
            gate_up(it)
            down(it - NJ)
            hid_msg(it).start()
            down_send(it - NJ)

        @pl.when((it >= n) & (it < n + NJ))
        def _():
            down_wait(it - NJ)
            down(it - NJ)
            down_send(it - NJ)

    def active(c, p, m):
        return True if m == 1 else lax.rem(c, m) == p % m

    def guarded(c, f, p=0, m=1):
        pl.when((c >= 0) & (c < n) & active(c, p, m))(lambda: f(c))

    def chain(c, k, acc, lbuf, rbuf, sbuf, msg, root):
        @pl.when((z >= 1) & (z <= k))
        def _():
            msg(True).wait_recv()
            acc[...] += lbuf[...].astype(F32)

        @pl.when((z <= NZ - 2) & (z >= k))
        def _():
            msg(False).wait_recv()
            acc[...] += rbuf[...].astype(F32)

        @pl.when(z != k)
        def _():
            sbuf[...] = acc[...].astype(BF16)
            pl.when(z < k)(lambda: msg(True).start())
            pl.when(z > k)(lambda: msg(False).start())

        pl.when(z == k)(root)

    def spread(k, msg):
        if k < NZ - 1:
            pl.when((z >= k) & (z < NZ - 1))(lambda: msg(True).start())
        if k > 0:
            pl.when((z <= k) & (z > 0))(lambda: msg(False).start())

    def reduce1(c, p):
        k = ROOT1[p]
        i = p // M1
        acc = part1(c, yy, p)
        m_y1(c, p).wait_recv()
        acc[...] += ry1[c, i].astype(F32)

        def root():
            y1_place(c, yy, p)[...] = acc[...].astype(BF16)
            spread(k, lambda to_right: m_b1(c, p, to_right))
            m_a1(c, p, yy).start()

        chain(c, k, acc, rl1.at[c, i], rr1.at[c, i], sz1.at[c, i], lambda to_right: m_z1(c, p, to_right), root)

    def bcast1(c, p):
        k = ROOT1[p]

        @pl.when(z != k)
        def _():
            m_b1(c, p, True).wait_recv()
            spread(k, lambda to_right: m_b1(c, p, to_right))
            m_a1(c, p, yy).start()

    def reduce2(c, q):
        k = ROOT2[q]
        i = q // M2
        acc = part2(c, q)

        def root():
            @pl.when(jnp.logical_not(y_root(c, q)))
            def _():
                sy2[c] = acc[...].astype(BF16)
                m_y2(c, q).start()

        chain(c, k, acc, rl2.at[c, i], rr2.at[c, i], sz2.at[c, i], lambda to_right: m_z2(c, q, to_right), root)

    def cross2(c, q):
        @pl.when((z == ROOT2[q]) & y_root(c, q))
        def _():
            m_y2(c, q).wait_recv()
            y2_place(c, q)[...] = (part2(c, q)[...] + ry2[c].astype(F32)).astype(BF16)
            m_a2(c, q).start()

    def bcast2(c, q):
        k = ROOT2[q]
        pl.when((z == k) & jnp.logical_not(y_root(c, q)))(lambda: m_a2(c, q).wait_recv())
        pl.when(z != k)(lambda: m_b2(c, q, True).wait_recv())
        spread(k, lambda to_right: m_b2(c, q, to_right))

    def finish(c):
        for p in range(len(ROOT1)):
            pl.when(active(c, p, M1))(lambda: m_a1(c, p, 1 - yy).wait_recv())
        m_df(c, core).start()

    def dist(k):
        return jnp.where(z < k, k - z, z - k)

    last = max(
        [NJ + HY + EB + HF + (HZ + HB) * _far(k) for k in ROOT1]
        + [NJ + 2 * HX + EB + (HZ + HB) * _far(k) for k in ROOT2]
    )

    def step(it, carry):
        compute(it)
        for p, k in enumerate(ROOT1):
            guarded(it - (NJ + HY) - HZ * _hops(z, k), functools.partial(reduce1, p=p), p, M1)
        for q, k in enumerate(ROOT2):
            guarded(it - NJ - HZ * _hops(z, k), functools.partial(reduce2, q=q), q, M2)
        for q, k in enumerate(ROOT2):
            guarded(it - (NJ + HX) - HZ * _far(k), functools.partial(cross2, q=q), q, M2)
        for p, k in enumerate(ROOT1):
            guarded(it - (NJ + HY + EB) - HZ * _far(k) - HB * dist(k), functools.partial(bcast1, p=p), p, M1)
        for q, k in enumerate(ROOT2):
            guarded(it - (NJ + 2 * HX + EB) - HZ * _far(k) - HB * dist(k), functools.partial(bcast2, q=q), q, M2)
        guarded(it - last, finish)
        return carry

    lax.fori_loop(0, n + last, step, 0)

    for j in range(NJ):
        wd_msg(j).wait_send()

    def drain(c, carry):
        hid_msg(c).wait_send()
        for p, k in enumerate(ROOT1):

            @pl.when(active(c, p, M1))
            def _():
                m_y1(c, p).wait_send()
                pl.when(z != k)(lambda: m_z1(c, p, True).wait_send())
                if k < NZ - 1:
                    pl.when((z >= k) & (z < NZ - 1))(lambda: m_b1(c, p, True).wait_send())
                if k > 0:
                    pl.when((z <= k) & (z > 0))(lambda: m_b1(c, p, False).wait_send())
                m_a1(c, p, yy).wait_send()

        for q, k in enumerate(ROOT2):

            @pl.when(active(c, q, M2))
            def _():
                pl.when(z != k)(lambda: m_z2(c, q, True).wait_send())
                pl.when((z == k) & jnp.logical_not(y_root(c, q)))(lambda: m_y2(c, q).wait_send())
                pl.when((z == k) & y_root(c, q))(lambda: m_a2(c, q).wait_send())
                if k < NZ - 1:
                    pl.when((z >= k) & (z < NZ - 1))(lambda: m_b2(c, q, True).wait_send())
                if k > 0:
                    pl.when((z <= k) & (z > 0))(lambda: m_b2(c, q, False).wait_send())

        m_df(c, core).wait_send()
        m_df(c, 1 - core).wait_recv()
        return carry

    lax.fori_loop(0, n, drain, 0)


def block(x, w_gate, w_up, w_down):
    rows, width = x.shape
    units = w_gate.shape[1]
    n_super = rows // R
    n = NJ * n_super
    cw = width // 2 // NJ
    n1, n2 = len(ROOT1) // M1, len(ROOT2) // M2
    w1, w2 = cw // 2 // n1, cw // n2
    nb = min(256, units // NJ)
    blocks = units // nb
    dma = pltpu.SemaphoreType.DMA
    one = pltpu.VMEM((n, n1, R1, w1), BF16)
    two = pltpu.VMEM((n, n2, R2, w2), BF16)
    cross = pltpu.VMEM((n, R2, w2), BF16)
    return pl.pallas_call(
        kernel,
        out_shape=pltpu.VMEM((rows, width), BF16),
        in_specs=[pl.BlockSpec(memory_space=pl.ANY)] * 4,
        out_specs=pl.BlockSpec(memory_space=pltpu.VMEM),
        scratch_shapes=[
            pltpu.VMEM((n_super, R, width), BF16),
            pltpu.VMEM((blocks, width, nb), BF16),
            pltpu.VMEM((blocks, width, nb), BF16),
            pltpu.VMEM((NJ, 2 * units, cw), BF16),
            pltpu.VMEM((n_super, R, 2 * units), BF16),
            pltpu.VMEM((n, R, cw), F32),
            one, one, one, one, one, two, two, two, cross, cross,
            dma((n_super + 2 * blocks + NJ,)), dma((NJ,)), dma((NJ,)), dma((n,)), dma((n,)),
            *[dma((n, n1))] * 10,
            *[dma((n, n2))] * 3, *[dma((n,))] * 4, *[dma((n, n2))] * 3,
            dma((n,)), dma((n,)),
        ],
        compiler_params=pltpu.CompilerParams(
            collective_id=0, has_side_effects=True, vmem_limit_bytes=52 * 1024 * 1024
        ),
    )(x, w_gate, w_up, w_down)


def solution(mesh):
    return jax.shard_map(
        block,
        mesh=mesh,
        in_specs=(P("dp", None), P(None, "tp"), P(None, "tp"), P("tp", None)),
        out_specs=P("dp", None),
        check_vma=False,
    )
```

```python
import functools

import jax
import jax.numpy as jnp
from jax import lax
from jax.experimental import pallas as pl
from jax.experimental.pallas import tpu as pltpu
from jax.sharding import PartitionSpec as P

F32, BF16 = jnp.float32, jnp.bfloat16

R = 256
R1, R2 = 192, 64
NJ = 2
ROOT1 = (0, 3)
ROOT2 = (0, 3, 1, 2)
M1, M2 = 2, 4
NZ = 4
HY, HZ, HX, HB, EB, HF = 2, 2, 2, 2, 1, 0


def _far(k):
    return max(k, NZ - 1 - k)


def _hops(z, k):
    return jnp.where(z < k, z, jnp.where(z > k, NZ - 1 - z, _far(k)))


def kernel(
    x_hbm, wg_hbm, wu_hbm, wd_hbm, y,
    x, wg, wu, wd, hid, part,
    sy1, ry1, sz1, rl1, rr1, sz2, rl2, rr2, sy2, ry2,
    in_sem, wd_s, wd_r, hid_s, hid_r,
    y1_s, y1_r, z1_s, l1_r, r1_r, bl1_s, br1_s, b1_r, a1_s, a1_r,
    z2_s, l2_r, r2_r, y2_s, y2_r, a2_s, a2_r, bl2_s, br2_s, b2_r,
    df_s, df_r,
):
    rows, width = y.shape
    n_super = rows // R
    n = NJ * n_super
    half = width // 2
    cw = half // NJ
    units = wg_hbm.shape[1]
    uh = units // NJ
    nb = min(256, uh)
    blocks = units // nb
    w1 = cw // 2 * M1 // len(ROOT1)
    w2 = cw * M2 // len(ROOT2)

    me = lax.axis_index("tp")
    core = lax.rem(me, 2)
    z = lax.rem(lax.div(me, 2), NZ)
    yy = lax.div(me, 2 * NZ)
    peer = {"tp": me + 1 - 2 * core}
    ypeer = {"tp": lax.rem(me + 2 * NZ, 4 * NZ)}
    left = {"tp": me - 2}
    right = {"tp": me + 2}

    def load(i, src, dst):
        return pltpu.make_async_copy(src, dst, in_sem.at[i])

    def al(v, m):
        return pl.multiple_of(v, m)

    def x_copy(s):
        return load(s, x_hbm.at[pl.ds(al(s * R, R), R)], x.at[s])

    def g_copy(b):
        return load(n_super + b, wg_hbm.at[:, pl.ds(b * nb, nb)], wg.at[b])

    def u_copy(b):
        return load(n_super + blocks + b, wu_hbm.at[:, pl.ds(b * nb, nb)], wu.at[b])

    def d_copy(j):
        return load(
            n_super + 2 * blocks + j,
            wd_hbm.at[:, pl.ds(al(core * half + j * cw, cw), cw)],
            wd.at[j, pl.ds(al(core * units, units), units)],
        )

    def remote(src, dst, ssem, rsem, dev):
        return pltpu.make_async_remote_copy(
            src_ref=src, dst_ref=dst, send_sem=ssem, recv_sem=rsem,
            device_id=dev, device_id_type=pl.DeviceIdType.MESH,
        )

    x_copy(0).start()
    for b in range(blocks):
        g_copy(b).start()
        u_copy(b).start()
    for j in range(NJ):
        d_copy(j).start()
    x_copy(1).start()

    barrier = pltpu.get_barrier_semaphore()

    def hello(dev):
        pl.semaphore_signal(barrier, inc=1, device_id=dev, device_id_type=pl.DeviceIdType.MESH)

    hello(peer)
    hello(ypeer)
    pl.when(z > 0)(lambda: hello(left))
    pl.when(z < NZ - 1)(lambda: hello(right))
    pl.semaphore_wait(barrier, 2 + jnp.minimum(z, 1) + jnp.minimum(NZ - 1 - z, 1))

    def wd_msg(j):
        return remote(
            wd_hbm.at[:, pl.ds(al((1 - core) * half + j * cw, cw), cw)],
            wd.at[j, pl.ds(al(core * units, units), units)],
            wd_s.at[j], wd_r.at[j], peer,
        )

    for j in range(NJ):
        wd_msg(j).start()
    for s in range(2, n_super):
        x_copy(s).start()

    def hid_msg(c):
        s, j = lax.div(c, NJ), lax.rem(c, NJ)
        place = hid.at[s, :, pl.ds(al(core * units + j * uh, uh), uh)]
        return remote(place, place, hid_s.at[c], hid_r.at[c], peer)

    def row0(c):
        return al(lax.div(c, NJ) * R, R)

    def col0(c, who):
        return al(who * half + lax.rem(c, NJ) * cw, cw)

    def y1_place(c, h, p):
        return y.at[pl.ds(row0(c), R1), pl.ds(al(col0(c, core) + h * (cw // 2) + p // M1 * w1, w1), w1)]

    def y2_place(c, q):
        return y.at[pl.ds(al(row0(c) + R1, 16), R2), pl.ds(al(col0(c, core) + q // M2 * w2, w2), w2)]

    def part1(c, h, p):
        return part.at[c, pl.ds(0, R1), pl.ds(al(h * (cw // 2) + p // M1 * w1, w1), w1)]

    def part2(c, q):
        return part.at[c, pl.ds(R1, R2), pl.ds(q // M2 * w2, w2)]

    def m_y1(c, p):
        i = p // M1
        return remote(sy1.at[c, i], ry1.at[c, i], y1_s.at[c, i], y1_r.at[c, i], ypeer)

    def m_z1(c, p, to_right):
        i = p // M1
        dst, sem = (rl1, l1_r) if to_right else (rr1, r1_r)
        return remote(sz1.at[c, i], dst.at[c, i], z1_s.at[c, i], sem.at[c, i], right if to_right else left)

    def m_b1(c, p, to_right):
        i = p // M1
        place = y1_place(c, yy, p)
        return remote(place, place, (br1_s if to_right else bl1_s).at[c, i], b1_r.at[c, i], right if to_right else left)

    def m_a1(c, p, h):
        i = p // M1
        place = y1_place(c, h, p)
        return remote(place, place, a1_s.at[c, i], a1_r.at[c, i], ypeer)

    def m_z2(c, q, to_right):
        i = q // M2
        dst, sem = (rl2, l2_r) if to_right else (rr2, r2_r)
        return remote(sz2.at[c, i], dst.at[c, i], z2_s.at[c, i], sem.at[c, i], right if to_right else left)

    def m_y2(c, q):
        return remote(sy2.at[c], ry2.at[c], y2_s.at[c], y2_r.at[c], ypeer)

    def m_a2(c, q):
        place = y2_place(c, q)
        return remote(place, place, a2_s.at[c], a2_r.at[c], ypeer)

    def m_b2(c, q, to_right):
        i = q // M2
        place = y2_place(c, q)
        return remote(place, place, (br2_s if to_right else bl2_s).at[c, i], b2_r.at[c, i], right if to_right else left)

    def y_root(c, q):
        return lax.rem(lax.div(c, M2) + q // 2, 2) == yy

    def m_df(c, who):
        place = y.at[pl.ds(row0(c), R), pl.ds(col0(c, who), cw)]
        return remote(place, place, df_s.at[c], df_r.at[c], peer)

    def gate_up_wait(it):
        @pl.when(lax.rem(it, NJ) == 0)
        def _():
            x_copy(lax.div(it, NJ)).wait()

    def gate_up(it, first=None):
        s, j = lax.div(it, NJ), lax.rem(it, NJ)
        for b in range(uh // nb):
            block = j * (uh // nb) + b
            if first is not None:
                g_copy(first * (uh // nb) + b).wait()
                u_copy(first * (uh // nb) + b).wait()
            gate = jnp.dot(x[s], wg[block], preferred_element_type=F32)
            up = jnp.dot(x[s], wu[block], preferred_element_type=F32)
            hid[s, :, pl.ds(al(core * units + j * uh + b * nb, nb), nb)] = (jax.nn.gelu(gate) * up).astype(BF16)

    def down_wait(c):
        for j in range(NJ):

            @pl.when(c == j)
            def _():
                d_copy(j).wait()
                wd_msg(j).wait_recv()

        @pl.when(lax.rem(c, NJ) == 0)
        def _():
            for j in range(NJ):
                hid_msg(c + j).wait_recv()

    def down(c):
        s, j = lax.div(c, NJ), lax.rem(c, NJ)
        db = min(256, cw)
        for b in range(cw // db):
            cols = pl.ds(b * db, db)
            part[c, :, cols] = jnp.dot(hid[s], wd[j, :, cols], preferred_element_type=F32)

    def down_send(c):
        for p in range(len(ROOT1)):

            @pl.when(active(c, p, M1))
            def _():
                sy1[c, p // M1] = part1(c, 1 - yy, p)[...].astype(BF16)
                m_y1(c, p).start()

    def compute(it):
        for j in range(NJ):

            @pl.when(it == j)
            def _():
                gate_up_wait(it)
                gate_up(it, first=j)
                hid_msg(it).start()

        @pl.when((it >= NJ) & (it < n))
        def _():
            down_wait(it - NJ)
            gate_up_wait(it)
            down(it - NJ)
            gate_up(it)
            hid_msg(it).start()
            down_send(it - NJ)

        @pl.when((it >= n) & (it < n + NJ))
        def _():
            down_wait(it - NJ)
            down(it - NJ)
            down_send(it - NJ)

    def active(c, p, m):
        return True if m == 1 else lax.rem(c, m) == p % m

    def guarded(c, f, p=0, m=1):
        pl.when((c >= 0) & (c < n) & active(c, p, m))(lambda: f(c))

    def chain(c, k, base, lbuf, rbuf, sbuf, msg, root):
        if k > 0:

            @pl.when(z == 0)
            def _():
                sbuf[...] = base().astype(BF16)
                msg(True).start()

        if k < NZ - 1:

            @pl.when(z == NZ - 1)
            def _():
                sbuf[...] = base().astype(BF16)
                msg(False).start()

        if k > 1:

            @pl.when((z > 0) & (z < k))
            def _():
                msg(True).wait_recv()
                sbuf[...] = (base() + lbuf[...].astype(F32)).astype(BF16)
                msg(True).start()

        if k < NZ - 2:

            @pl.when((z < NZ - 1) & (z > k))
            def _():
                msg(False).wait_recv()
                sbuf[...] = (base() + rbuf[...].astype(F32)).astype(BF16)
                msg(False).start()

        pl.when(z == k)(root)

    def arrived(k, lbuf, rbuf, msg):
        total = 0.0
        if k > 0:
            msg(True).wait_recv()
            total = lbuf[...].astype(F32)
        if k < NZ - 1:
            msg(False).wait_recv()
            total = total + rbuf[...].astype(F32)
        return total

    def spread(k, msg):
        if k < NZ - 1:
            pl.when((z >= k) & (z < NZ - 1))(lambda: msg(True).start())
        if k > 0:
            pl.when((z <= k) & (z > 0))(lambda: msg(False).start())

    def reduce1(c, p):
        k = ROOT1[p]
        i = p // M1
        bufs = rl1.at[c, i], rr1.at[c, i]
        m_y1(c, p).wait_recv()

        def base():
            return part1(c, yy, p)[...] + ry1[c, i].astype(F32)

        def msg(to_right):
            return m_z1(c, p, to_right)

        def root():
            more = arrived(k, *bufs, msg)
            y1_place(c, yy, p)[...] = (base() + more).astype(BF16)
            spread(k, lambda to_right: m_b1(c, p, to_right))
            m_a1(c, p, yy).start()

        chain(c, k, base, *bufs, sz1.at[c, i], msg, root)

    def bcast1(c, p):
        k = ROOT1[p]

        @pl.when(z != k)
        def _():
            m_b1(c, p, True).wait_recv()
            spread(k, lambda to_right: m_b1(c, p, to_right))
            m_a1(c, p, yy).start()

    def reduce2(c, q):
        k = ROOT2[q]
        i = q // M2
        bufs = rl2.at[c, i], rr2.at[c, i]

        def base():
            return part2(c, q)[...]

        def msg(to_right):
            return m_z2(c, q, to_right)

        def root():
            @pl.when(jnp.logical_not(y_root(c, q)))
            def _():
                more = arrived(k, *bufs, msg)
                sy2[c] = (base() + more).astype(BF16)
                m_y2(c, q).start()

        chain(c, k, base, *bufs, sz2.at[c, i], msg, root)

    def cross2(c, q):
        k = ROOT2[q]
        i = q // M2

        @pl.when((z == k) & y_root(c, q))
        def _():
            more = arrived(k, rl2.at[c, i], rr2.at[c, i], lambda to_right: m_z2(c, q, to_right))
            m_y2(c, q).wait_recv()
            y2_place(c, q)[...] = (part2(c, q)[...] + more + ry2[c].astype(F32)).astype(BF16)
            m_a2(c, q).start()

    def bcast2(c, q):
        k = ROOT2[q]
        pl.when((z == k) & jnp.logical_not(y_root(c, q)))(lambda: m_a2(c, q).wait_recv())
        pl.when(z != k)(lambda: m_b2(c, q, True).wait_recv())
        spread(k, lambda to_right: m_b2(c, q, to_right))

    def finish(c):
        for p in range(len(ROOT1)):
            pl.when(active(c, p, M1))(lambda: m_a1(c, p, 1 - yy).wait_recv())
        m_df(c, core).start()

    def dist(k):
        return jnp.where(z < k, k - z, z - k)

    last = max(
        [NJ + HY + EB + HF + (HZ + HB) * _far(k) for k in ROOT1]
        + [NJ + 2 * HX + EB + (HZ + HB) * _far(k) for k in ROOT2]
    )

    def step(it, carry):
        compute(it)
        for p, k in enumerate(ROOT1):
            guarded(it - (NJ + HY) - HZ * _hops(z, k), functools.partial(reduce1, p=p), p, M1)
        for q, k in enumerate(ROOT2):
            guarded(it - NJ - HZ * _hops(z, k), functools.partial(reduce2, q=q), q, M2)
        for q, k in enumerate(ROOT2):
            guarded(it - (NJ + HX) - HZ * _far(k), functools.partial(cross2, q=q), q, M2)
        for p, k in enumerate(ROOT1):
            guarded(it - (NJ + HY + EB) - HZ * _far(k) - HB * dist(k), functools.partial(bcast1, p=p), p, M1)
        for q, k in enumerate(ROOT2):
            guarded(it - (NJ + 2 * HX + EB) - HZ * _far(k) - HB * dist(k), functools.partial(bcast2, q=q), q, M2)
        guarded(it - last, finish)
        return carry

    lax.fori_loop(0, n + last, step, 0)

    for j in range(NJ):
        wd_msg(j).wait_send()

    def drain(c, carry):
        hid_msg(c).wait_send()
        for p, k in enumerate(ROOT1):

            @pl.when(active(c, p, M1))
            def _():
                m_y1(c, p).wait_send()
                pl.when(z != k)(lambda: m_z1(c, p, True).wait_send())
                if k < NZ - 1:
                    pl.when((z >= k) & (z < NZ - 1))(lambda: m_b1(c, p, True).wait_send())
                if k > 0:
                    pl.when((z <= k) & (z > 0))(lambda: m_b1(c, p, False).wait_send())
                m_a1(c, p, yy).wait_send()

        for q, k in enumerate(ROOT2):

            @pl.when(active(c, q, M2))
            def _():
                pl.when(z != k)(lambda: m_z2(c, q, True).wait_send())
                pl.when((z == k) & jnp.logical_not(y_root(c, q)))(lambda: m_y2(c, q).wait_send())
                pl.when((z == k) & y_root(c, q))(lambda: m_a2(c, q).wait_send())
                if k < NZ - 1:
                    pl.when((z >= k) & (z < NZ - 1))(lambda: m_b2(c, q, True).wait_send())
                if k > 0:
                    pl.when((z <= k) & (z > 0))(lambda: m_b2(c, q, False).wait_send())

        m_df(c, core).wait_send()
        m_df(c, 1 - core).wait_recv()
        return carry

    lax.fori_loop(0, n, drain, 0)


def block(x, w_gate, w_up, w_down):
    rows, width = x.shape
    units = w_gate.shape[1]
    n_super = rows // R
    n = NJ * n_super
    cw = width // 2 // NJ
    n1, n2 = len(ROOT1) // M1, len(ROOT2) // M2
    w1, w2 = cw // 2 // n1, cw // n2
    nb = min(256, units // NJ)
    blocks = units // nb
    dma = pltpu.SemaphoreType.DMA
    one = pltpu.VMEM((n, n1, R1, w1), BF16)
    two = pltpu.VMEM((n, n2, R2, w2), BF16)
    cross = pltpu.VMEM((n, R2, w2), BF16)
    return pl.pallas_call(
        kernel,
        out_shape=pltpu.VMEM((rows, width), BF16),
        in_specs=[pl.BlockSpec(memory_space=pl.ANY)] * 4,
        out_specs=pl.BlockSpec(memory_space=pltpu.VMEM),
        scratch_shapes=[
            pltpu.VMEM((n_super, R, width), BF16),
            pltpu.VMEM((blocks, width, nb), BF16),
            pltpu.VMEM((blocks, width, nb), BF16),
            pltpu.VMEM((NJ, 2 * units, cw), BF16),
            pltpu.VMEM((n_super, R, 2 * units), BF16),
            pltpu.VMEM((n, R, cw), F32),
            one, one, one, one, one, two, two, two, cross, cross,
            dma((n_super + 2 * blocks + NJ,)), dma((NJ,)), dma((NJ,)), dma((n,)), dma((n,)),
            *[dma((n, n1))] * 10,
            *[dma((n, n2))] * 3, *[dma((n,))] * 4, *[dma((n, n2))] * 3,
            dma((n,)), dma((n,)),
        ],
        compiler_params=pltpu.CompilerParams(
            collective_id=0, has_side_effects=True, vmem_limit_bytes=52 * 1024 * 1024
        ),
    )(x, w_gate, w_up, w_down)


def solution(mesh):
    return jax.shard_map(
        block,
        mesh=mesh,
        in_specs=(P("dp", None), P(None, "tp"), P(None, "tp"), P("tp", None)),
        out_specs=P("dp", None),
        check_vma=False,
    )
```

```python
import functools

import jax
import jax.numpy as jnp
from jax import lax
from jax.experimental import pallas as pl
from jax.experimental.pallas import tpu as pltpu
from jax.sharding import PartitionSpec as P

F32, BF16 = jnp.float32, jnp.bfloat16

R = 256
R1, R2 = 208, 48
NJ = 2
ROOT1 = (0, 3)
ROOT2 = (0, 2, 1, 3)
M1, M2 = 1, 4
NZ = 4
HY, HZ, HX, HB, EB, HF = 2, 2, 3, 3, 0, 1


def _far(k):
    return max(k, NZ - 1 - k)


def _hops(z, k):
    return jnp.where(z < k, z, jnp.where(z > k, NZ - 1 - z, _far(k)))


def kernel(
    x_hbm, wg_hbm, wu_hbm, wd_hbm, y,
    x, wg, wu, wd, hid, part,
    sy1, ry1, sz1, rl1, rr1, sz2, rl2, rr2, sy2, ry2,
    in_sem, wd_s, wd_r, hid_s, hid_r,
    y1_s, y1_r, z1_s, l1_r, r1_r, bl1_s, br1_s, b1_r, a1_s, a1_r,
    z2_s, l2_r, r2_r, y2_s, y2_r, a2_s, a2_r, bl2_s, br2_s, b2_r,
    df_s, df_r,
):
    rows, width = y.shape
    n_super = rows // R
    n = NJ * n_super
    half = width // 2
    cw = half // NJ
    units = wg_hbm.shape[1]
    uh = units // NJ
    nb = min(256, uh)
    blocks = units // nb
    w1 = cw // 2 * M1 // len(ROOT1)
    w2 = cw * M2 // len(ROOT2)

    me = lax.axis_index("tp")
    core = lax.rem(me, 2)
    z = lax.rem(lax.div(me, 2), NZ)
    yy = lax.div(me, 2 * NZ)
    peer = {"tp": me + 1 - 2 * core}
    ypeer = {"tp": lax.rem(me + 2 * NZ, 4 * NZ)}
    left = {"tp": me - 2}
    right = {"tp": me + 2}

    def load(i, src, dst):
        return pltpu.make_async_copy(src, dst, in_sem.at[i])

    def al(v, m):
        return pl.multiple_of(v, m)

    def x_copy(s):
        return load(s, x_hbm.at[pl.ds(al(s * R, R), R)], x.at[s])

    def g_copy(b):
        return load(n_super + b, wg_hbm.at[:, pl.ds(b * nb, nb)], wg.at[b])

    def u_copy(b):
        return load(n_super + blocks + b, wu_hbm.at[:, pl.ds(b * nb, nb)], wu.at[b])

    def d_copy(j):
        return load(
            n_super + 2 * blocks + j,
            wd_hbm.at[:, pl.ds(al(core * half + j * cw, cw), cw)],
            wd.at[j, pl.ds(al(core * units, units), units)],
        )

    def remote(src, dst, ssem, rsem, dev):
        return pltpu.make_async_remote_copy(
            src_ref=src, dst_ref=dst, send_sem=ssem, recv_sem=rsem,
            device_id=dev, device_id_type=pl.DeviceIdType.MESH,
        )

    x_copy(0).start()
    for b in range(blocks):
        g_copy(b).start()
        u_copy(b).start()
    for j in range(NJ):
        d_copy(j).start()
    x_copy(1).start()

    barrier = pltpu.get_barrier_semaphore()

    def hello(dev):
        pl.semaphore_signal(barrier, inc=1, device_id=dev, device_id_type=pl.DeviceIdType.MESH)

    hello(peer)
    hello(ypeer)
    pl.when(z > 0)(lambda: hello(left))
    pl.when(z < NZ - 1)(lambda: hello(right))
    pl.semaphore_wait(barrier, 2 + jnp.minimum(z, 1) + jnp.minimum(NZ - 1 - z, 1))

    def wd_msg(j):
        return remote(
            wd_hbm.at[:, pl.ds(al((1 - core) * half + j * cw, cw), cw)],
            wd.at[j, pl.ds(al(core * units, units), units)],
            wd_s.at[j], wd_r.at[j], peer,
        )

    for j in range(NJ):
        wd_msg(j).start()
    for s in range(2, n_super):
        x_copy(s).start()

    def hid_msg(c):
        s, j = lax.div(c, NJ), lax.rem(c, NJ)
        place = hid.at[s, :, pl.ds(al(core * units + j * uh, uh), uh)]
        return remote(place, place, hid_s.at[c], hid_r.at[c], peer)

    def row0(c):
        return al(lax.div(c, NJ) * R, R)

    def col0(c, who):
        return al(who * half + lax.rem(c, NJ) * cw, cw)

    def y1_place(c, h, p):
        return y.at[pl.ds(row0(c), R1), pl.ds(al(col0(c, core) + h * (cw // 2) + p // M1 * w1, w1), w1)]

    def y2_place(c, q):
        return y.at[pl.ds(al(row0(c) + R1, 16), R2), pl.ds(al(col0(c, core) + q // M2 * w2, w2), w2)]

    def part1(c, h, p):
        return part.at[c, pl.ds(0, R1), pl.ds(al(h * (cw // 2) + p // M1 * w1, w1), w1)]

    def part2(c, q):
        return part.at[c, pl.ds(R1, R2), pl.ds(q // M2 * w2, w2)]

    def m_y1(c, p):
        i = p // M1
        return remote(sy1.at[c, i], ry1.at[c, i], y1_s.at[c, i], y1_r.at[c, i], ypeer)

    def m_z1(c, p, to_right):
        i = p // M1
        dst, sem = (rl1, l1_r) if to_right else (rr1, r1_r)
        return remote(sz1.at[c, i], dst.at[c, i], z1_s.at[c, i], sem.at[c, i], right if to_right else left)

    def m_b1(c, p, to_right):
        i = p // M1
        place = y1_place(c, yy, p)
        return remote(place, place, (br1_s if to_right else bl1_s).at[c, i], b1_r.at[c, i], right if to_right else left)

    def m_a1(c, p, h):
        i = p // M1
        place = y1_place(c, h, p)
        return remote(place, place, a1_s.at[c, i], a1_r.at[c, i], ypeer)

    def m_z2(c, q, to_right):
        i = q // M2
        dst, sem = (rl2, l2_r) if to_right else (rr2, r2_r)
        return remote(sz2.at[c, i], dst.at[c, i], z2_s.at[c, i], sem.at[c, i], right if to_right else left)

    def m_y2(c, q):
        return remote(sy2.at[c], ry2.at[c], y2_s.at[c], y2_r.at[c], ypeer)

    def m_a2(c, q):
        place = y2_place(c, q)
        return remote(place, place, a2_s.at[c], a2_r.at[c], ypeer)

    def m_b2(c, q, to_right):
        i = q // M2
        place = y2_place(c, q)
        return remote(place, place, (br2_s if to_right else bl2_s).at[c, i], b2_r.at[c, i], right if to_right else left)

    def y_root(c, q):
        return lax.rem(lax.div(c, M2) + q // 2, 2) == yy

    def m_df(c, who):
        place = y.at[pl.ds(row0(c), R), pl.ds(col0(c, who), cw)]
        return remote(place, place, df_s.at[c], df_r.at[c], peer)

    def gate_up_wait(it):
        @pl.when(lax.rem(it, NJ) == 0)
        def _():
            x_copy(lax.div(it, NJ)).wait()

    def gate_up(it, first=None):
        s, j = lax.div(it, NJ), lax.rem(it, NJ)
        for b in range(uh // nb):
            block = j * (uh // nb) + b
            if first is not None:
                g_copy(first * (uh // nb) + b).wait()
                u_copy(first * (uh // nb) + b).wait()
            gate = jnp.dot(x[s], wg[block], preferred_element_type=F32)
            up = jnp.dot(x[s], wu[block], preferred_element_type=F32)
            hid[s, :, pl.ds(al(core * units + j * uh + b * nb, nb), nb)] = (jax.nn.gelu(gate) * up).astype(BF16)

    def down_wait(c):
        for j in range(NJ):

            @pl.when(c == j)
            def _():
                d_copy(j).wait()
                wd_msg(j).wait_recv()

        @pl.when(lax.rem(c, NJ) == 0)
        def _():
            for j in range(NJ):
                hid_msg(c + j).wait_recv()

    def down(c):
        s, j = lax.div(c, NJ), lax.rem(c, NJ)
        db = min(256, cw)
        for b in range(cw // db):
            cols = pl.ds(b * db, db)
            part[c, :, cols] = jnp.dot(hid[s], wd[j, :, cols], preferred_element_type=F32)

    def down_send(c):
        for p in range(len(ROOT1)):

            @pl.when(active(c, p, M1))
            def _():
                sy1[c, p // M1] = part1(c, 1 - yy, p)[...].astype(BF16)
                m_y1(c, p).start()

    def compute(it):
        for j in range(NJ):

            @pl.when(it == j)
            def _():
                gate_up_wait(it)
                gate_up(it, first=j)
                hid_msg(it).start()

        @pl.when((it >= NJ) & (it < n))
        def _():
            down_wait(it - NJ)
            gate_up_wait(it)
            down(it - NJ)
            gate_up(it)
            hid_msg(it).start()
            down_send(it - NJ)

        @pl.when((it >= n) & (it < n + NJ))
        def _():
            down_wait(it - NJ)
            down(it - NJ)
            down_send(it - NJ)

    def active(c, p, m):
        return True if m == 1 else lax.rem(c, m) == p % m

    def guarded(c, f, p=0, m=1):
        pl.when((c >= 0) & (c < n) & active(c, p, m))(lambda: f(c))

    def chain(c, k, base, lbuf, rbuf, sbuf, msg, root):
        if k > 0:

            @pl.when(z == 0)
            def _():
                sbuf[...] = base().astype(BF16)
                msg(True).start()

        if k < NZ - 1:

            @pl.when(z == NZ - 1)
            def _():
                sbuf[...] = base().astype(BF16)
                msg(False).start()

        if k > 1:

            @pl.when((z > 0) & (z < k))
            def _():
                msg(True).wait_recv()
                sbuf[...] = (base() + lbuf[...].astype(F32)).astype(BF16)
                msg(True).start()

        if k < NZ - 2:

            @pl.when((z < NZ - 1) & (z > k))
            def _():
                msg(False).wait_recv()
                sbuf[...] = (base() + rbuf[...].astype(F32)).astype(BF16)
                msg(False).start()

        pl.when(z == k)(root)

    def arrived(k, lbuf, rbuf, msg):
        total = 0.0
        if k > 0:
            msg(True).wait_recv()
            total = lbuf[...].astype(F32)
        if k < NZ - 1:
            msg(False).wait_recv()
            total = total + rbuf[...].astype(F32)
        return total

    def spread(k, msg):
        if k < NZ - 1:
            pl.when((z >= k) & (z < NZ - 1))(lambda: msg(True).start())
        if k > 0:
            pl.when((z <= k) & (z > 0))(lambda: msg(False).start())

    def reduce1(c, p):
        k = ROOT1[p]
        i = p // M1
        bufs = rl1.at[c, i], rr1.at[c, i]
        m_y1(c, p).wait_recv()

        def base():
            return part1(c, yy, p)[...] + ry1[c, i].astype(F32)

        def msg(to_right):
            return m_z1(c, p, to_right)

        def root():
            more = arrived(k, *bufs, msg)
            y1_place(c, yy, p)[...] = (base() + more).astype(BF16)
            spread(k, lambda to_right: m_b1(c, p, to_right))
            m_a1(c, p, yy).start()

        chain(c, k, base, *bufs, sz1.at[c, i], msg, root)

    def bcast1(c, p):
        k = ROOT1[p]

        @pl.when(z != k)
        def _():
            m_b1(c, p, True).wait_recv()
            spread(k, lambda to_right: m_b1(c, p, to_right))
            m_a1(c, p, yy).start()

    def reduce2(c, q):
        k = ROOT2[q]
        i = q // M2
        bufs = rl2.at[c, i], rr2.at[c, i]

        def base():
            return part2(c, q)[...]

        def msg(to_right):
            return m_z2(c, q, to_right)

        def root():
            @pl.when(jnp.logical_not(y_root(c, q)))
            def _():
                more = arrived(k, *bufs, msg)
                sy2[c] = (base() + more).astype(BF16)
                m_y2(c, q).start()

        chain(c, k, base, *bufs, sz2.at[c, i], msg, root)

    def cross2(c, q):
        k = ROOT2[q]
        i = q // M2

        @pl.when((z == k) & y_root(c, q))
        def _():
            more = arrived(k, rl2.at[c, i], rr2.at[c, i], lambda to_right: m_z2(c, q, to_right))
            m_y2(c, q).wait_recv()
            y2_place(c, q)[...] = (part2(c, q)[...] + more + ry2[c].astype(F32)).astype(BF16)
            m_a2(c, q).start()

    def bcast2(c, q):
        k = ROOT2[q]
        pl.when((z == k) & jnp.logical_not(y_root(c, q)))(lambda: m_a2(c, q).wait_recv())
        pl.when(z != k)(lambda: m_b2(c, q, True).wait_recv())
        spread(k, lambda to_right: m_b2(c, q, to_right))

    def finish(c):
        for p in range(len(ROOT1)):
            pl.when(active(c, p, M1))(lambda: m_a1(c, p, 1 - yy).wait_recv())
        m_df(c, core).start()

    def dist(k):
        return jnp.where(z < k, k - z, z - k)

    last = max(
        [NJ + HY + EB + HF + (HZ + HB) * _far(k) for k in ROOT1]
        + [NJ + 2 * HX + EB + (HZ + HB) * _far(k) for k in ROOT2]
    )

    def step(it, carry):
        compute(it)
        for p, k in enumerate(ROOT1):
            guarded(it - (NJ + HY) - HZ * _hops(z, k), functools.partial(reduce1, p=p), p, M1)
        for q, k in enumerate(ROOT2):
            guarded(it - NJ - HZ * _hops(z, k), functools.partial(reduce2, q=q), q, M2)
        for q, k in enumerate(ROOT2):
            guarded(it - (NJ + HX) - HZ * _far(k), functools.partial(cross2, q=q), q, M2)
        for p, k in enumerate(ROOT1):
            guarded(it - (NJ + HY + EB) - HZ * _far(k) - HB * dist(k), functools.partial(bcast1, p=p), p, M1)
        for q, k in enumerate(ROOT2):
            guarded(it - (NJ + 2 * HX + EB) - HZ * _far(k) - HB * dist(k), functools.partial(bcast2, q=q), q, M2)
        guarded(it - last, finish)
        return carry

    lax.fori_loop(0, n + last, step, 0)

    for j in range(NJ):
        wd_msg(j).wait_send()

    def drain(c, carry):
        hid_msg(c).wait_send()
        for p, k in enumerate(ROOT1):

            @pl.when(active(c, p, M1))
            def _():
                m_y1(c, p).wait_send()
                pl.when(z != k)(lambda: m_z1(c, p, True).wait_send())
                if k < NZ - 1:
                    pl.when((z >= k) & (z < NZ - 1))(lambda: m_b1(c, p, True).wait_send())
                if k > 0:
                    pl.when((z <= k) & (z > 0))(lambda: m_b1(c, p, False).wait_send())
                m_a1(c, p, yy).wait_send()

        for q, k in enumerate(ROOT2):

            @pl.when(active(c, q, M2))
            def _():
                pl.when(z != k)(lambda: m_z2(c, q, True).wait_send())
                pl.when((z == k) & jnp.logical_not(y_root(c, q)))(lambda: m_y2(c, q).wait_send())
                pl.when((z == k) & y_root(c, q))(lambda: m_a2(c, q).wait_send())
                if k < NZ - 1:
                    pl.when((z >= k) & (z < NZ - 1))(lambda: m_b2(c, q, True).wait_send())
                if k > 0:
                    pl.when((z <= k) & (z > 0))(lambda: m_b2(c, q, False).wait_send())

        m_df(c, core).wait_send()
        m_df(c, 1 - core).wait_recv()
        return carry

    lax.fori_loop(0, n, drain, 0)


def block(x, w_gate, w_up, w_down):
    rows, width = x.shape
    units = w_gate.shape[1]
    n_super = rows // R
    n = NJ * n_super
    cw = width // 2 // NJ
    n1, n2 = len(ROOT1) // M1, len(ROOT2) // M2
    w1, w2 = cw // 2 // n1, cw // n2
    nb = min(256, units // NJ)
    blocks = units // nb
    dma = pltpu.SemaphoreType.DMA
    one = pltpu.VMEM((n, n1, R1, w1), BF16)
    two = pltpu.VMEM((n, n2, R2, w2), BF16)
    cross = pltpu.VMEM((n, R2, w2), BF16)
    return pl.pallas_call(
        kernel,
        out_shape=pltpu.VMEM((rows, width), BF16),
        in_specs=[pl.BlockSpec(memory_space=pl.ANY)] * 4,
        out_specs=pl.BlockSpec(memory_space=pltpu.VMEM),
        scratch_shapes=[
            pltpu.VMEM((n_super, R, width), BF16),
            pltpu.VMEM((blocks, width, nb), BF16),
            pltpu.VMEM((blocks, width, nb), BF16),
            pltpu.VMEM((NJ, 2 * units, cw), BF16),
            pltpu.VMEM((n_super, R, 2 * units), BF16),
            pltpu.VMEM((n, R, cw), F32),
            one, one, one, one, one, two, two, two, cross, cross,
            dma((n_super + 2 * blocks + NJ,)), dma((NJ,)), dma((NJ,)), dma((n,)), dma((n,)),
            *[dma((n, n1))] * 10,
            *[dma((n, n2))] * 3, *[dma((n,))] * 4, *[dma((n, n2))] * 3,
            dma((n,)), dma((n,)),
        ],
        compiler_params=pltpu.CompilerParams(
            collective_id=0, has_side_effects=True, vmem_limit_bytes=52 * 1024 * 1024
        ),
    )(x, w_gate, w_up, w_down)


def solution(mesh):
    return jax.shard_map(
        block,
        mesh=mesh,
        in_specs=(P("dp", None), P(None, "tp"), P(None, "tp"), P("tp", None)),
        out_specs=P("dp", None),
        check_vma=False,
    )
```

```python
import functools

import jax
import jax.numpy as jnp
from jax import lax
from jax.experimental import pallas as pl
from jax.experimental.pallas import tpu as pltpu
from jax.sharding import PartitionSpec as P

F32, BF16 = jnp.float32, jnp.bfloat16

R = 256
R1, R2 = 192, 64
NJ = 2
ROOT2 = (0, 1, 2, 3)
M2 = 1
NZ = 4
HY, HC, HE, HO, HF = 2, 2, 2, 2, 1
HZ, HX, HB, E2 = 1, 3, 3, 1
ORDER = "zscxeob"


def _far(k):
    return max(k, NZ - 1 - k)


def _hops(z, k):
    return jnp.where(z < k, z, jnp.where(z > k, NZ - 1 - z, _far(k)))


def kernel(
    x_hbm, wg_hbm, wu_hbm, wd_hbm, y,
    x, wg, wu, wd, hid, part,
    sy1, ry1, s1, r_in, r_ex, s2, rl2, rr2, ry2,
    in_sem, wd_s, wd_r, hid_s, hid_r,
    y1_s, y1_r, z1_s, in_r, ex_r, o1_s, o1_r, a1_s, a1_r, y2_s, y2_r, df_s, df_r,
    z2_s, l2_r, r2_r, bl2_s, br2_s, b2_r,
):
    rows, width = y.shape
    n_super = rows // R
    n = NJ * n_super
    half = width // 2
    cw = half // NJ
    units = wg_hbm.shape[1]
    uh = units // NJ
    nb = min(256, uh)
    blocks = units // nb
    w1 = cw // 2
    w2 = cw * M2 // len(ROOT2)

    me = lax.axis_index("tp")
    core = lax.rem(me, 2)
    z = lax.rem(lax.div(me, 2), NZ)
    yy = lax.div(me, 2 * NZ)
    peer = {"tp": me + 1 - 2 * core}
    ypeer = {"tp": lax.rem(me + 2 * NZ, 4 * NZ)}
    left = {"tp": me - 2}
    right = {"tp": me + 2}
    outer = (z == 0) | (z == NZ - 1)
    step_in = jnp.where(z < NZ // 2, 2, -2)
    inward = {"tp": me + step_in}
    outward = {"tp": me - step_in}

    def load(i, src, dst):
        return pltpu.make_async_copy(src, dst, in_sem.at[i])

    def al(v, m):
        return pl.multiple_of(v, m)

    def x_copy(s):
        return load(s, x_hbm.at[pl.ds(al(s * R, R), R)], x.at[s])

    def g_copy(b):
        return load(n_super + b, wg_hbm.at[:, pl.ds(b * nb, nb)], wg.at[b])

    def u_copy(b):
        return load(n_super + blocks + b, wu_hbm.at[:, pl.ds(b * nb, nb)], wu.at[b])

    def d_copy(j):
        return load(
            n_super + 2 * blocks + j,
            wd_hbm.at[:, pl.ds(al(core * half + j * cw, cw), cw)],
            wd.at[j, pl.ds(al(core * units, units), units)],
        )

    def remote(src, dst, ssem, rsem, dev):
        return pltpu.make_async_remote_copy(
            src_ref=src, dst_ref=dst, send_sem=ssem, recv_sem=rsem,
            device_id=dev, device_id_type=pl.DeviceIdType.MESH,
        )

    x_copy(0).start()
    for b in range(blocks):
        g_copy(b).start()
        u_copy(b).start()
    for j in range(NJ):
        d_copy(j).start()
    x_copy(1).start()

    barrier = pltpu.get_barrier_semaphore()

    def hello(dev):
        pl.semaphore_signal(barrier, inc=1, device_id=dev, device_id_type=pl.DeviceIdType.MESH)

    hello(peer)
    hello(ypeer)
    pl.when(z > 0)(lambda: hello(left))
    pl.when(z < NZ - 1)(lambda: hello(right))
    pl.semaphore_wait(barrier, 2 + jnp.minimum(z, 1) + jnp.minimum(NZ - 1 - z, 1))

    def wd_msg(j):
        return remote(
            wd_hbm.at[:, pl.ds(al((1 - core) * half + j * cw, cw), cw)],
            wd.at[j, pl.ds(al(core * units, units), units)],
            wd_s.at[j], wd_r.at[j], peer,
        )

    for j in range(NJ):
        wd_msg(j).start()
    for s in range(2, n_super):
        x_copy(s).start()

    def hid_msg(c):
        s, j = lax.div(c, NJ), lax.rem(c, NJ)
        place = hid.at[s, :, pl.ds(al(core * units + j * uh, uh), uh)]
        return remote(place, place, hid_s.at[c], hid_r.at[c], peer)

    def row0(c):
        return al(lax.div(c, NJ) * R, R)

    def col0(c, who):
        return al(who * half + lax.rem(c, NJ) * cw, cw)

    def y1_place(c, h):
        return y.at[pl.ds(row0(c), R1), pl.ds(al(col0(c, core) + h * w1, w1), w1)]

    def y2_place(c, q):
        return y.at[pl.ds(al(row0(c) + R1, 16), R2), pl.ds(al(col0(c, core) + q // M2 * w2, w2), w2)]

    def part1(c, h):
        return part.at[c, pl.ds(0, R1), pl.ds(al(h * w1, w1), w1)]

    def part2(c, q):
        return part.at[c, pl.ds(R1, R2), pl.ds(q // M2 * w2, w2)]

    def m_y1(c):
        return remote(sy1.at[c], ry1.at[c], y1_s.at[c], y1_r.at[c], ypeer)

    def m_in(c):
        return remote(s1.at[c], r_in.at[c], z1_s.at[c], in_r.at[c], inward)

    def m_ex(c):
        return remote(s1.at[c], r_ex.at[c], z1_s.at[c], ex_r.at[c], inward)

    def m_o1(c):
        place = y1_place(c, yy)
        return remote(place, place, o1_s.at[c], o1_r.at[c], outward)

    def m_a1(c, h):
        place = y1_place(c, h)
        return remote(place, place, a1_s.at[c], a1_r.at[c], ypeer)

    def m_z2(c, q, to_right):
        i = q // M2
        dst, sem = (rl2, l2_r) if to_right else (rr2, r2_r)
        return remote(s2.at[c, i], dst.at[c, i], z2_s.at[c, i], sem.at[c, i], right if to_right else left)

    def m_y2(c, q):
        return remote(s2.at[c, q // M2], ry2.at[c], y2_s.at[c], y2_r.at[c], ypeer)

    def m_b2(c, q, to_right):
        i = q // M2
        place = y2_place(c, q)
        return remote(place, place, (br2_s if to_right else bl2_s).at[c, i], b2_r.at[c, i], right if to_right else left)

    def m_df(c, who):
        place = y.at[pl.ds(row0(c), R), pl.ds(col0(c, who), cw)]
        return remote(place, place, df_s.at[c], df_r.at[c], peer)

    def gate_up_wait(it):
        @pl.when(lax.rem(it, NJ) == 0)
        def _():
            x_copy(lax.div(it, NJ)).wait()

    def gate_up(it, first=None):
        s, j = lax.div(it, NJ), lax.rem(it, NJ)
        for b in range(uh // nb):
            block = j * (uh // nb) + b
            if first is not None:
                g_copy(first * (uh // nb) + b).wait()
                u_copy(first * (uh // nb) + b).wait()
            gate = jnp.dot(x[s], wg[block], preferred_element_type=F32)
            up = jnp.dot(x[s], wu[block], preferred_element_type=F32)
            hid[s, :, pl.ds(al(core * units + j * uh + b * nb, nb), nb)] = (jax.nn.gelu(gate) * up).astype(BF16)

    def down_wait(c):
        for j in range(NJ):

            @pl.when(c == j)
            def _():
                d_copy(j).wait()
                wd_msg(j).wait_recv()

        @pl.when(lax.rem(c, NJ) == 0)
        def _():
            for j in range(NJ):
                hid_msg(c + j).wait_recv()

    def down(c):
        s, j = lax.div(c, NJ), lax.rem(c, NJ)
        db = min(256, cw)
        for b in range(cw // db):
            cols = pl.ds(b * db, db)
            part[c, :, cols] = jnp.dot(hid[s], wd[j, :, cols], preferred_element_type=F32)

    def down_send(c):
        sy1[c] = part1(c, 1 - yy)[...].astype(BF16)
        m_y1(c).start()

    def compute(it):
        for j in range(NJ):

            @pl.when(it == j)
            def _():
                gate_up_wait(it)
                gate_up(it, first=j)
                hid_msg(it).start()

        @pl.when((it >= NJ) & (it < n))
        def _():
            down_wait(it - NJ)
            gate_up_wait(it)
            down(it - NJ)
            gate_up(it)
            hid_msg(it).start()
            down_send(it - NJ)

        @pl.when((it >= n) & (it < n + NJ))
        def _():
            down_wait(it - NJ)
            down(it - NJ)
            down_send(it - NJ)

    def active(c, p, m):
        return True if m == 1 else lax.rem(c, m) == p % m

    def guarded(c, f, p=0, m=1):
        pl.when((c >= 0) & (c < n) & active(c, p, m))(lambda: f(c))

    def chain(c, k, base, lbuf, rbuf, sbuf, msg, root):
        if k > 0:

            @pl.when(z == 0)
            def _():
                sbuf[...] = base().astype(BF16)
                msg(True).start()

        if k < NZ - 1:

            @pl.when(z == NZ - 1)
            def _():
                sbuf[...] = base().astype(BF16)
                msg(False).start()

        if k > 1:

            @pl.when((z > 0) & (z < k))
            def _():
                msg(True).wait_recv()
                sbuf[...] = (base() + lbuf[...].astype(F32)).astype(BF16)
                msg(True).start()

        if k < NZ - 2:

            @pl.when((z < NZ - 1) & (z > k))
            def _():
                msg(False).wait_recv()
                sbuf[...] = (base() + rbuf[...].astype(F32)).astype(BF16)
                msg(False).start()

        pl.when(z == k)(root)

    def arrived(k, lbuf, rbuf, msg):
        total = 0.0
        if k > 0:
            msg(True).wait_recv()
            total = lbuf[...].astype(F32)
        if k < NZ - 1:
            msg(False).wait_recv()
            total = total + rbuf[...].astype(F32)
        return total

    def spread(k, msg):
        if k < NZ - 1:
            pl.when((z >= k) & (z < NZ - 1))(lambda: msg(True).start())
        if k > 0:
            pl.when((z <= k) & (z > 0))(lambda: msg(False).start())

    def outer_in(c):
        m_y1(c).wait_recv()
        s1[c] = (part1(c, yy)[...] + ry1[c].astype(F32)).astype(BF16)
        m_in(c).start()

    def centre_sum(c):
        m_y1(c).wait_recv()
        m_in(c).wait_recv()
        s1[c] = (part1(c, yy)[...] + ry1[c].astype(F32) + r_in[c].astype(F32)).astype(BF16)
        m_ex(c).start()

    def centre_out(c):
        m_ex(c).wait_recv()
        y1_place(c, yy)[...] = (s1[c].astype(F32) + r_ex[c].astype(F32)).astype(BF16)
        m_o1(c).start()
        m_a1(c, yy).start()

    def outer_out(c):
        m_o1(c).wait_recv()
        m_a1(c, yy).start()

    def reduce2(c, q):
        k = ROOT2[q]
        i = q // M2
        bufs = rl2.at[c, i], rr2.at[c, i]

        def base():
            return part2(c, q)[...]

        def msg(to_right):
            return m_z2(c, q, to_right)

        def root():
            more = arrived(k, *bufs, msg)
            s2[c, i] = (base() + more).astype(BF16)
            m_y2(c, q).start()

        chain(c, k, base, *bufs, s2.at[c, i], msg, root)

    def cross2(c, q):
        k = ROOT2[q]

        @pl.when(z == k)
        def _():
            m_y2(c, q).wait_recv()
            y2_place(c, q)[...] = (s2[c, q // M2].astype(F32) + ry2[c].astype(F32)).astype(BF16)
            spread(k, lambda to_right: m_b2(c, q, to_right))

    def bcast2(c, q):
        k = ROOT2[q]

        @pl.when(z != k)
        def _():
            m_b2(c, q, True).wait_recv()
            spread(k, lambda to_right: m_b2(c, q, to_right))

    def finish(c):
        m_a1(c, 1 - yy).wait_recv()
        m_df(c, core).start()

    def dist(k):
        return jnp.where(z < k, k - z, z - k)

    def when_in(c, cond, f):
        pl.when((c >= 0) & (c < n) & cond)(lambda: f(c))

    at_in = NJ + HY
    at_sum = at_in + HC
    at_out = at_sum + HE
    at_end = at_out + HO
    last = max([at_end + HF] + [NJ + HX + E2 + (HZ + HB) * _far(k) for k in ROOT2])
    centre = jnp.logical_not(outer)

    def second(it, lag, f):
        for q, k in enumerate(ROOT2):
            guarded(it - lag(k), functools.partial(f, q=q), q, M2)

    def step(it, carry):
        compute(it)
        for name in ORDER:
            if name == "s":
                when_in(it - at_in, outer, outer_in)
            if name == "c":
                when_in(it - at_sum, centre, centre_sum)
            if name == "e":
                when_in(it - at_out, centre, centre_out)
            if name == "o":
                when_in(it - at_end, outer, outer_out)
            if name == "z":
                second(it, lambda k: NJ + HZ * _hops(z, k), reduce2)
            if name == "x":
                second(it, lambda k: NJ + HX + HZ * _far(k), cross2)
            if name == "b":
                second(it, lambda k: NJ + HX + E2 + HZ * _far(k) + HB * dist(k), bcast2)
        guarded(it - last, finish)
        return carry

    lax.fori_loop(0, n + last, step, 0)

    for j in range(NJ):
        wd_msg(j).wait_send()

    def drain(c, carry):
        hid_msg(c).wait_send()
        m_y1(c).wait_send()
        m_in(c).wait_send()
        pl.when(centre)(lambda: m_o1(c).wait_send())
        m_a1(c, yy).wait_send()
        for q, k in enumerate(ROOT2):

            @pl.when(active(c, q, M2))
            def _():
                pl.when(z != k)(lambda: m_z2(c, q, True).wait_send())
                pl.when(z == k)(lambda: m_y2(c, q).wait_send())
                if k < NZ - 1:
                    pl.when((z >= k) & (z < NZ - 1))(lambda: m_b2(c, q, True).wait_send())
                if k > 0:
                    pl.when((z <= k) & (z > 0))(lambda: m_b2(c, q, False).wait_send())

        m_df(c, core).wait_send()
        m_df(c, 1 - core).wait_recv()
        return carry

    lax.fori_loop(0, n, drain, 0)


def block(x, w_gate, w_up, w_down):
    rows, width = x.shape
    units = w_gate.shape[1]
    n_super = rows // R
    n = NJ * n_super
    cw = width // 2 // NJ
    n2 = len(ROOT2) // M2
    w1, w2 = cw // 2, cw // n2
    nb = min(256, units // NJ)
    blocks = units // nb
    dma = pltpu.SemaphoreType.DMA
    one = pltpu.VMEM((n, R1, w1), BF16)
    two = pltpu.VMEM((n, n2, R2, w2), BF16)
    cross = pltpu.VMEM((n, R2, w2), BF16)
    return pl.pallas_call(
        kernel,
        out_shape=pltpu.VMEM((rows, width), BF16),
        in_specs=[pl.BlockSpec(memory_space=pl.ANY)] * 4,
        out_specs=pl.BlockSpec(memory_space=pltpu.VMEM),
        scratch_shapes=[
            pltpu.VMEM((n_super, R, width), BF16),
            pltpu.VMEM((blocks, width, nb), BF16),
            pltpu.VMEM((blocks, width, nb), BF16),
            pltpu.VMEM((NJ, 2 * units, cw), BF16),
            pltpu.VMEM((n_super, R, 2 * units), BF16),
            pltpu.VMEM((n, R, cw), F32),
            one, one, one, one, one, two, two, two, cross,
            dma((n_super + 2 * blocks + NJ,)), dma((NJ,)), dma((NJ,)), dma((n,)), dma((n,)),
            *[dma((n,))] * 13,
            *[dma((n, n2))] * 6,
        ],
        compiler_params=pltpu.CompilerParams(
            collective_id=0, has_side_effects=True, vmem_limit_bytes=52 * 1024 * 1024
        ),
    )(x, w_gate, w_up, w_down)


def solution(mesh):
    return jax.shard_map(
        block,
        mesh=mesh,
        in_specs=(P("dp", None), P(None, "tp"), P(None, "tp"), P("tp", None)),
        out_specs=P("dp", None),
        check_vma=False,
    )
```

```python
import functools

import jax
import jax.numpy as jnp
from jax import lax
from jax.experimental import pallas as pl
from jax.experimental.pallas import tpu as pltpu
from jax.sharding import PartitionSpec as P

F32, BF16 = jnp.float32, jnp.bfloat16

R = 256
R1, R2 = 192, 64
NJ = 2
ROOT2 = (0, 3, 1, 2)
M2 = 4
NZ = 4
HY, HC, HE, HO, HF = 3, 2, 2, 2, 1
HZ, HX, HB, E2 = 2, 3, 2, 0
ORDER = "sczexob"


def _far(k):
    return max(k, NZ - 1 - k)


def _hops(z, k):
    return jnp.where(z < k, z, jnp.where(z > k, NZ - 1 - z, _far(k)))


def kernel(
    x_hbm, wg_hbm, wu_hbm, wd_hbm, y,
    x, wg, wu, wd, hid, part,
    sy1, ry1, s1, r_in, r_ex, s2, rl2, rr2, ry2,
    in_sem, wd_s, wd_r, hid_s, hid_r,
    y1_s, y1_r, z1_s, in_r, ex_r, o1_s, o1_r, a1_s, a1_r, y2_s, y2_r, df_s, df_r,
    z2_s, l2_r, r2_r, bl2_s, br2_s, b2_r,
):
    rows, width = y.shape
    n_super = rows // R
    n = NJ * n_super
    half = width // 2
    cw = half // NJ
    units = wg_hbm.shape[1]
    uh = units // NJ
    nb = min(256, uh)
    blocks = units // nb
    w1 = cw // 2
    w2 = cw * M2 // len(ROOT2)

    me = lax.axis_index("tp")
    core = lax.rem(me, 2)
    z = lax.rem(lax.div(me, 2), NZ)
    yy = lax.div(me, 2 * NZ)
    peer = {"tp": me + 1 - 2 * core}
    ypeer = {"tp": lax.rem(me + 2 * NZ, 4 * NZ)}
    left = {"tp": me - 2}
    right = {"tp": me + 2}
    outer = (z == 0) | (z == NZ - 1)
    step_in = jnp.where(z < NZ // 2, 2, -2)
    inward = {"tp": me + step_in}
    outward = {"tp": me - step_in}

    def load(i, src, dst):
        return pltpu.make_async_copy(src, dst, in_sem.at[i])

    def al(v, m):
        return pl.multiple_of(v, m)

    def x_copy(s):
        return load(s, x_hbm.at[pl.ds(al(s * R, R), R)], x.at[s])

    def g_copy(b):
        return load(n_super + b, wg_hbm.at[:, pl.ds(b * nb, nb)], wg.at[b])

    def u_copy(b):
        return load(n_super + blocks + b, wu_hbm.at[:, pl.ds(b * nb, nb)], wu.at[b])

    def d_copy(j):
        return load(
            n_super + 2 * blocks + j,
            wd_hbm.at[:, pl.ds(al(core * half + j * cw, cw), cw)],
            wd.at[j, pl.ds(al(core * units, units), units)],
        )

    def remote(src, dst, ssem, rsem, dev):
        return pltpu.make_async_remote_copy(
            src_ref=src, dst_ref=dst, send_sem=ssem, recv_sem=rsem,
            device_id=dev, device_id_type=pl.DeviceIdType.MESH,
        )

    x_copy(0).start()
    for b in range(blocks):
        g_copy(b).start()
        u_copy(b).start()
    for j in range(NJ):
        d_copy(j).start()
    x_copy(1).start()

    barrier = pltpu.get_barrier_semaphore()

    def hello(dev):
        pl.semaphore_signal(barrier, inc=1, device_id=dev, device_id_type=pl.DeviceIdType.MESH)

    hello(peer)
    hello(ypeer)
    pl.when(z > 0)(lambda: hello(left))
    pl.when(z < NZ - 1)(lambda: hello(right))
    pl.semaphore_wait(barrier, 2 + jnp.minimum(z, 1) + jnp.minimum(NZ - 1 - z, 1))

    def wd_msg(j):
        return remote(
            wd_hbm.at[:, pl.ds(al((1 - core) * half + j * cw, cw), cw)],
            wd.at[j, pl.ds(al(core * units, units), units)],
            wd_s.at[j], wd_r.at[j], peer,
        )

    for j in range(NJ):
        wd_msg(j).start()
    for s in range(2, n_super):
        x_copy(s).start()

    def hid_msg(c):
        s, j = lax.div(c, NJ), lax.rem(c, NJ)
        place = hid.at[s, :, pl.ds(al(core * units + j * uh, uh), uh)]
        return remote(place, place, hid_s.at[c], hid_r.at[c], peer)

    def row0(c):
        return al(lax.div(c, NJ) * R, R)

    def col0(c, who):
        return al(who * half + lax.rem(c, NJ) * cw, cw)

    def y1_place(c, h):
        return y.at[pl.ds(row0(c), R1), pl.ds(al(col0(c, core) + h * w1, w1), w1)]

    def y2_place(c, q):
        return y.at[pl.ds(al(row0(c) + R1, 16), R2), pl.ds(al(col0(c, core) + q // M2 * w2, w2), w2)]

    def part1(c, h):
        return part.at[c, pl.ds(0, R1), pl.ds(al(h * w1, w1), w1)]

    def part2(c, q):
        return part.at[c, pl.ds(R1, R2), pl.ds(q // M2 * w2, w2)]

    def m_y1(c):
        return remote(sy1.at[c], ry1.at[c], y1_s.at[c], y1_r.at[c], ypeer)

    def m_in(c):
        return remote(s1.at[c], r_in.at[c], z1_s.at[c], in_r.at[c], inward)

    def m_ex(c):
        return remote(s1.at[c], r_ex.at[c], z1_s.at[c], ex_r.at[c], inward)

    def m_o1(c):
        place = y1_place(c, yy)
        return remote(place, place, o1_s.at[c], o1_r.at[c], outward)

    def m_a1(c, h):
        place = y1_place(c, h)
        return remote(place, place, a1_s.at[c], a1_r.at[c], ypeer)

    def m_z2(c, q, to_right):
        i = q // M2
        dst, sem = (rl2, l2_r) if to_right else (rr2, r2_r)
        return remote(s2.at[c, i], dst.at[c, i], z2_s.at[c, i], sem.at[c, i], right if to_right else left)

    def m_y2(c, q):
        return remote(s2.at[c, q // M2], ry2.at[c], y2_s.at[c], y2_r.at[c], ypeer)

    def m_b2(c, q, to_right):
        i = q // M2
        place = y2_place(c, q)
        return remote(place, place, (br2_s if to_right else bl2_s).at[c, i], b2_r.at[c, i], right if to_right else left)

    def m_df(c, who):
        place = y.at[pl.ds(row0(c), R), pl.ds(col0(c, who), cw)]
        return remote(place, place, df_s.at[c], df_r.at[c], peer)

    def gate_up_wait(it):
        @pl.when(lax.rem(it, NJ) == 0)
        def _():
            x_copy(lax.div(it, NJ)).wait()

    def gate_up(it, first=None):
        s, j = lax.div(it, NJ), lax.rem(it, NJ)
        for b in range(uh // nb):
            block = j * (uh // nb) + b
            if first is not None:
                g_copy(first * (uh // nb) + b).wait()
                u_copy(first * (uh // nb) + b).wait()
            gate = jnp.dot(x[s], wg[block], preferred_element_type=F32)
            up = jnp.dot(x[s], wu[block], preferred_element_type=F32)
            hid[s, :, pl.ds(al(core * units + j * uh + b * nb, nb), nb)] = (jax.nn.gelu(gate) * up).astype(BF16)

    def down_wait(c):
        for j in range(NJ):

            @pl.when(c == j)
            def _():
                d_copy(j).wait()
                wd_msg(j).wait_recv()

        @pl.when(lax.rem(c, NJ) == 0)
        def _():
            for j in range(NJ):
                hid_msg(c + j).wait_recv()

    def down(c):
        s, j = lax.div(c, NJ), lax.rem(c, NJ)
        db = min(256, cw)
        for b in range(cw // db):
            cols = pl.ds(b * db, db)
            part[c, :, cols] = jnp.dot(hid[s], wd[j, :, cols], preferred_element_type=F32)

    def down_send(c):
        sy1[c] = part1(c, 1 - yy)[...].astype(BF16)
        m_y1(c).start()

    def compute(it):
        for j in range(NJ):

            @pl.when(it == j)
            def _():
                gate_up_wait(it)
                gate_up(it, first=j)
                hid_msg(it).start()

        @pl.when((it >= NJ) & (it < n))
        def _():
            down_wait(it - NJ)
            gate_up_wait(it)
            down(it - NJ)
            gate_up(it)
            hid_msg(it).start()
            down_send(it - NJ)

        @pl.when((it >= n) & (it < n + NJ))
        def _():
            down_wait(it - NJ)
            down(it - NJ)
            down_send(it - NJ)

    def active(c, p, m):
        return True if m == 1 else lax.rem(c, m) == p % m

    def guarded(c, f, p=0, m=1):
        pl.when((c >= 0) & (c < n) & active(c, p, m))(lambda: f(c))

    def chain(c, k, base, lbuf, rbuf, sbuf, msg, root):
        if k > 0:

            @pl.when(z == 0)
            def _():
                sbuf[...] = base().astype(BF16)
                msg(True).start()

        if k < NZ - 1:

            @pl.when(z == NZ - 1)
            def _():
                sbuf[...] = base().astype(BF16)
                msg(False).start()

        if k > 1:

            @pl.when((z > 0) & (z < k))
            def _():
                msg(True).wait_recv()
                sbuf[...] = (base() + lbuf[...].astype(F32)).astype(BF16)
                msg(True).start()

        if k < NZ - 2:

            @pl.when((z < NZ - 1) & (z > k))
            def _():
                msg(False).wait_recv()
                sbuf[...] = (base() + rbuf[...].astype(F32)).astype(BF16)
                msg(False).start()

        pl.when(z == k)(root)

    def arrived(k, lbuf, rbuf, msg):
        total = 0.0
        if k > 0:
            msg(True).wait_recv()
            total = lbuf[...].astype(F32)
        if k < NZ - 1:
            msg(False).wait_recv()
            total = total + rbuf[...].astype(F32)
        return total

    def spread(k, msg):
        if k < NZ - 1:
            pl.when((z >= k) & (z < NZ - 1))(lambda: msg(True).start())
        if k > 0:
            pl.when((z <= k) & (z > 0))(lambda: msg(False).start())

    def outer_in(c):
        m_y1(c).wait_recv()
        s1[c] = (part1(c, yy)[...] + ry1[c].astype(F32)).astype(BF16)
        m_in(c).start()

    def centre_sum(c):
        m_y1(c).wait_recv()
        m_in(c).wait_recv()
        s1[c] = (part1(c, yy)[...] + ry1[c].astype(F32) + r_in[c].astype(F32)).astype(BF16)
        m_ex(c).start()

    def centre_out(c):
        m_ex(c).wait_recv()
        y1_place(c, yy)[...] = (s1[c].astype(F32) + r_ex[c].astype(F32)).astype(BF16)
        m_o1(c).start()
        m_a1(c, yy).start()

    def outer_out(c):
        m_o1(c).wait_recv()
        m_a1(c, yy).start()

    def reduce2(c, q):
        k = ROOT2[q]
        i = q // M2
        bufs = rl2.at[c, i], rr2.at[c, i]

        def base():
            return part2(c, q)[...]

        def msg(to_right):
            return m_z2(c, q, to_right)

        def root():
            more = arrived(k, *bufs, msg)
            s2[c, i] = (base() + more).astype(BF16)
            m_y2(c, q).start()

        chain(c, k, base, *bufs, s2.at[c, i], msg, root)

    def cross2(c, q):
        k = ROOT2[q]

        @pl.when(z == k)
        def _():
            m_y2(c, q).wait_recv()
            y2_place(c, q)[...] = (s2[c, q // M2].astype(F32) + ry2[c].astype(F32)).astype(BF16)
            spread(k, lambda to_right: m_b2(c, q, to_right))

    def bcast2(c, q):
        k = ROOT2[q]

        @pl.when(z != k)
        def _():
            m_b2(c, q, True).wait_recv()
            spread(k, lambda to_right: m_b2(c, q, to_right))

    def finish(c):
        m_a1(c, 1 - yy).wait_recv()
        m_df(c, core).start()

    def dist(k):
        return jnp.where(z < k, k - z, z - k)

    def when_in(c, cond, f):
        pl.when((c >= 0) & (c < n) & cond)(lambda: f(c))

    at_in = NJ + HY
    at_sum = at_in + HC
    at_out = at_sum + HE
    at_end = at_out + HO
    last = max([at_end + HF] + [NJ + HX + E2 + (HZ + HB) * _far(k) for k in ROOT2])
    centre = jnp.logical_not(outer)

    def second(it, lag, f):
        for q, k in enumerate(ROOT2):
            guarded(it - lag(k), functools.partial(f, q=q), q, M2)

    def step(it, carry):
        compute(it)
        for name in ORDER:
            if name == "s":
                when_in(it - at_in, outer, outer_in)
            if name == "c":
                when_in(it - at_sum, centre, centre_sum)
            if name == "e":
                when_in(it - at_out, centre, centre_out)
            if name == "o":
                when_in(it - at_end, outer, outer_out)
            if name == "z":
                second(it, lambda k: NJ + HZ * _hops(z, k), reduce2)
            if name == "x":
                second(it, lambda k: NJ + HX + HZ * _far(k), cross2)
            if name == "b":
                second(it, lambda k: NJ + HX + E2 + HZ * _far(k) + HB * dist(k), bcast2)
        guarded(it - last, finish)
        return carry

    lax.fori_loop(0, n + last, step, 0)

    for j in range(NJ):
        wd_msg(j).wait_send()

    def drain(c, carry):
        hid_msg(c).wait_send()
        m_y1(c).wait_send()
        m_in(c).wait_send()
        pl.when(centre)(lambda: m_o1(c).wait_send())
        m_a1(c, yy).wait_send()
        for q, k in enumerate(ROOT2):

            @pl.when(active(c, q, M2))
            def _():
                pl.when(z != k)(lambda: m_z2(c, q, True).wait_send())
                pl.when(z == k)(lambda: m_y2(c, q).wait_send())
                if k < NZ - 1:
                    pl.when((z >= k) & (z < NZ - 1))(lambda: m_b2(c, q, True).wait_send())
                if k > 0:
                    pl.when((z <= k) & (z > 0))(lambda: m_b2(c, q, False).wait_send())

        m_df(c, core).wait_send()
        m_df(c, 1 - core).wait_recv()
        return carry

    lax.fori_loop(0, n, drain, 0)


def block(x, w_gate, w_up, w_down):
    rows, width = x.shape
    units = w_gate.shape[1]
    n_super = rows // R
    n = NJ * n_super
    cw = width // 2 // NJ
    n2 = len(ROOT2) // M2
    w1, w2 = cw // 2, cw // n2
    nb = min(256, units // NJ)
    blocks = units // nb
    dma = pltpu.SemaphoreType.DMA
    one = pltpu.VMEM((n, R1, w1), BF16)
    two = pltpu.VMEM((n, n2, R2, w2), BF16)
    cross = pltpu.VMEM((n, R2, w2), BF16)
    return pl.pallas_call(
        kernel,
        out_shape=pltpu.VMEM((rows, width), BF16),
        in_specs=[pl.BlockSpec(memory_space=pl.ANY)] * 4,
        out_specs=pl.BlockSpec(memory_space=pltpu.VMEM),
        scratch_shapes=[
            pltpu.VMEM((n_super, R, width), BF16),
            pltpu.VMEM((blocks, width, nb), BF16),
            pltpu.VMEM((blocks, width, nb), BF16),
            pltpu.VMEM((NJ, 2 * units, cw), BF16),
            pltpu.VMEM((n_super, R, 2 * units), BF16),
            pltpu.VMEM((n, R, cw), F32),
            one, one, one, one, one, two, two, two, cross,
            dma((n_super + 2 * blocks + NJ,)), dma((NJ,)), dma((NJ,)), dma((n,)), dma((n,)),
            *[dma((n,))] * 13,
            *[dma((n, n2))] * 6,
        ],
        compiler_params=pltpu.CompilerParams(
            collective_id=0, has_side_effects=True, vmem_limit_bytes=52 * 1024 * 1024
        ),
    )(x, w_gate, w_up, w_down)


def solution(mesh):
    return jax.shard_map(
        block,
        mesh=mesh,
        in_specs=(P("dp", None), P(None, "tp"), P(None, "tp"), P("tp", None)),
        out_specs=P("dp", None),
        check_vma=False,
    )
```

```python
import functools

import jax
import jax.numpy as jnp
from jax import lax
from jax.experimental import pallas as pl
from jax.experimental.pallas import tpu as pltpu
from jax.sharding import PartitionSpec as P

F32, BF16 = jnp.float32, jnp.bfloat16

R = 256
R1, R2 = 192, 64
NJ = 2
ROOT2 = (0, 3, 1, 2)
M2 = 4
NZ = 4
HY, HC, HE, HO, HF = 3, 2, 2, 2, 1
HZ, HX, HB, E2 = 2, 3, 2, 0
ORDER = "sczexob"


def _far(k):
    return max(k, NZ - 1 - k)


def _hops(z, k):
    return jnp.where(z < k, z, jnp.where(z > k, NZ - 1 - z, _far(k)))


def kernel(
    x_hbm, wg_hbm, wu_hbm, wd_hbm, y,
    x, wg, wu, wd, hid, part,
    sy1, ry1, s1, r_in, r_ex, s2, rl2, rr2, ry2,
    in_sem, wd_s, wd_r, hid_s, hid_r,
    y1_s, y1_r, z1_s, in_r, ex_r, o1_s, o1_r, a1_s, a1_r, y2_s, y2_r, df_s, df_r,
    z2_s, l2_r, r2_r, bl2_s, br2_s, b2_r,
):
    rows, width = y.shape
    n_super = rows // R
    n = NJ * n_super
    half = width // 2
    cw = half // NJ
    units = wg_hbm.shape[1]
    uh = units // NJ
    nb = min(256, uh)
    blocks = units // nb
    w1 = cw // 2
    w2 = cw * M2 // len(ROOT2)

    me = lax.axis_index("tp")
    core = lax.rem(me, 2)
    z = lax.rem(lax.div(me, 2), NZ)
    yy = lax.div(me, 2 * NZ)
    peer = {"tp": me + 1 - 2 * core}
    ypeer = {"tp": lax.rem(me + 2 * NZ, 4 * NZ)}
    left = {"tp": me - 2}
    right = {"tp": me + 2}
    outer = (z == 0) | (z == NZ - 1)
    step_in = jnp.where(z < NZ // 2, 2, -2)
    inward = {"tp": me + step_in}
    outward = {"tp": me - step_in}

    def load(i, src, dst):
        return pltpu.make_async_copy(src, dst, in_sem.at[i])

    def al(v, m):
        return pl.multiple_of(v, m)

    def x_copy(s):
        return load(s, x_hbm.at[pl.ds(al(s * R, R), R)], x.at[s])

    def g_copy(b):
        return load(n_super + b, wg_hbm.at[:, pl.ds(b * nb, nb)], wg.at[b])

    def u_copy(b):
        return load(n_super + blocks + b, wu_hbm.at[:, pl.ds(b * nb, nb)], wu.at[b])

    def d_copy(j):
        return load(
            n_super + 2 * blocks + j,
            wd_hbm.at[:, pl.ds(al(core * half + j * cw, cw), cw)],
            wd.at[j, pl.ds(al(core * units, units), units)],
        )

    def remote(src, dst, ssem, rsem, dev):
        return pltpu.make_async_remote_copy(
            src_ref=src, dst_ref=dst, send_sem=ssem, recv_sem=rsem,
            device_id=dev, device_id_type=pl.DeviceIdType.MESH,
        )

    x_copy(0).start()
    for b in range(blocks):
        g_copy(b).start()
        u_copy(b).start()
    for j in range(NJ):
        d_copy(j).start()
    x_copy(1).start()

    barrier = pltpu.get_barrier_semaphore()

    def hello(dev):
        pl.semaphore_signal(barrier, inc=1, device_id=dev, device_id_type=pl.DeviceIdType.MESH)

    hello(peer)
    hello(ypeer)
    pl.when(z > 0)(lambda: hello(left))
    pl.when(z < NZ - 1)(lambda: hello(right))
    pl.semaphore_wait(barrier, 2 + jnp.minimum(z, 1) + jnp.minimum(NZ - 1 - z, 1))

    def wd_msg(j):
        return remote(
            wd_hbm.at[:, pl.ds(al((1 - core) * half + j * cw, cw), cw)],
            wd.at[j, pl.ds(al(core * units, units), units)],
            wd_s.at[j], wd_r.at[j], peer,
        )

    for j in range(NJ):
        wd_msg(j).start()
    for s in range(2, n_super):
        x_copy(s).start()

    def hid_msg(c):
        s, j = lax.div(c, NJ), lax.rem(c, NJ)
        place = hid.at[s, :, pl.ds(al(core * units + j * uh, uh), uh)]
        return remote(place, place, hid_s.at[c], hid_r.at[c], peer)

    def row0(c):
        return al(lax.div(c, NJ) * R, R)

    def col0(c, who):
        return al(who * half + lax.rem(c, NJ) * cw, cw)

    def y1_place(c, h):
        return y.at[pl.ds(row0(c), R1), pl.ds(al(col0(c, core) + h * w1, w1), w1)]

    def y2_place(c, q):
        return y.at[pl.ds(al(row0(c) + R1, 16), R2), pl.ds(al(col0(c, core) + q // M2 * w2, w2), w2)]

    def part1(c, h):
        return part.at[c, pl.ds(0, R1), pl.ds(al(h * w1, w1), w1)]

    def part2(c, q):
        return part.at[c, pl.ds(R1, R2), pl.ds(q // M2 * w2, w2)]

    def m_y1(c):
        return remote(sy1.at[c], ry1.at[c], y1_s.at[c], y1_r.at[c], ypeer)

    def m_in(c):
        return remote(s1.at[c], r_in.at[c], z1_s.at[c], in_r.at[c], inward)

    def m_ex(c):
        return remote(s1.at[c], r_ex.at[c], z1_s.at[c], ex_r.at[c], inward)

    def m_o1(c):
        place = y1_place(c, yy)
        return remote(place, place, o1_s.at[c], o1_r.at[c], outward)

    def m_a1(c, h):
        place = y1_place(c, h)
        return remote(place, place, a1_s.at[c], a1_r.at[c], ypeer)

    def m_z2(c, q, to_right):
        i = q // M2
        dst, sem = (rl2, l2_r) if to_right else (rr2, r2_r)
        return remote(s2.at[c, i], dst.at[c, i], z2_s.at[c, i], sem.at[c, i], right if to_right else left)

    def m_y2(c, q):
        return remote(s2.at[c, q // M2], ry2.at[c], y2_s.at[c], y2_r.at[c], ypeer)

    def m_b2(c, q, to_right):
        i = q // M2
        place = y2_place(c, q)
        return remote(place, place, (br2_s if to_right else bl2_s).at[c, i], b2_r.at[c, i], right if to_right else left)

    def m_df(c, who):
        place = y.at[pl.ds(row0(c), R), pl.ds(col0(c, who), cw)]
        return remote(place, place, df_s.at[c], df_r.at[c], peer)

    def gate_up_wait(it):
        @pl.when(lax.rem(it, NJ) == 0)
        def _():
            x_copy(lax.div(it, NJ)).wait()

    def gate_up(it, first=None):
        s, j = lax.div(it, NJ), lax.rem(it, NJ)
        for b in range(uh // nb):
            block = j * (uh // nb) + b
            if first is not None:
                g_copy(first * (uh // nb) + b).wait()
                u_copy(first * (uh // nb) + b).wait()
            gate = jnp.dot(x[s], wg[block], preferred_element_type=F32)
            up = jnp.dot(x[s], wu[block], preferred_element_type=F32)
            hid[s, :, pl.ds(al(core * units + j * uh + b * nb, nb), nb)] = (jax.nn.gelu(gate) * up).astype(BF16)

    def down_wait(c):
        for j in range(NJ):

            @pl.when(c == j)
            def _():
                d_copy(j).wait()
                wd_msg(j).wait_recv()

        @pl.when(lax.rem(c, NJ) == 0)
        def _():
            for j in range(NJ):
                hid_msg(c + j).wait_recv()

    def down(c):
        s, j = lax.div(c, NJ), lax.rem(c, NJ)
        db = min(256, cw)
        for b in range(cw // db):
            cols = pl.ds(b * db, db)
            part[c, :, cols] = jnp.dot(hid[s], wd[j, :, cols], preferred_element_type=F32)

    def down_send(c):
        sy1[c] = part1(c, 1 - yy)[...].astype(BF16)
        m_y1(c).start()

    def compute(it):
        for j in range(NJ):

            @pl.when(it == j)
            def _():
                gate_up_wait(it)
                gate_up(it, first=j)
                hid_msg(it).start()

        @pl.when((it >= NJ) & (it < n))
        def _():
            down_wait(it - NJ)
            gate_up_wait(it)
            down(it - NJ)
            gate_up(it)
            hid_msg(it).start()
            down_send(it - NJ)

        @pl.when((it >= n) & (it < n + NJ))
        def _():
            down_wait(it - NJ)
            down(it - NJ)
            down_send(it - NJ)

    def active(c, p, m):
        return True if m == 1 else lax.rem(c, m) == p % m

    def guarded(c, f, p=0, m=1):
        pl.when((c >= 0) & (c < n) & active(c, p, m))(lambda: f(c))

    def chain(c, k, base, lbuf, rbuf, sbuf, msg, root):
        if k > 0:

            @pl.when(z == 0)
            def _():
                sbuf[...] = base().astype(BF16)
                msg(True).start()

        if k < NZ - 1:

            @pl.when(z == NZ - 1)
            def _():
                sbuf[...] = base().astype(BF16)
                msg(False).start()

        if k > 1:

            @pl.when((z > 0) & (z < k))
            def _():
                msg(True).wait_recv()
                sbuf[...] = (base() + lbuf[...].astype(F32)).astype(BF16)
                msg(True).start()

        if k < NZ - 2:

            @pl.when((z < NZ - 1) & (z > k))
            def _():
                msg(False).wait_recv()
                sbuf[...] = (base() + rbuf[...].astype(F32)).astype(BF16)
                msg(False).start()

        pl.when(z == k)(root)

    def arrived(k, lbuf, rbuf, msg):
        total = 0.0
        if k > 0:
            msg(True).wait_recv()
            total = lbuf[...].astype(F32)
        if k < NZ - 1:
            msg(False).wait_recv()
            total = total + rbuf[...].astype(F32)
        return total

    def spread(k, msg):
        if k < NZ - 1:
            pl.when((z >= k) & (z < NZ - 1))(lambda: msg(True).start())
        if k > 0:
            pl.when((z <= k) & (z > 0))(lambda: msg(False).start())

    def outer_in(c):
        m_y1(c).wait_recv()
        s1[c] = (part1(c, yy)[...] + ry1[c].astype(F32)).astype(BF16)
        m_in(c).start()

    def centre_sum(c):
        m_y1(c).wait_recv()
        m_in(c).wait_recv()
        s1[c] = (part1(c, yy)[...] + ry1[c].astype(F32) + r_in[c].astype(F32)).astype(BF16)
        m_ex(c).start()

    def centre_out(c):
        m_ex(c).wait_recv()
        y1_place(c, yy)[...] = (s1[c].astype(F32) + r_ex[c].astype(F32)).astype(BF16)
        m_o1(c).start()
        m_a1(c, yy).start()

    def outer_out(c):
        m_o1(c).wait_recv()
        m_a1(c, yy).start()

    def reduce2(c, q):
        k = ROOT2[q]
        i = q // M2
        bufs = rl2.at[c, i], rr2.at[c, i]

        def base():
            return part2(c, q)[...]

        def msg(to_right):
            return m_z2(c, q, to_right)

        def root():
            more = arrived(k, *bufs, msg)
            s2[c, i] = (base() + more).astype(BF16)
            m_y2(c, q).start()

        chain(c, k, base, *bufs, s2.at[c, i], msg, root)

    def cross2(c, q):
        k = ROOT2[q]

        @pl.when(z == k)
        def _():
            m_y2(c, q).wait_recv()
            y2_place(c, q)[...] = (s2[c, q // M2].astype(F32) + ry2[c].astype(F32)).astype(BF16)
            spread(k, lambda to_right: m_b2(c, q, to_right))

    def bcast2(c, q):
        k = ROOT2[q]

        @pl.when(z != k)
        def _():
            m_b2(c, q, True).wait_recv()
            spread(k, lambda to_right: m_b2(c, q, to_right))

    def finish(c):
        m_a1(c, 1 - yy).wait_recv()
        m_df(c, core).start()

    def dist(k):
        return jnp.where(z < k, k - z, z - k)

    def when_in(c, cond, f):
        pl.when((c >= 0) & (c < n) & cond)(lambda: f(c))

    at_in = NJ + HY
    at_sum = at_in + HC
    at_out = at_sum + HE
    at_end = at_out + HO
    last = max([at_end + HF] + [NJ + HX + E2 + (HZ + HB) * _far(k) for k in ROOT2])
    centre = jnp.logical_not(outer)

    def second(it, lag, f):
        for q, k in enumerate(ROOT2):
            guarded(it - lag(k), functools.partial(f, q=q), q, M2)

    def step(it, carry):
        compute(it)
        for name in ORDER:
            if name == "s":
                when_in(it - at_in, outer, outer_in)
            if name == "c":
                when_in(it - at_sum, centre, centre_sum)
            if name == "e":
                when_in(it - at_out, centre, centre_out)
            if name == "o":
                when_in(it - at_end, outer, outer_out)
            if name == "z":
                second(it, lambda k: NJ + HZ * _hops(z, k), reduce2)
            if name == "x":
                second(it, lambda k: NJ + HX + HZ * _far(k), cross2)
            if name == "b":
                second(it, lambda k: NJ + HX + E2 + HZ * _far(k) + HB * dist(k), bcast2)
        guarded(it - last, finish)
        return carry

    lax.fori_loop(0, n + last, step, 0)

    for j in range(NJ):
        wd_msg(j).wait_send()

    def drain(c, carry):
        hid_msg(c).wait_send()
        m_y1(c).wait_send()
        m_in(c).wait_send()
        pl.when(centre)(lambda: m_o1(c).wait_send())
        m_a1(c, yy).wait_send()
        for q, k in enumerate(ROOT2):

            @pl.when(active(c, q, M2))
            def _():
                pl.when(z != k)(lambda: m_z2(c, q, True).wait_send())
                pl.when(z == k)(lambda: m_y2(c, q).wait_send())
                if k < NZ - 1:
                    pl.when((z >= k) & (z < NZ - 1))(lambda: m_b2(c, q, True).wait_send())
                if k > 0:
                    pl.when((z <= k) & (z > 0))(lambda: m_b2(c, q, False).wait_send())

        return carry

    lax.fori_loop(0, n, drain, 0)

    def drain_rows(c, carry):
        m_df(c, core).wait_send()
        m_df(c, 1 - core).wait_recv()
        return carry

    lax.fori_loop(0, n, drain_rows, 0)


def put_out(y, out, sem):
    parts = sem.shape[0]
    rows = y.shape[0] // parts
    copies = [
        pltpu.make_async_copy(y.at[pl.ds(i * rows, rows)], out.at[pl.ds(i * rows, rows)], sem.at[i]) for i in range(parts)
    ]
    for c in copies:
        c.start()
    for c in copies:
        c.wait()


def block(x, w_gate, w_up, w_down):
    rows, width = x.shape
    units = w_gate.shape[1]
    n_super = rows // R
    n = NJ * n_super
    cw = width // 2 // NJ
    n2 = len(ROOT2) // M2
    w1, w2 = cw // 2, cw // n2
    nb = min(256, units // NJ)
    blocks = units // nb
    dma = pltpu.SemaphoreType.DMA
    one = pltpu.VMEM((n, R1, w1), BF16)
    two = pltpu.VMEM((n, n2, R2, w2), BF16)
    cross = pltpu.VMEM((n, R2, w2), BF16)
    y = pl.pallas_call(
        kernel,
        out_shape=pltpu.VMEM((rows, width), BF16),
        in_specs=[pl.BlockSpec(memory_space=pl.ANY)] * 4,
        out_specs=pl.BlockSpec(memory_space=pltpu.VMEM),
        scratch_shapes=[
            pltpu.VMEM((n_super, R, width), BF16),
            pltpu.VMEM((blocks, width, nb), BF16),
            pltpu.VMEM((blocks, width, nb), BF16),
            pltpu.VMEM((NJ, 2 * units, cw), BF16),
            pltpu.VMEM((n_super, R, 2 * units), BF16),
            pltpu.VMEM((n, R, cw), F32),
            one, one, one, one, one, two, two, two, cross,
            dma((n_super + 2 * blocks + NJ,)), dma((NJ,)), dma((NJ,)), dma((n,)), dma((n,)),
            *[dma((n,))] * 13,
            *[dma((n, n2))] * 6,
        ],
        compiler_params=pltpu.CompilerParams(
            collective_id=0, has_side_effects=True, vmem_limit_bytes=52 * 1024 * 1024
        ),
    )(x, w_gate, w_up, w_down)
    return pl.pallas_call(
        put_out,
        out_shape=jax.ShapeDtypeStruct((rows, width), BF16),
        in_specs=[pl.BlockSpec(memory_space=pltpu.VMEM)],
        out_specs=pl.BlockSpec(memory_space=pl.ANY),
        scratch_shapes=[dma((8,))],
        name="put_out",
        compiler_params=pltpu.CompilerParams(vmem_limit_bytes=1024 * 1024),
    )(y)


def solution(mesh):
    return jax.shard_map(
        block,
        mesh=mesh,
        in_specs=(P("dp", None), P(None, "tp"), P(None, "tp"), P("tp", None)),
        out_specs=P("dp", None),
        check_vma=False,
    )
```

```python
import functools

import jax
import jax.numpy as jnp
from jax import lax
from jax.experimental import pallas as pl
from jax.experimental.pallas import tpu as pltpu
from jax.sharding import PartitionSpec as P

F32, BF16 = jnp.float32, jnp.bfloat16

R = 256
R1, R2 = 192, 64
NJ = 2
ROOT2 = (0, 3, 2, 1)
M2 = 4
NZ = 4
HY, HC, HE, HO, HF = 3, 2, 2, 2, 0
HZ, HX, HB, E2 = 2, 4, 2, 0
ORDER = "zsecxob"


def _far(k):
    return max(k, NZ - 1 - k)


def _hops(z, k):
    return jnp.where(z < k, z, jnp.where(z > k, NZ - 1 - z, _far(k)))


def kernel(
    x_hbm, wg_hbm, wu_hbm, wd_hbm, y,
    x, wg, wu, wd, hid, part,
    sy1, ry1, s1, r_in, r_ex, s2, rl2, rr2, ry2,
    in_sem, wd_s, wd_r, hid_s, hid_r,
    y1_s, y1_r, z1_s, in_r, ex_r, o1_s, o1_r, a1_s, a1_r, y2_s, y2_r, df_s, df_r,
    z2_s, l2_r, r2_r, bl2_s, br2_s, b2_r,
):
    rows, width = y.shape
    n_super = rows // R
    n = NJ * n_super
    half = width // 2
    cw = half // NJ
    units = wg_hbm.shape[1]
    uh = units // NJ
    nb = min(256, uh)
    blocks = units // nb
    w1 = cw // 2
    w2 = cw * M2 // len(ROOT2)

    me = lax.axis_index("tp")
    core = lax.rem(me, 2)
    z = lax.rem(lax.div(me, 2), NZ)
    yy = lax.div(me, 2 * NZ)
    peer = {"tp": me + 1 - 2 * core}
    ypeer = {"tp": lax.rem(me + 2 * NZ, 4 * NZ)}
    left = {"tp": me - 2}
    right = {"tp": me + 2}
    outer = (z == 0) | (z == NZ - 1)
    step_in = jnp.where(z < NZ // 2, 2, -2)
    inward = {"tp": me + step_in}
    outward = {"tp": me - step_in}

    def load(i, src, dst):
        return pltpu.make_async_copy(src, dst, in_sem.at[i])

    def al(v, m):
        return pl.multiple_of(v, m)

    def x_copy(s):
        return load(s, x_hbm.at[pl.ds(al(s * R, R), R)], x.at[s])

    def g_copy(b):
        return load(n_super + b, wg_hbm.at[:, pl.ds(b * nb, nb)], wg.at[b])

    def u_copy(b):
        return load(n_super + blocks + b, wu_hbm.at[:, pl.ds(b * nb, nb)], wu.at[b])

    def d_copy(j):
        return load(
            n_super + 2 * blocks + j,
            wd_hbm.at[:, pl.ds(al(core * half + j * cw, cw), cw)],
            wd.at[j, pl.ds(al(core * units, units), units)],
        )

    def remote(src, dst, ssem, rsem, dev):
        return pltpu.make_async_remote_copy(
            src_ref=src, dst_ref=dst, send_sem=ssem, recv_sem=rsem,
            device_id=dev, device_id_type=pl.DeviceIdType.MESH,
        )

    x_copy(0).start()
    for b in range(blocks):
        g_copy(b).start()
        u_copy(b).start()
    for j in range(NJ):
        d_copy(j).start()
    x_copy(1).start()

    barrier = pltpu.get_barrier_semaphore()

    def hello(dev):
        pl.semaphore_signal(barrier, inc=1, device_id=dev, device_id_type=pl.DeviceIdType.MESH)

    hello(peer)
    hello(ypeer)
    pl.when(z > 0)(lambda: hello(left))
    pl.when(z < NZ - 1)(lambda: hello(right))
    pl.semaphore_wait(barrier, 2 + jnp.minimum(z, 1) + jnp.minimum(NZ - 1 - z, 1))

    def wd_msg(j):
        return remote(
            wd_hbm.at[:, pl.ds(al((1 - core) * half + j * cw, cw), cw)],
            wd.at[j, pl.ds(al(core * units, units), units)],
            wd_s.at[j], wd_r.at[j], peer,
        )

    for j in range(NJ):
        wd_msg(j).start()
    for s in range(2, n_super):
        x_copy(s).start()

    def hid_msg(c):
        s, j = lax.div(c, NJ), lax.rem(c, NJ)
        place = hid.at[s, :, pl.ds(al(core * units + j * uh, uh), uh)]
        return remote(place, place, hid_s.at[c], hid_r.at[c], peer)

    def row0(c):
        return al(lax.div(c, NJ) * R, R)

    def col0(c, who):
        return al(who * half + lax.rem(c, NJ) * cw, cw)

    def y1_place(c, h):
        return y.at[pl.ds(row0(c), R1), pl.ds(al(col0(c, core) + h * w1, w1), w1)]

    def y2_place(c, q):
        return y.at[pl.ds(al(row0(c) + R1, 16), R2), pl.ds(al(col0(c, core) + q // M2 * w2, w2), w2)]

    def part1(c, h):
        return part.at[c, pl.ds(0, R1), pl.ds(al(h * w1, w1), w1)]

    def part2(c, q):
        return part.at[c, pl.ds(R1, R2), pl.ds(q // M2 * w2, w2)]

    def m_y1(c):
        return remote(sy1.at[c], ry1.at[c], y1_s.at[c], y1_r.at[c], ypeer)

    def m_in(c):
        return remote(s1.at[c], r_in.at[c], z1_s.at[c], in_r.at[c], inward)

    def m_ex(c):
        return remote(s1.at[c], r_ex.at[c], z1_s.at[c], ex_r.at[c], inward)

    def m_o1(c):
        place = y1_place(c, yy)
        return remote(place, place, o1_s.at[c], o1_r.at[c], outward)

    def m_a1(c, h):
        place = y1_place(c, h)
        return remote(place, place, a1_s.at[c], a1_r.at[c], ypeer)

    def m_z2(c, q, to_right):
        i = q // M2
        dst, sem = (rl2, l2_r) if to_right else (rr2, r2_r)
        return remote(s2.at[c, i], dst.at[c, i], z2_s.at[c, i], sem.at[c, i], right if to_right else left)

    def m_y2(c, q):
        return remote(s2.at[c, q // M2], ry2.at[c], y2_s.at[c], y2_r.at[c], ypeer)

    def m_b2(c, q, to_right):
        i = q // M2
        place = y2_place(c, q)
        return remote(place, place, (br2_s if to_right else bl2_s).at[c, i], b2_r.at[c, i], right if to_right else left)

    def m_df(c, who):
        place = y.at[pl.ds(row0(c), R), pl.ds(col0(c, who), cw)]
        return remote(place, place, df_s.at[c], df_r.at[c], peer)

    def gate_up_wait(it):
        @pl.when(lax.rem(it, NJ) == 0)
        def _():
            x_copy(lax.div(it, NJ)).wait()

    def gate_up(it, first=None):
        s, j = lax.div(it, NJ), lax.rem(it, NJ)
        for b in range(uh // nb):
            block = j * (uh // nb) + b
            if first is not None:
                g_copy(first * (uh // nb) + b).wait()
                u_copy(first * (uh // nb) + b).wait()
            gate = jnp.dot(x[s], wg[block], preferred_element_type=F32)
            up = jnp.dot(x[s], wu[block], preferred_element_type=F32)
            hid[s, :, pl.ds(al(core * units + j * uh + b * nb, nb), nb)] = (jax.nn.gelu(gate) * up).astype(BF16)

    def down_wait(c):
        for j in range(NJ):

            @pl.when(c == j)
            def _():
                d_copy(j).wait()
                wd_msg(j).wait_recv()

        @pl.when(lax.rem(c, NJ) == 0)
        def _():
            for j in range(NJ):
                hid_msg(c + j).wait_recv()

    def down(c):
        s, j = lax.div(c, NJ), lax.rem(c, NJ)
        db = min(256, cw)
        for b in range(cw // db):
            cols = pl.ds(b * db, db)
            part[c, :, cols] = jnp.dot(hid[s], wd[j, :, cols], preferred_element_type=F32)

    def down_send(c):
        sy1[c] = part1(c, 1 - yy)[...].astype(BF16)
        m_y1(c).start()

    def compute(it):
        for j in range(NJ):

            @pl.when(it == j)
            def _():
                gate_up_wait(it)
                gate_up(it, first=j)
                hid_msg(it).start()

        @pl.when((it >= NJ) & (it < n))
        def _():
            down_wait(it - NJ)
            gate_up_wait(it)
            down(it - NJ)
            gate_up(it)
            hid_msg(it).start()
            down_send(it - NJ)

        @pl.when((it >= n) & (it < n + NJ))
        def _():
            down_wait(it - NJ)
            down(it - NJ)
            down_send(it - NJ)

    def active(c, p, m):
        return True if m == 1 else lax.rem(c, m) == p % m

    def guarded(c, f, p=0, m=1):
        pl.when((c >= 0) & (c < n) & active(c, p, m))(lambda: f(c))

    def chain(c, k, base, lbuf, rbuf, sbuf, msg, root):
        if k > 0:

            @pl.when(z == 0)
            def _():
                sbuf[...] = base().astype(BF16)
                msg(True).start()

        if k < NZ - 1:

            @pl.when(z == NZ - 1)
            def _():
                sbuf[...] = base().astype(BF16)
                msg(False).start()

        if k > 1:

            @pl.when((z > 0) & (z < k))
            def _():
                msg(True).wait_recv()
                sbuf[...] = (base() + lbuf[...].astype(F32)).astype(BF16)
                msg(True).start()

        if k < NZ - 2:

            @pl.when((z < NZ - 1) & (z > k))
            def _():
                msg(False).wait_recv()
                sbuf[...] = (base() + rbuf[...].astype(F32)).astype(BF16)
                msg(False).start()

        pl.when(z == k)(root)

    def arrived(k, lbuf, rbuf, msg):
        total = 0.0
        if k > 0:
            msg(True).wait_recv()
            total = lbuf[...].astype(F32)
        if k < NZ - 1:
            msg(False).wait_recv()
            total = total + rbuf[...].astype(F32)
        return total

    def spread(k, msg):
        if k < NZ - 1:
            pl.when((z >= k) & (z < NZ - 1))(lambda: msg(True).start())
        if k > 0:
            pl.when((z <= k) & (z > 0))(lambda: msg(False).start())

    def outer_in(c):
        m_y1(c).wait_recv()
        s1[c] = (part1(c, yy)[...] + ry1[c].astype(F32)).astype(BF16)
        m_in(c).start()

    def centre_sum(c):
        m_y1(c).wait_recv()
        m_in(c).wait_recv()
        s1[c] = (part1(c, yy)[...] + ry1[c].astype(F32) + r_in[c].astype(F32)).astype(BF16)
        m_ex(c).start()

    def centre_out(c):
        m_ex(c).wait_recv()
        y1_place(c, yy)[...] = (s1[c].astype(F32) + r_ex[c].astype(F32)).astype(BF16)
        m_o1(c).start()
        m_a1(c, yy).start()

    def outer_out(c):
        m_o1(c).wait_recv()
        m_a1(c, yy).start()

    def reduce2(c, q):
        k = ROOT2[q]
        i = q // M2
        bufs = rl2.at[c, i], rr2.at[c, i]

        def base():
            return part2(c, q)[...]

        def msg(to_right):
            return m_z2(c, q, to_right)

        def root():
            more = arrived(k, *bufs, msg)
            s2[c, i] = (base() + more).astype(BF16)
            m_y2(c, q).start()

        chain(c, k, base, *bufs, s2.at[c, i], msg, root)

    def cross2(c, q):
        k = ROOT2[q]

        @pl.when(z == k)
        def _():
            m_y2(c, q).wait_recv()
            y2_place(c, q)[...] = (s2[c, q // M2].astype(F32) + ry2[c].astype(F32)).astype(BF16)
            spread(k, lambda to_right: m_b2(c, q, to_right))

    def bcast2(c, q):
        k = ROOT2[q]

        @pl.when(z != k)
        def _():
            m_b2(c, q, True).wait_recv()
            spread(k, lambda to_right: m_b2(c, q, to_right))

    def finish(c):
        m_a1(c, 1 - yy).wait_recv()
        m_df(c, core).start()

    def dist(k):
        return jnp.where(z < k, k - z, z - k)

    def when_in(c, cond, f):
        pl.when((c >= 0) & (c < n) & cond)(lambda: f(c))

    at_in = NJ + HY
    at_sum = at_in + HC
    at_out = at_sum + HE
    at_end = at_out + HO
    last = max([at_end + HF] + [NJ + HX + E2 + (HZ + HB) * _far(k) for k in ROOT2])
    centre = jnp.logical_not(outer)

    def second(it, lag, f):
        for q, k in enumerate(ROOT2):
            guarded(it - lag(k), functools.partial(f, q=q), q, M2)

    def step(it, carry):
        compute(it)
        for name in ORDER:
            if name == "s":
                when_in(it - at_in, outer, outer_in)
            if name == "c":
                when_in(it - at_sum, centre, centre_sum)
            if name == "e":
                when_in(it - at_out, centre, centre_out)
            if name == "o":
                when_in(it - at_end, outer, outer_out)
            if name == "z":
                second(it, lambda k: NJ + HZ * _hops(z, k), reduce2)
            if name == "x":
                second(it, lambda k: NJ + HX + HZ * _far(k), cross2)
            if name == "b":
                second(it, lambda k: NJ + HX + E2 + HZ * _far(k) + HB * dist(k), bcast2)
        guarded(it - last, finish)
        return carry

    lax.fori_loop(0, n + last, step, 0)

    for j in range(NJ):
        wd_msg(j).wait_send()

    def drain(c, carry):
        hid_msg(c).wait_send()
        m_y1(c).wait_send()
        m_in(c).wait_send()
        pl.when(centre)(lambda: m_o1(c).wait_send())
        m_a1(c, yy).wait_send()
        for q, k in enumerate(ROOT2):

            @pl.when(active(c, q, M2))
            def _():
                pl.when(z != k)(lambda: m_z2(c, q, True).wait_send())
                pl.when(z == k)(lambda: m_y2(c, q).wait_send())
                if k < NZ - 1:
                    pl.when((z >= k) & (z < NZ - 1))(lambda: m_b2(c, q, True).wait_send())
                if k > 0:
                    pl.when((z <= k) & (z > 0))(lambda: m_b2(c, q, False).wait_send())

        return carry

    lax.fori_loop(0, n, drain, 0)

    def drain_rows(c, carry):
        m_df(c, core).wait_send()
        m_df(c, 1 - core).wait_recv()
        return carry

    lax.fori_loop(0, n, drain_rows, 0)


def put_out(y, out, sem):
    parts = sem.shape[0]
    rows = y.shape[0] // parts
    copies = [
        pltpu.make_async_copy(y.at[pl.ds(i * rows, rows)], out.at[pl.ds(i * rows, rows)], sem.at[i]) for i in range(parts)
    ]
    for c in copies:
        c.start()
    for c in copies:
        c.wait()


def block(x, w_gate, w_up, w_down):
    rows, width = x.shape
    units = w_gate.shape[1]
    n_super = rows // R
    n = NJ * n_super
    cw = width // 2 // NJ
    n2 = len(ROOT2) // M2
    w1, w2 = cw // 2, cw // n2
    nb = min(256, units // NJ)
    blocks = units // nb
    dma = pltpu.SemaphoreType.DMA
    one = pltpu.VMEM((n, R1, w1), BF16)
    two = pltpu.VMEM((n, n2, R2, w2), BF16)
    cross = pltpu.VMEM((n, R2, w2), BF16)
    y = pl.pallas_call(
        kernel,
        out_shape=pltpu.VMEM((rows, width), BF16),
        in_specs=[pl.BlockSpec(memory_space=pl.ANY)] * 4,
        out_specs=pl.BlockSpec(memory_space=pltpu.VMEM),
        scratch_shapes=[
            pltpu.VMEM((n_super, R, width), BF16),
            pltpu.VMEM((blocks, width, nb), BF16),
            pltpu.VMEM((blocks, width, nb), BF16),
            pltpu.VMEM((NJ, 2 * units, cw), BF16),
            pltpu.VMEM((n_super, R, 2 * units), BF16),
            pltpu.VMEM((n, R, cw), F32),
            one, one, one, one, one, two, two, two, cross,
            dma((n_super + 2 * blocks + NJ,)), dma((NJ,)), dma((NJ,)), dma((n,)), dma((n,)),
            *[dma((n,))] * 13,
            *[dma((n, n2))] * 6,
        ],
        compiler_params=pltpu.CompilerParams(
            collective_id=0, has_side_effects=True, vmem_limit_bytes=52 * 1024 * 1024
        ),
    )(x, w_gate, w_up, w_down)
    return pl.pallas_call(
        put_out,
        out_shape=jax.ShapeDtypeStruct((rows, width), BF16),
        in_specs=[pl.BlockSpec(memory_space=pltpu.VMEM)],
        out_specs=pl.BlockSpec(memory_space=pl.ANY),
        scratch_shapes=[dma((8,))],
        name="put_out",
        compiler_params=pltpu.CompilerParams(vmem_limit_bytes=1024 * 1024),
    )(y)


def solution(mesh):
    return jax.shard_map(
        block,
        mesh=mesh,
        in_specs=(P("dp", None), P(None, "tp"), P(None, "tp"), P("tp", None)),
        out_specs=P("dp", None),
        check_vma=False,
    )
```

```python
import functools

import jax
import jax.numpy as jnp
from jax import lax
from jax.experimental import pallas as pl
from jax.experimental.pallas import tpu as pltpu
from jax.sharding import PartitionSpec as P

F32, BF16 = jnp.float32, jnp.bfloat16

R = 256
R1, R2 = 192, 64
NJ = 2
ROOT2 = (0, 3, 2, 1)
M2 = 4
NZ = 4
HY, HC, HE, HO, HF = 3, 2, 2, 2, 0
HZ, HX, HB, E2 = 2, 4, 2, 0
ORDER = "zsecxob"


def _far(k):
    return max(k, NZ - 1 - k)


def _hops(z, k):
    return jnp.where(z < k, z, jnp.where(z > k, NZ - 1 - z, _far(k)))


def kernel(
    x_hbm, wg_hbm, wu_hbm, wd_hbm, y,
    x, wg, wu, wd, hid, part,
    sy1, ry1, s1, r_in, r_ex, s2, rl2, rr2, ry2,
    in_sem, wd_s, wd_r, hid_s, hid_r,
    y1_s, y1_r, z1_s, in_r, ex_r, o1_s, o1_r, a1_s, a1_r, y2_s, y2_r, df_s, df_r,
    z2_s, l2_r, r2_r, bl2_s, br2_s, b2_r,
):
    rows, width = y.shape
    n_super = rows // R
    n = NJ * n_super
    half = width // 2
    cw = half // NJ
    units = wg_hbm.shape[1]
    uh = units // NJ
    nb = min(256, uh)
    blocks = units // nb
    w1 = cw // 2
    w2 = cw * M2 // len(ROOT2)

    me = lax.axis_index("tp")
    core = lax.rem(me, 2)
    z = lax.rem(lax.div(me, 2), NZ)
    yy = lax.div(me, 2 * NZ)
    peer = {"tp": me + 1 - 2 * core}
    ypeer = {"tp": lax.rem(me + 2 * NZ, 4 * NZ)}
    left = {"tp": me - 2}
    right = {"tp": me + 2}
    outer = (z == 0) | (z == NZ - 1)
    step_in = jnp.where(z < NZ // 2, 2, -2)
    inward = {"tp": me + step_in}
    outward = {"tp": me - step_in}

    def load(i, src, dst):
        return pltpu.make_async_copy(src, dst, in_sem.at[i])

    def al(v, m):
        return pl.multiple_of(v, m)

    def x_copy(s):
        return load(s, x_hbm.at[pl.ds(al(s * R, R), R)], x.at[s])

    def g_copy(b):
        return load(n_super + b, wg_hbm.at[:, pl.ds(b * nb, nb)], wg.at[b])

    def u_copy(b):
        return load(n_super + blocks + b, wu_hbm.at[:, pl.ds(b * nb, nb)], wu.at[b])

    def d_copy(j):
        return load(
            n_super + 2 * blocks + j,
            wd_hbm.at[:, pl.ds(al(core * half + j * cw, cw), cw)],
            wd.at[j, pl.ds(al(core * units, units), units)],
        )

    def remote(src, dst, ssem, rsem, dev):
        return pltpu.make_async_remote_copy(
            src_ref=src, dst_ref=dst, send_sem=ssem, recv_sem=rsem,
            device_id=dev, device_id_type=pl.DeviceIdType.MESH,
        )

    x_copy(0).start()
    for b in range(blocks):
        g_copy(b).start()
        u_copy(b).start()
    for j in range(NJ):
        d_copy(j).start()
    x_copy(1).start()

    barrier = pltpu.get_barrier_semaphore()

    def hello(dev):
        pl.semaphore_signal(barrier, inc=1, device_id=dev, device_id_type=pl.DeviceIdType.MESH)

    hello(peer)
    hello(ypeer)
    pl.when(z > 0)(lambda: hello(left))
    pl.when(z < NZ - 1)(lambda: hello(right))
    pl.semaphore_wait(barrier, 2 + jnp.minimum(z, 1) + jnp.minimum(NZ - 1 - z, 1))

    def wd_msg(j):
        return remote(
            wd_hbm.at[:, pl.ds(al((1 - core) * half + j * cw, cw), cw)],
            wd.at[j, pl.ds(al(core * units, units), units)],
            wd_s.at[j], wd_r.at[j], peer,
        )

    for j in range(NJ):
        wd_msg(j).start()
    for s in range(2, n_super):
        x_copy(s).start()

    def hid_msg(c):
        s, j = lax.div(c, NJ), lax.rem(c, NJ)
        place = hid.at[s, :, pl.ds(al(core * units + j * uh, uh), uh)]
        return remote(place, place, hid_s.at[c], hid_r.at[c], peer)

    def row0(c):
        return al(lax.div(c, NJ) * R, R)

    def col0(c, who):
        return al(who * half + lax.rem(c, NJ) * cw, cw)

    def y1_place(c, h):
        return y.at[pl.ds(row0(c), R1), pl.ds(al(col0(c, core) + h * w1, w1), w1)]

    def y2_place(c, q):
        return y.at[pl.ds(al(row0(c) + R1, 16), R2), pl.ds(al(col0(c, core) + q // M2 * w2, w2), w2)]

    def part1(c, h):
        return part.at[c, pl.ds(0, R1), pl.ds(al(h * w1, w1), w1)]

    def part2(c, q):
        return part.at[c, pl.ds(R1, R2), pl.ds(q // M2 * w2, w2)]

    def m_y1(c):
        return remote(sy1.at[c], ry1.at[c], y1_s.at[c], y1_r.at[c], ypeer)

    def m_in(c):
        return remote(s1.at[c], r_in.at[c], z1_s.at[c], in_r.at[c], inward)

    def m_ex(c):
        return remote(s1.at[c], r_ex.at[c], z1_s.at[c], ex_r.at[c], inward)

    def m_o1(c):
        place = y1_place(c, yy)
        return remote(place, place, o1_s.at[c], o1_r.at[c], outward)

    def m_a1(c, h):
        place = y1_place(c, h)
        return remote(place, place, a1_s.at[c], a1_r.at[c], ypeer)

    def m_z2(c, q, to_right):
        i = q // M2
        dst, sem = (rl2, l2_r) if to_right else (rr2, r2_r)
        return remote(s2.at[c, i], dst.at[c, i], z2_s.at[c, i], sem.at[c, i], right if to_right else left)

    def m_y2(c, q):
        return remote(s2.at[c, q // M2], ry2.at[c], y2_s.at[c], y2_r.at[c], ypeer)

    def m_b2(c, q, to_right):
        i = q // M2
        place = y2_place(c, q)
        return remote(place, place, (br2_s if to_right else bl2_s).at[c, i], b2_r.at[c, i], right if to_right else left)

    def m_df(c, who):
        place = y.at[pl.ds(row0(c), R), pl.ds(col0(c, who), cw)]
        return remote(place, place, df_s.at[c], df_r.at[c], peer)

    def gate_up_wait(it):
        @pl.when(lax.rem(it, NJ) == 0)
        def _():
            x_copy(lax.div(it, NJ)).wait()

    def gate_up(it, first=None, part_of=range(uh // nb)):
        s, j = lax.div(it, NJ), lax.rem(it, NJ)
        for b in part_of:
            block = j * (uh // nb) + b
            if first is not None:
                g_copy(first * (uh // nb) + b).wait()
                u_copy(first * (uh // nb) + b).wait()
            gate = jnp.dot(x[s], wg[block], preferred_element_type=F32)
            up = jnp.dot(x[s], wu[block], preferred_element_type=F32)
            hid[s, :, pl.ds(al(core * units + j * uh + b * nb, nb), nb)] = (jax.nn.gelu(gate) * up).astype(BF16)

    def down_wait(c):
        for j in range(NJ):

            @pl.when(c == j)
            def _():
                d_copy(j).wait()
                wd_msg(j).wait_recv()

        @pl.when(lax.rem(c, NJ) == 0)
        def _():
            for j in range(NJ):
                hid_msg(c + j).wait_recv()

    def down(c):
        s, j = lax.div(c, NJ), lax.rem(c, NJ)
        db = min(256, cw)
        for b in range(cw // db):
            cols = pl.ds(b * db, db)
            part[c, :, cols] = jnp.dot(hid[s], wd[j, :, cols], preferred_element_type=F32)

    def down_send(c):
        sy1[c] = part1(c, 1 - yy)[...].astype(BF16)
        m_y1(c).start()

    def compute(it):
        for j in range(NJ):

            @pl.when(it == j)
            def _():
                gate_up_wait(it)
                gate_up(it, first=j)
                hid_msg(it).start()

        @pl.when((it >= NJ) & (it < n) & (lax.rem(it, NJ) == 0))
        def _():
            gate_up_wait(it)
            gate_up(it, part_of=range(1))
            down_wait(it - NJ)
            down(it - NJ)
            gate_up(it, part_of=range(1, uh // nb))
            hid_msg(it).start()
            down_send(it - NJ)

        @pl.when((it >= NJ) & (it < n) & (lax.rem(it, NJ) != 0))
        def _():
            down_wait(it - NJ)
            down(it - NJ)
            gate_up(it)
            hid_msg(it).start()
            down_send(it - NJ)

        @pl.when((it >= n) & (it < n + NJ))
        def _():
            down_wait(it - NJ)
            down(it - NJ)
            down_send(it - NJ)

    def active(c, p, m):
        return True if m == 1 else lax.rem(c, m) == p % m

    def guarded(c, f, p=0, m=1):
        pl.when((c >= 0) & (c < n) & active(c, p, m))(lambda: f(c))

    def chain(c, k, base, lbuf, rbuf, sbuf, msg, root):
        if k > 0:

            @pl.when(z == 0)
            def _():
                sbuf[...] = base().astype(BF16)
                msg(True).start()

        if k < NZ - 1:

            @pl.when(z == NZ - 1)
            def _():
                sbuf[...] = base().astype(BF16)
                msg(False).start()

        if k > 1:

            @pl.when((z > 0) & (z < k))
            def _():
                msg(True).wait_recv()
                sbuf[...] = (base() + lbuf[...].astype(F32)).astype(BF16)
                msg(True).start()

        if k < NZ - 2:

            @pl.when((z < NZ - 1) & (z > k))
            def _():
                msg(False).wait_recv()
                sbuf[...] = (base() + rbuf[...].astype(F32)).astype(BF16)
                msg(False).start()

        pl.when(z == k)(root)

    def arrived(k, lbuf, rbuf, msg):
        total = 0.0
        if k > 0:
            msg(True).wait_recv()
            total = lbuf[...].astype(F32)
        if k < NZ - 1:
            msg(False).wait_recv()
            total = total + rbuf[...].astype(F32)
        return total

    def spread(k, msg):
        if k < NZ - 1:
            pl.when((z >= k) & (z < NZ - 1))(lambda: msg(True).start())
        if k > 0:
            pl.when((z <= k) & (z > 0))(lambda: msg(False).start())

    def outer_in(c):
        m_y1(c).wait_recv()
        s1[c] = (part1(c, yy)[...] + ry1[c].astype(F32)).astype(BF16)
        m_in(c).start()

    def centre_sum(c):
        m_y1(c).wait_recv()
        m_in(c).wait_recv()
        s1[c] = (part1(c, yy)[...] + ry1[c].astype(F32) + r_in[c].astype(F32)).astype(BF16)
        m_ex(c).start()

    def centre_out(c):
        m_ex(c).wait_recv()
        y1_place(c, yy)[...] = (s1[c].astype(F32) + r_ex[c].astype(F32)).astype(BF16)
        m_o1(c).start()
        m_a1(c, yy).start()

    def outer_out(c):
        m_o1(c).wait_recv()
        m_a1(c, yy).start()

    def reduce2(c, q):
        k = ROOT2[q]
        i = q // M2
        bufs = rl2.at[c, i], rr2.at[c, i]

        def base():
            return part2(c, q)[...]

        def msg(to_right):
            return m_z2(c, q, to_right)

        def root():
            more = arrived(k, *bufs, msg)
            s2[c, i] = (base() + more).astype(BF16)
            m_y2(c, q).start()

        chain(c, k, base, *bufs, s2.at[c, i], msg, root)

    def cross2(c, q):
        k = ROOT2[q]

        @pl.when(z == k)
        def _():
            m_y2(c, q).wait_recv()
            y2_place(c, q)[...] = (s2[c, q // M2].astype(F32) + ry2[c].astype(F32)).astype(BF16)
            spread(k, lambda to_right: m_b2(c, q, to_right))

    def bcast2(c, q):
        k = ROOT2[q]

        @pl.when(z != k)
        def _():
            m_b2(c, q, True).wait_recv()
            spread(k, lambda to_right: m_b2(c, q, to_right))

    def finish(c):
        m_a1(c, 1 - yy).wait_recv()
        m_df(c, core).start()

    def dist(k):
        return jnp.where(z < k, k - z, z - k)

    def when_in(c, cond, f):
        pl.when((c >= 0) & (c < n) & cond)(lambda: f(c))

    at_in = NJ + HY
    at_sum = at_in + HC
    at_out = at_sum + HE
    at_end = at_out + HO
    last = max([at_end + HF] + [NJ + HX + E2 + (HZ + HB) * _far(k) for k in ROOT2])
    centre = jnp.logical_not(outer)

    def second(it, lag, f):
        for q, k in enumerate(ROOT2):
            guarded(it - lag(k), functools.partial(f, q=q), q, M2)

    def step(it, carry):
        compute(it)
        for name in ORDER:
            if name == "s":
                when_in(it - at_in, outer, outer_in)
            if name == "c":
                when_in(it - at_sum, centre, centre_sum)
            if name == "e":
                when_in(it - at_out, centre, centre_out)
            if name == "o":
                when_in(it - at_end, outer, outer_out)
            if name == "z":
                second(it, lambda k: NJ + HZ * _hops(z, k), reduce2)
            if name == "x":
                second(it, lambda k: NJ + HX + HZ * _far(k), cross2)
            if name == "b":
                second(it, lambda k: NJ + HX + E2 + HZ * _far(k) + HB * dist(k), bcast2)
        guarded(it - last, finish)
        return carry

    lax.fori_loop(0, n + last, step, 0)

    for j in range(NJ):
        wd_msg(j).wait_send()

    def drain(c, carry):
        hid_msg(c).wait_send()
        m_y1(c).wait_send()
        m_in(c).wait_send()
        pl.when(centre)(lambda: m_o1(c).wait_send())
        m_a1(c, yy).wait_send()
        for q, k in enumerate(ROOT2):

            @pl.when(active(c, q, M2))
            def _():
                pl.when(z != k)(lambda: m_z2(c, q, True).wait_send())
                pl.when(z == k)(lambda: m_y2(c, q).wait_send())
                if k < NZ - 1:
                    pl.when((z >= k) & (z < NZ - 1))(lambda: m_b2(c, q, True).wait_send())
                if k > 0:
                    pl.when((z <= k) & (z > 0))(lambda: m_b2(c, q, False).wait_send())

        return carry

    lax.fori_loop(0, n, drain, 0)

    def drain_rows(c, carry):
        m_df(c, core).wait_send()
        m_df(c, 1 - core).wait_recv()
        return carry

    lax.fori_loop(0, n, drain_rows, 0)


def put_out(y, out, sem):
    parts = sem.shape[0]
    rows = y.shape[0] // parts
    copies = [
        pltpu.make_async_copy(y.at[pl.ds(i * rows, rows)], out.at[pl.ds(i * rows, rows)], sem.at[i]) for i in range(parts)
    ]
    for c in copies:
        c.start()
    for c in copies:
        c.wait()


def block(x, w_gate, w_up, w_down):
    rows, width = x.shape
    units = w_gate.shape[1]
    n_super = rows // R
    n = NJ * n_super
    cw = width // 2 // NJ
    n2 = len(ROOT2) // M2
    w1, w2 = cw // 2, cw // n2
    nb = min(256, units // NJ)
    blocks = units // nb
    dma = pltpu.SemaphoreType.DMA
    one = pltpu.VMEM((n, R1, w1), BF16)
    two = pltpu.VMEM((n, n2, R2, w2), BF16)
    cross = pltpu.VMEM((n, R2, w2), BF16)
    y = pl.pallas_call(
        kernel,
        out_shape=pltpu.VMEM((rows, width), BF16),
        in_specs=[pl.BlockSpec(memory_space=pl.ANY)] * 4,
        out_specs=pl.BlockSpec(memory_space=pltpu.VMEM),
        scratch_shapes=[
            pltpu.VMEM((n_super, R, width), BF16),
            pltpu.VMEM((blocks, width, nb), BF16),
            pltpu.VMEM((blocks, width, nb), BF16),
            pltpu.VMEM((NJ, 2 * units, cw), BF16),
            pltpu.VMEM((n_super, R, 2 * units), BF16),
            pltpu.VMEM((n, R, cw), F32),
            one, one, one, one, one, two, two, two, cross,
            dma((n_super + 2 * blocks + NJ,)), dma((NJ,)), dma((NJ,)), dma((n,)), dma((n,)),
            *[dma((n,))] * 13,
            *[dma((n, n2))] * 6,
        ],
        compiler_params=pltpu.CompilerParams(
            collective_id=0, has_side_effects=True, vmem_limit_bytes=52 * 1024 * 1024
        ),
    )(x, w_gate, w_up, w_down)
    return pl.pallas_call(
        put_out,
        out_shape=jax.ShapeDtypeStruct((rows, width), BF16),
        in_specs=[pl.BlockSpec(memory_space=pltpu.VMEM)],
        out_specs=pl.BlockSpec(memory_space=pl.ANY),
        scratch_shapes=[dma((8,))],
        name="put_out",
        compiler_params=pltpu.CompilerParams(vmem_limit_bytes=1024 * 1024),
    )(y)


def solution(mesh):
    return jax.shard_map(
        block,
        mesh=mesh,
        in_specs=(P("dp", None), P(None, "tp"), P(None, "tp"), P("tp", None)),
        out_specs=P("dp", None),
        check_vma=False,
    )
```

```python
import functools

import jax
import jax.numpy as jnp
from jax import lax
from jax.experimental import pallas as pl
from jax.experimental.pallas import tpu as pltpu
from jax.sharding import PartitionSpec as P

F32, BF16 = jnp.float32, jnp.bfloat16

R = 256
R1, R2 = 192, 64
NJ = 2
ROOT2 = (0, 3, 2, 1)
M2 = 4
NZ = 4
HY, HC, HE, HO, HF = 3, 2, 2, 2, 0
HZ, HX, HB, E2 = 2, 4, 2, 0
ORDER = "zsecxob"


def _far(k):
    return max(k, NZ - 1 - k)


def _hops(z, k):
    return jnp.where(z < k, z, jnp.where(z > k, NZ - 1 - z, _far(k)))


def kernel(
    x_hbm, wg_hbm, wu_hbm, wd_hbm, y,
    x, wg, wu, wd, hid, part,
    sy1, ry1, s1, r_in, r_ex, s2, rl2, rr2, ry2,
    in_sem, wd_s, wd_r, hid_s, hid_r,
    y1_s, y1_r, z1_s, in_r, ex_r, o1_s, o1_r, a1_s, a1_r, y2_s, y2_r, df_s, df_r,
    z2_s, l2_r, r2_r, bl2_s, br2_s, b2_r,
):
    rows, width = y.shape
    n_super = rows // R
    n = NJ * n_super
    half = width // 2
    cw = half // NJ
    units = wg_hbm.shape[1]
    uh = units // NJ
    nb = min(256, uh)
    blocks = units // nb
    w1 = cw // 2
    w2 = cw * M2 // len(ROOT2)

    me = lax.axis_index("tp")
    core = lax.rem(me, 2)
    z = lax.rem(lax.div(me, 2), NZ)
    yy = lax.div(me, 2 * NZ)
    peer = {"tp": me + 1 - 2 * core}
    ypeer = {"tp": lax.rem(me + 2 * NZ, 4 * NZ)}
    left = {"tp": me - 2}
    right = {"tp": me + 2}
    outer = (z == 0) | (z == NZ - 1)
    step_in = jnp.where(z < NZ // 2, 2, -2)
    inward = {"tp": me + step_in}
    outward = {"tp": me - step_in}

    def load(i, src, dst):
        return pltpu.make_async_copy(src, dst, in_sem.at[i])

    def al(v, m):
        return pl.multiple_of(v, m)

    def x_copy(s):
        return load(s, x_hbm.at[pl.ds(al(s * R, R), R)], x.at[s])

    def g_copy(b):
        return load(n_super + b, wg_hbm.at[:, pl.ds(b * nb, nb)], wg.at[b])

    def u_copy(b):
        return load(n_super + blocks + b, wu_hbm.at[:, pl.ds(b * nb, nb)], wu.at[b])

    def d_copy(j):
        return load(
            n_super + 2 * blocks + j,
            wd_hbm.at[:, pl.ds(al(core * half + j * cw, cw), cw)],
            wd.at[j, pl.ds(al(core * units, units), units)],
        )

    def remote(src, dst, ssem, rsem, dev):
        return pltpu.make_async_remote_copy(
            src_ref=src, dst_ref=dst, send_sem=ssem, recv_sem=rsem,
            device_id=dev, device_id_type=pl.DeviceIdType.MESH,
        )

    x_copy(0).start()
    for b in range(blocks):
        g_copy(b).start()
        u_copy(b).start()
    for j in range(NJ):
        d_copy(j).start()
    x_copy(1).start()

    barrier = pltpu.get_barrier_semaphore()

    def hello(dev):
        pl.semaphore_signal(barrier, inc=1, device_id=dev, device_id_type=pl.DeviceIdType.MESH)

    hello(peer)
    hello(ypeer)
    pl.when(z > 0)(lambda: hello(left))
    pl.when(z < NZ - 1)(lambda: hello(right))
    pl.semaphore_wait(barrier, 2 + jnp.minimum(z, 1) + jnp.minimum(NZ - 1 - z, 1))

    def wd_msg(j):
        return remote(
            wd_hbm.at[:, pl.ds(al((1 - core) * half + j * cw, cw), cw)],
            wd.at[j, pl.ds(al(core * units, units), units)],
            wd_s.at[j], wd_r.at[j], peer,
        )

    for j in range(NJ):
        wd_msg(j).start()
    for s in range(2, n_super):
        x_copy(s).start()

    def hid_msg(c):
        s, j = lax.div(c, NJ), lax.rem(c, NJ)
        place = hid.at[s, :, pl.ds(al(core * units + j * uh, uh), uh)]
        return remote(place, place, hid_s.at[c], hid_r.at[c], peer)

    def row0(c):
        return al(lax.div(c, NJ) * R, R)

    def col0(c, who):
        return al(who * half + lax.rem(c, NJ) * cw, cw)

    def y1_place(c, h):
        return y.at[pl.ds(row0(c), R1), pl.ds(al(col0(c, core) + h * w1, w1), w1)]

    def y2_place(c, q):
        return y.at[pl.ds(al(row0(c) + R1, 16), R2), pl.ds(al(col0(c, core) + q // M2 * w2, w2), w2)]

    def part1(c, h):
        return part.at[c, pl.ds(0, R1), pl.ds(al(h * w1, w1), w1)]

    def part2(c, q):
        return part.at[c, pl.ds(R1, R2), pl.ds(q // M2 * w2, w2)]

    def m_y1(c):
        return remote(sy1.at[c], ry1.at[c], y1_s.at[c], y1_r.at[c], ypeer)

    def m_in(c):
        return remote(s1.at[c], r_in.at[c], z1_s.at[c], in_r.at[c], inward)

    def m_ex(c):
        return remote(s1.at[c], r_ex.at[c], z1_s.at[c], ex_r.at[c], inward)

    def m_o1(c):
        place = y1_place(c, yy)
        return remote(place, place, o1_s.at[c], o1_r.at[c], outward)

    def m_a1(c, h):
        place = y1_place(c, h)
        return remote(place, place, a1_s.at[c], a1_r.at[c], ypeer)

    def m_z2(c, q, to_right):
        i = q // M2
        dst, sem = (rl2, l2_r) if to_right else (rr2, r2_r)
        return remote(s2.at[c, i], dst.at[c, i], z2_s.at[c, i], sem.at[c, i], right if to_right else left)

    def m_y2(c, q):
        return remote(s2.at[c, q // M2], ry2.at[c], y2_s.at[c], y2_r.at[c], ypeer)

    def m_b2(c, q, to_right):
        i = q // M2
        place = y2_place(c, q)
        return remote(place, place, (br2_s if to_right else bl2_s).at[c, i], b2_r.at[c, i], right if to_right else left)

    def m_df(c, who):
        place = y.at[pl.ds(row0(c), R), pl.ds(col0(c, who), cw)]
        return remote(place, place, df_s.at[c], df_r.at[c], peer)

    def gate_up_wait(it):
        @pl.when(lax.rem(it, NJ) == 0)
        def _():
            x_copy(lax.div(it, NJ)).wait()

    def gate_up(it, first=None, part_of=range(uh // nb)):
        s, j = lax.div(it, NJ), lax.rem(it, NJ)
        for b in part_of:
            block = j * (uh // nb) + b
            if first is not None:
                g_copy(first * (uh // nb) + b).wait()
                u_copy(first * (uh // nb) + b).wait()
            gate = jnp.dot(x[s], wg[block], preferred_element_type=F32)
            up = jnp.dot(x[s], wu[block], preferred_element_type=F32)
            hid[s, :, pl.ds(al(core * units + j * uh + b * nb, nb), nb)] = (jax.nn.gelu(gate) * up).astype(BF16)

    def down_wait(c):
        for j in range(NJ):

            @pl.when(c == j)
            def _():
                d_copy(j).wait()
                wd_msg(j).wait_recv()

        @pl.when(lax.rem(c, NJ) == 0)
        def _():
            for j in range(NJ):
                hid_msg(c + j).wait_recv()

    def down(c):
        s, j = lax.div(c, NJ), lax.rem(c, NJ)
        db = min(256, cw)
        for b in range(cw // db):
            cols = pl.ds(b * db, db)
            part[c, :, cols] = jnp.dot(hid[s], wd[j, :, cols], preferred_element_type=F32)

    def down_send(c):
        sy1[c] = part1(c, 1 - yy)[...].astype(BF16)
        m_y1(c).start()

    def compute(it):
        for j in range(NJ):

            @pl.when(it == j)
            def _():
                gate_up_wait(it)
                gate_up(it, first=j)
                hid_msg(it).start()

        @pl.when((it >= NJ) & (it < n) & (lax.rem(it, NJ) == 0))
        def _():
            gate_up_wait(it)
            gate_up(it, part_of=range(1))
            down_wait(it - NJ)
            down(it - NJ)
            gate_up(it, part_of=range(1, uh // nb))
            hid_msg(it).start()
            down_send(it - NJ)

        @pl.when((it >= NJ) & (it < n) & (lax.rem(it, NJ) != 0))
        def _():
            down_wait(it - NJ)
            down(it - NJ)
            gate_up(it)
            hid_msg(it).start()
            down_send(it - NJ)

        @pl.when((it >= n) & (it < n + NJ))
        def _():
            down_wait(it - NJ)
            down(it - NJ)
            down_send(it - NJ)

    def active(c, p, m):
        return True if m == 1 else lax.rem(c, m) == p % m

    def guarded(c, f, p=0, m=1):
        pl.when((c >= 0) & (c < n) & active(c, p, m))(lambda: f(c))

    def chain(c, k, base, lbuf, rbuf, sbuf, msg, root):
        if k > 0:

            @pl.when(z == 0)
            def _():
                sbuf[...] = base().astype(BF16)
                msg(True).start()

        if k < NZ - 1:

            @pl.when(z == NZ - 1)
            def _():
                sbuf[...] = base().astype(BF16)
                msg(False).start()

        if k > 1:

            @pl.when((z > 0) & (z < k))
            def _():
                msg(True).wait_recv()
                sbuf[...] = (base() + lbuf[...].astype(F32)).astype(BF16)
                msg(True).start()

        if k < NZ - 2:

            @pl.when((z < NZ - 1) & (z > k))
            def _():
                msg(False).wait_recv()
                sbuf[...] = (base() + rbuf[...].astype(F32)).astype(BF16)
                msg(False).start()

        pl.when(z == k)(root)

    def arrived(k, lbuf, rbuf, msg):
        total = 0.0
        if k > 0:
            msg(True).wait_recv()
            total = lbuf[...].astype(F32)
        if k < NZ - 1:
            msg(False).wait_recv()
            total = total + rbuf[...].astype(F32)
        return total

    def spread(k, msg):
        if k < NZ - 1:
            pl.when((z >= k) & (z < NZ - 1))(lambda: msg(True).start())
        if k > 0:
            pl.when((z <= k) & (z > 0))(lambda: msg(False).start())

    def outer_in(c):
        m_y1(c).wait_recv()
        s1[c] = (part1(c, yy)[...] + ry1[c].astype(F32)).astype(BF16)
        m_in(c).start()

    def centre_sum(c):
        m_y1(c).wait_recv()
        m_in(c).wait_recv()
        s1[c] = (part1(c, yy)[...] + ry1[c].astype(F32) + r_in[c].astype(F32)).astype(BF16)
        m_ex(c).start()

    def centre_out(c):
        m_ex(c).wait_recv()
        y1_place(c, yy)[...] = (s1[c].astype(F32) + r_ex[c].astype(F32)).astype(BF16)
        m_o1(c).start()
        m_a1(c, yy).start()

    def outer_out(c):
        m_o1(c).wait_recv()
        m_a1(c, yy).start()

    def reduce2(c, q):
        k = ROOT2[q]
        i = q // M2
        bufs = rl2.at[c, i], rr2.at[c, i]

        def base():
            return part2(c, q)[...]

        def msg(to_right):
            return m_z2(c, q, to_right)

        def root():
            more = arrived(k, *bufs, msg)
            s2[c, i] = (base() + more).astype(BF16)
            m_y2(c, q).start()

        chain(c, k, base, *bufs, s2.at[c, i], msg, root)

    def cross2(c, q):
        k = ROOT2[q]

        @pl.when(z == k)
        def _():
            m_y2(c, q).wait_recv()
            y2_place(c, q)[...] = (s2[c, q // M2].astype(F32) + ry2[c].astype(F32)).astype(BF16)
            spread(k, lambda to_right: m_b2(c, q, to_right))

    def bcast2(c, q):
        k = ROOT2[q]

        @pl.when(z != k)
        def _():
            m_b2(c, q, True).wait_recv()
            spread(k, lambda to_right: m_b2(c, q, to_right))

    def finish(c):
        m_a1(c, 1 - yy).wait_recv()
        m_df(c, core).start()

    def dist(k):
        return jnp.where(z < k, k - z, z - k)

    def when_in(c, cond, f):
        pl.when((c >= 0) & (c < n) & cond)(lambda: f(c))

    at_in = NJ + HY
    at_sum = at_in + HC
    at_out = at_sum + HE
    at_end = at_out + HO
    last = max([at_end + HF] + [NJ + HX + E2 + (HZ + HB) * _far(k) for k in ROOT2])
    centre = jnp.logical_not(outer)

    def second(it, lag, f):
        for q, k in enumerate(ROOT2):
            guarded(it - lag(k), functools.partial(f, q=q), q, M2)

    def drain(c):
        hid_msg(c).wait_send()
        m_y1(c).wait_send()
        m_in(c).wait_send()
        pl.when(centre)(lambda: m_o1(c).wait_send())
        m_a1(c, yy).wait_send()
        for q, k in enumerate(ROOT2):

            @pl.when(active(c, q, M2))
            def _():
                pl.when(z != k)(lambda: m_z2(c, q, True).wait_send())
                pl.when(z == k)(lambda: m_y2(c, q).wait_send())
                if k < NZ - 1:
                    pl.when((z >= k) & (z < NZ - 1))(lambda: m_b2(c, q, True).wait_send())
                if k > 0:
                    pl.when((z <= k) & (z > 0))(lambda: m_b2(c, q, False).wait_send())

    def step(it, carry):
        compute(it)
        for name in ORDER:
            if name == "s":
                when_in(it - at_in, outer, outer_in)
            if name == "c":
                when_in(it - at_sum, centre, centre_sum)
            if name == "e":
                when_in(it - at_out, centre, centre_out)
            if name == "o":
                when_in(it - at_end, outer, outer_out)
            if name == "z":
                second(it, lambda k: NJ + HZ * _hops(z, k), reduce2)
            if name == "x":
                second(it, lambda k: NJ + HX + HZ * _far(k), cross2)
            if name == "b":
                second(it, lambda k: NJ + HX + E2 + HZ * _far(k) + HB * dist(k), bcast2)
        guarded(it - last, finish)
        guarded(it - last - 1, drain)
        return carry

    lax.fori_loop(0, n + last, step, 0)

    for j in range(NJ):
        wd_msg(j).wait_send()

    drain(n - 1)

    def drain_rows(c, carry):
        m_df(c, core).wait_send()
        m_df(c, 1 - core).wait_recv()
        return carry

    lax.fori_loop(0, n, drain_rows, 0)


def put_out(y, out, sem):
    parts = sem.shape[0]
    rows = y.shape[0] // parts
    copies = [
        pltpu.make_async_copy(y.at[pl.ds(i * rows, rows)], out.at[pl.ds(i * rows, rows)], sem.at[i]) for i in range(parts)
    ]
    for c in copies:
        c.start()
    for c in copies:
        c.wait()


def block(x, w_gate, w_up, w_down):
    rows, width = x.shape
    units = w_gate.shape[1]
    n_super = rows // R
    n = NJ * n_super
    cw = width // 2 // NJ
    n2 = len(ROOT2) // M2
    w1, w2 = cw // 2, cw // n2
    nb = min(256, units // NJ)
    blocks = units // nb
    dma = pltpu.SemaphoreType.DMA
    one = pltpu.VMEM((n, R1, w1), BF16)
    two = pltpu.VMEM((n, n2, R2, w2), BF16)
    cross = pltpu.VMEM((n, R2, w2), BF16)
    y = pl.pallas_call(
        kernel,
        out_shape=pltpu.VMEM((rows, width), BF16),
        in_specs=[pl.BlockSpec(memory_space=pl.ANY)] * 4,
        out_specs=pl.BlockSpec(memory_space=pltpu.VMEM),
        scratch_shapes=[
            pltpu.VMEM((n_super, R, width), BF16),
            pltpu.VMEM((blocks, width, nb), BF16),
            pltpu.VMEM((blocks, width, nb), BF16),
            pltpu.VMEM((NJ, 2 * units, cw), BF16),
            pltpu.VMEM((n_super, R, 2 * units), BF16),
            pltpu.VMEM((n, R, cw), F32),
            one, one, one, one, one, two, two, two, cross,
            dma((n_super + 2 * blocks + NJ,)), dma((NJ,)), dma((NJ,)), dma((n,)), dma((n,)),
            *[dma((n,))] * 13,
            *[dma((n, n2))] * 6,
        ],
        compiler_params=pltpu.CompilerParams(
            collective_id=0, has_side_effects=True, vmem_limit_bytes=52 * 1024 * 1024
        ),
    )(x, w_gate, w_up, w_down)
    return pl.pallas_call(
        put_out,
        out_shape=jax.ShapeDtypeStruct((rows, width), BF16),
        in_specs=[pl.BlockSpec(memory_space=pltpu.VMEM)],
        out_specs=pl.BlockSpec(memory_space=pl.ANY),
        scratch_shapes=[dma((8,))],
        name="put_out",
        compiler_params=pltpu.CompilerParams(vmem_limit_bytes=1024 * 1024),
    )(y)


def solution(mesh):
    return jax.shard_map(
        block,
        mesh=mesh,
        in_specs=(P("dp", None), P(None, "tp"), P(None, "tp"), P("tp", None)),
        out_specs=P("dp", None),
        check_vma=False,
    )
```

```python
import functools

import jax
import jax.numpy as jnp
from jax import lax
from jax.experimental import pallas as pl
from jax.experimental.pallas import tpu as pltpu
from jax.sharding import PartitionSpec as P

F32, BF16 = jnp.float32, jnp.bfloat16

R = 256
R1, R2 = 192, 64
NJ = 2
ROOT2 = (0, 3, 2, 1)
M2 = 4
NZ = 4
HY, HC, HE, HO, HF = 3, 2, 2, 2, 0
HZ, HX, HB, E2 = 2, 4, 2, 0
ORDER = "zsecxob"


def _far(k):
    return max(k, NZ - 1 - k)


def _hops(z, k):
    return jnp.where(z < k, z, jnp.where(z > k, NZ - 1 - z, _far(k)))


def kernel(
    x_hbm, wg_hbm, wu_hbm, wd_hbm, y,
    x, wg, wu, wd, hid0, hid1, part,
    sy1, ry1, s1, r_in, r_ex, s2, rl2, rr2, ry2,
    in_sem, wd_s, wd_r, hid_s, hid_r,
    y1_s, y1_r, z1_s, in_r, ex_r, o1_s, o1_r, a1_s, a1_r, y2_s, y2_r, df_s, df_r,
    z2_s, l2_r, r2_r, bl2_s, br2_s, b2_r,
):
    rows, width = y.shape
    n_super = rows // R
    n = NJ * n_super
    half = width // 2
    cw = half // NJ
    units = wg_hbm.shape[1]
    uh = units // NJ
    nb = min(256, uh)
    blocks = units // nb
    w1 = cw // 2
    w2 = cw * M2 // len(ROOT2)

    me = lax.axis_index("tp")
    core = lax.rem(me, 2)
    z = lax.rem(lax.div(me, 2), NZ)
    yy = lax.div(me, 2 * NZ)
    peer = {"tp": me + 1 - 2 * core}
    ypeer = {"tp": lax.rem(me + 2 * NZ, 4 * NZ)}
    left = {"tp": me - 2}
    right = {"tp": me + 2}
    outer = (z == 0) | (z == NZ - 1)
    step_in = jnp.where(z < NZ // 2, 2, -2)
    inward = {"tp": me + step_in}
    outward = {"tp": me - step_in}

    def load(i, src, dst):
        return pltpu.make_async_copy(src, dst, in_sem.at[i])

    def al(v, m):
        return pl.multiple_of(v, m)

    def x_copy(s):
        return load(s, x_hbm.at[pl.ds(al(s * R, R), R)], x.at[s])

    def g_copy(b):
        return load(n_super + b, wg_hbm.at[:, pl.ds(b * nb, nb)], wg.at[b])

    def u_copy(b):
        return load(n_super + blocks + b, wu_hbm.at[:, pl.ds(b * nb, nb)], wu.at[b])

    def d_copy(j):
        return load(
            n_super + 2 * blocks + j,
            wd_hbm.at[:, pl.ds(al(core * half + j * cw, cw), cw)],
            wd.at[j, pl.ds(al(core * units, units), units)],
        )

    def remote(src, dst, ssem, rsem, dev):
        return pltpu.make_async_remote_copy(
            src_ref=src, dst_ref=dst, send_sem=ssem, recv_sem=rsem,
            device_id=dev, device_id_type=pl.DeviceIdType.MESH,
        )

    x_copy(0).start()
    for b in range(blocks):
        g_copy(b).start()
        u_copy(b).start()
    for j in range(NJ):
        d_copy(j).start()
    x_copy(1).start()

    barrier = pltpu.get_barrier_semaphore()

    def hello(dev):
        pl.semaphore_signal(barrier, inc=1, device_id=dev, device_id_type=pl.DeviceIdType.MESH)

    hello(peer)
    hello(ypeer)
    pl.when(z > 0)(lambda: hello(left))
    pl.when(z < NZ - 1)(lambda: hello(right))
    pl.semaphore_wait(barrier, 2 + jnp.minimum(z, 1) + jnp.minimum(NZ - 1 - z, 1))

    def wd_msg(j):
        return remote(
            wd_hbm.at[:, pl.ds(al((1 - core) * half + j * cw, cw), cw)],
            wd.at[j, pl.ds(al(core * units, units), units)],
            wd_s.at[j], wd_r.at[j], peer,
        )

    for j in range(NJ):
        wd_msg(j).start()
    for s in range(2, n_super):
        x_copy(s).start()

    hid = hid0, hid1

    def hid_msg(c, odd):
        s, j = lax.div(c, 2 * NJ), lax.rem(c, NJ)
        place = hid[odd].at[s, :, pl.ds(al(core * units + j * uh, uh), uh)]
        return remote(place, place, hid_s.at[c], hid_r.at[c], peer)

    def row0(c):
        return al(lax.div(c, NJ) * R, R)

    def col0(c, who):
        return al(who * half + lax.rem(c, NJ) * cw, cw)

    def y1_place(c, h):
        return y.at[pl.ds(row0(c), R1), pl.ds(al(col0(c, core) + h * w1, w1), w1)]

    def y2_place(c, q):
        return y.at[pl.ds(al(row0(c) + R1, 16), R2), pl.ds(al(col0(c, core) + q // M2 * w2, w2), w2)]

    def part1(c, h):
        return part.at[c, pl.ds(0, R1), pl.ds(al(h * w1, w1), w1)]

    def part2(c, q):
        return part.at[c, pl.ds(R1, R2), pl.ds(q // M2 * w2, w2)]

    def m_y1(c):
        return remote(sy1.at[c], ry1.at[c], y1_s.at[c], y1_r.at[c], ypeer)

    def m_in(c):
        return remote(s1.at[c], r_in.at[c], z1_s.at[c], in_r.at[c], inward)

    def m_ex(c):
        return remote(s1.at[c], r_ex.at[c], z1_s.at[c], ex_r.at[c], inward)

    def m_o1(c):
        place = y1_place(c, yy)
        return remote(place, place, o1_s.at[c], o1_r.at[c], outward)

    def m_a1(c, h):
        place = y1_place(c, h)
        return remote(place, place, a1_s.at[c], a1_r.at[c], ypeer)

    def m_z2(c, q, to_right):
        i = q // M2
        dst, sem = (rl2, l2_r) if to_right else (rr2, r2_r)
        return remote(s2.at[c, i], dst.at[c, i], z2_s.at[c, i], sem.at[c, i], right if to_right else left)

    def m_y2(c, q):
        return remote(s2.at[c, q // M2], ry2.at[c], y2_s.at[c], y2_r.at[c], ypeer)

    def m_b2(c, q, to_right):
        i = q // M2
        place = y2_place(c, q)
        return remote(place, place, (br2_s if to_right else bl2_s).at[c, i], b2_r.at[c, i], right if to_right else left)

    def m_df(c, who):
        place = y.at[pl.ds(row0(c), R), pl.ds(col0(c, who), cw)]
        return remote(place, place, df_s.at[c], df_r.at[c], peer)

    def gate_up_wait(it):
        @pl.when(lax.rem(it, NJ) == 0)
        def _():
            x_copy(lax.div(it, NJ)).wait()

    def gate_up(it, odd, first=None, part_of=range(uh // nb)):
        s, j = lax.div(it, NJ), lax.rem(it, NJ)
        for b in part_of:
            block = j * (uh // nb) + b
            if first is not None:
                g_copy(first * (uh // nb) + b).wait()
                u_copy(first * (uh // nb) + b).wait()
            gate = jnp.dot(x[s], wg[block], preferred_element_type=F32)
            up = jnp.dot(x[s], wu[block], preferred_element_type=F32)
            cols = pl.ds(al(core * units + j * uh + b * nb, nb), nb)
            hid[odd][lax.div(s, 2), :, cols] = (jax.nn.gelu(gate) * up).astype(BF16)

    def down_wait(c, odd):
        for j in range(NJ):

            @pl.when(c == j)
            def _():
                d_copy(j).wait()
                wd_msg(j).wait_recv()

        @pl.when(lax.rem(c, NJ) == 0)
        def _():
            for j in range(NJ):
                hid_msg(c + j, odd).wait_recv()

    def down(c, odd, blocks):
        s, j = lax.div(c, 2 * NJ), lax.rem(c, NJ)
        for b in blocks:
            cols = pl.ds(b * db, db)
            part[c, :, cols] = jnp.dot(hid[odd][s], wd[j, :, cols], preferred_element_type=F32)

    db = min(256, cw)
    down_blocks = range(cw // db)

    def down_send(c):
        sy1[c] = part1(c, 1 - yy)[...].astype(BF16)
        m_y1(c).start()

    def compute(it):
        for j in range(NJ):

            @pl.when(it == j)
            def _():
                gate_up_wait(it)
                gate_up(it, 0, first=j)
                hid_msg(it, 0).start()

        for odd in range(2):
            here = (it >= NJ) & (it < n) & (lax.rem(lax.div(it, NJ), 2) == odd)

            @pl.when(here & (lax.rem(it, NJ) == 0))
            def _():
                gate_up_wait(it)
                gate_up(it, odd, part_of=range(1))
                down_wait(it - NJ, 1 - odd)
                gate_up(it, odd, part_of=range(1, uh // nb))
                down(it - NJ, 1 - odd, down_blocks)
                hid_msg(it, odd).start()
                down_send(it - NJ)

            @pl.when(here & (lax.rem(it, NJ) != 0))
            def _():
                down_wait(it - NJ, 1 - odd)
                gate_up(it, odd)
                down(it - NJ, 1 - odd, down_blocks)
                hid_msg(it, odd).start()
                down_send(it - NJ)

        @pl.when((it >= n) & (it < n + NJ))
        def _():
            odd = (n_super - 1) % 2
            down_wait(it - NJ, odd)
            down(it - NJ, odd, down_blocks)
            down_send(it - NJ)

    def active(c, p, m):
        return True if m == 1 else lax.rem(c, m) == p % m

    def guarded(c, f, p=0, m=1):
        pl.when((c >= 0) & (c < n) & active(c, p, m))(lambda: f(c))

    def chain(c, k, base, lbuf, rbuf, sbuf, msg, root):
        if k > 0:

            @pl.when(z == 0)
            def _():
                sbuf[...] = base().astype(BF16)
                msg(True).start()

        if k < NZ - 1:

            @pl.when(z == NZ - 1)
            def _():
                sbuf[...] = base().astype(BF16)
                msg(False).start()

        if k > 1:

            @pl.when((z > 0) & (z < k))
            def _():
                msg(True).wait_recv()
                sbuf[...] = (base() + lbuf[...].astype(F32)).astype(BF16)
                msg(True).start()

        if k < NZ - 2:

            @pl.when((z < NZ - 1) & (z > k))
            def _():
                msg(False).wait_recv()
                sbuf[...] = (base() + rbuf[...].astype(F32)).astype(BF16)
                msg(False).start()

        pl.when(z == k)(root)

    def arrived(k, lbuf, rbuf, msg):
        total = 0.0
        if k > 0:
            msg(True).wait_recv()
            total = lbuf[...].astype(F32)
        if k < NZ - 1:
            msg(False).wait_recv()
            total = total + rbuf[...].astype(F32)
        return total

    def spread(k, msg):
        if k < NZ - 1:
            pl.when((z >= k) & (z < NZ - 1))(lambda: msg(True).start())
        if k > 0:
            pl.when((z <= k) & (z > 0))(lambda: msg(False).start())

    def outer_in(c):
        m_y1(c).wait_recv()
        s1[c] = (part1(c, yy)[...] + ry1[c].astype(F32)).astype(BF16)
        m_in(c).start()

    def centre_sum(c):
        m_y1(c).wait_recv()
        m_in(c).wait_recv()
        s1[c] = (part1(c, yy)[...] + ry1[c].astype(F32) + r_in[c].astype(F32)).astype(BF16)
        m_ex(c).start()

    def centre_out(c):
        m_ex(c).wait_recv()
        y1_place(c, yy)[...] = (s1[c].astype(F32) + r_ex[c].astype(F32)).astype(BF16)
        m_o1(c).start()
        m_a1(c, yy).start()

    def outer_out(c):
        m_o1(c).wait_recv()
        m_a1(c, yy).start()

    def reduce2(c, q):
        k = ROOT2[q]
        i = q // M2
        bufs = rl2.at[c, i], rr2.at[c, i]

        def base():
            return part2(c, q)[...]

        def msg(to_right):
            return m_z2(c, q, to_right)

        def root():
            more = arrived(k, *bufs, msg)
            s2[c, i] = (base() + more).astype(BF16)
            m_y2(c, q).start()

        chain(c, k, base, *bufs, s2.at[c, i], msg, root)

    def cross2(c, q):
        k = ROOT2[q]

        @pl.when(z == k)
        def _():
            m_y2(c, q).wait_recv()
            y2_place(c, q)[...] = (s2[c, q // M2].astype(F32) + ry2[c].astype(F32)).astype(BF16)
            spread(k, lambda to_right: m_b2(c, q, to_right))

    def bcast2(c, q):
        k = ROOT2[q]

        @pl.when(z != k)
        def _():
            m_b2(c, q, True).wait_recv()
            spread(k, lambda to_right: m_b2(c, q, to_right))

    def finish(c):
        m_a1(c, 1 - yy).wait_recv()
        m_df(c, core).start()

    def dist(k):
        return jnp.where(z < k, k - z, z - k)

    def when_in(c, cond, f):
        pl.when((c >= 0) & (c < n) & cond)(lambda: f(c))

    at_in = NJ + HY
    at_sum = at_in + HC
    at_out = at_sum + HE
    at_end = at_out + HO
    last = max([at_end + HF] + [NJ + HX + E2 + (HZ + HB) * _far(k) for k in ROOT2])
    centre = jnp.logical_not(outer)

    def second(it, lag, f):
        for q, k in enumerate(ROOT2):
            guarded(it - lag(k), functools.partial(f, q=q), q, M2)

    def step(it, carry):
        compute(it)
        for name in ORDER:
            if name == "s":
                when_in(it - at_in, outer, outer_in)
            if name == "c":
                when_in(it - at_sum, centre, centre_sum)
            if name == "e":
                when_in(it - at_out, centre, centre_out)
            if name == "o":
                when_in(it - at_end, outer, outer_out)
            if name == "z":
                second(it, lambda k: NJ + HZ * _hops(z, k), reduce2)
            if name == "x":
                second(it, lambda k: NJ + HX + HZ * _far(k), cross2)
            if name == "b":
                second(it, lambda k: NJ + HX + E2 + HZ * _far(k) + HB * dist(k), bcast2)
        guarded(it - last, finish)
        return carry

    lax.fori_loop(0, n + last, step, 0)

    for j in range(NJ):
        wd_msg(j).wait_send()

    def drain(c, carry):
        for odd in range(2):
            pl.when(lax.rem(lax.div(c, NJ), 2) == odd)(lambda: hid_msg(c, odd).wait_send())
        m_y1(c).wait_send()
        m_in(c).wait_send()
        pl.when(centre)(lambda: m_o1(c).wait_send())
        m_a1(c, yy).wait_send()
        for q, k in enumerate(ROOT2):

            @pl.when(active(c, q, M2))
            def _():
                pl.when(z != k)(lambda: m_z2(c, q, True).wait_send())
                pl.when(z == k)(lambda: m_y2(c, q).wait_send())
                if k < NZ - 1:
                    pl.when((z >= k) & (z < NZ - 1))(lambda: m_b2(c, q, True).wait_send())
                if k > 0:
                    pl.when((z <= k) & (z > 0))(lambda: m_b2(c, q, False).wait_send())

        return carry

    lax.fori_loop(0, n, drain, 0)

    def drain_rows(c, carry):
        m_df(c, core).wait_send()
        m_df(c, 1 - core).wait_recv()
        return carry

    lax.fori_loop(0, n, drain_rows, 0)


def put_out(y, out, sem):
    parts = sem.shape[0]
    rows = y.shape[0] // parts
    copies = [
        pltpu.make_async_copy(y.at[pl.ds(i * rows, rows)], out.at[pl.ds(i * rows, rows)], sem.at[i]) for i in range(parts)
    ]
    for c in copies:
        c.start()
    for c in copies:
        c.wait()


def block(x, w_gate, w_up, w_down):
    rows, width = x.shape
    units = w_gate.shape[1]
    n_super = rows // R
    n = NJ * n_super
    cw = width // 2 // NJ
    n2 = len(ROOT2) // M2
    w1, w2 = cw // 2, cw // n2
    nb = min(256, units // NJ)
    blocks = units // nb
    dma = pltpu.SemaphoreType.DMA
    one = pltpu.VMEM((n, R1, w1), BF16)
    two = pltpu.VMEM((n, n2, R2, w2), BF16)
    cross = pltpu.VMEM((n, R2, w2), BF16)
    y = pl.pallas_call(
        kernel,
        out_shape=pltpu.VMEM((rows, width), BF16),
        in_specs=[pl.BlockSpec(memory_space=pl.ANY)] * 4,
        out_specs=pl.BlockSpec(memory_space=pltpu.VMEM),
        scratch_shapes=[
            pltpu.VMEM((n_super, R, width), BF16),
            pltpu.VMEM((blocks, width, nb), BF16),
            pltpu.VMEM((blocks, width, nb), BF16),
            pltpu.VMEM((NJ, 2 * units, cw), BF16),
            *[pltpu.VMEM(((n_super + 1) // 2, R, 2 * units), BF16)] * 2,
            pltpu.VMEM((n, R, cw), F32),
            one, one, one, one, one, two, two, two, cross,
            dma((n_super + 2 * blocks + NJ,)), dma((NJ,)), dma((NJ,)), dma((n,)), dma((n,)),
            *[dma((n,))] * 13,
            *[dma((n, n2))] * 6,
        ],
        compiler_params=pltpu.CompilerParams(
            collective_id=0, has_side_effects=True, vmem_limit_bytes=52 * 1024 * 1024
        ),
    )(x, w_gate, w_up, w_down)
    return pl.pallas_call(
        put_out,
        out_shape=jax.ShapeDtypeStruct((rows, width), BF16),
        in_specs=[pl.BlockSpec(memory_space=pltpu.VMEM)],
        out_specs=pl.BlockSpec(memory_space=pl.ANY),
        scratch_shapes=[dma((8,))],
        name="put_out",
        compiler_params=pltpu.CompilerParams(vmem_limit_bytes=1024 * 1024),
    )(y)


def solution(mesh):
    return jax.shard_map(
        block,
        mesh=mesh,
        in_specs=(P("dp", None), P(None, "tp"), P(None, "tp"), P("tp", None)),
        out_specs=P("dp", None),
        check_vma=False,
    )
```
